16 devices in a mesh: fsdp: 16 (over z, y, x, core).
Axes of the slice: x: 2, y: 2, z: 2, core: 2. Of those that a mesh axis runs over, the one named last changes fastest.
Arguments:
- token_ids: int32 [2, 64, 64], P(None, 'fsdp')
- labels: int32 [2, 64, 64], P(None, 'fsdp')
- emb_table: bfloat16 [32128, 768], P('fsdp')
- w_gate: bfloat16 [768, 2048], P('fsdp')
- w_up: bfloat16 [768, 2048], P('fsdp')
- w_down: bfloat16 [2048, 768], P('fsdp')
- gain_in: float32 [768], replicated
- gain_out: float32 [768], replicated
Outputs:
- output 1: float32 [], replicated
- output 2: float32 [32128, 768], P('fsdp')
- output 3: float32 [768, 2048], P('fsdp')
- output 4: float32 [768, 2048], P('fsdp')
- output 5: float32 [2048, 768], P('fsdp')
All inputs are finite; a program needn't handle non-finite values.
Results may differ from the reference program's by a relative error of at most 0.0126113.
Values are sent between devices in bfloat16 or wider.
A program may use at most 1 GiB of HBM per device.

```python
import jax
import jax.numpy as jnp
from jax import lax

VOCAB_SIZE = 32128
MODEL_DIM = 768
FFN_DIM = 2048
SEQ_LEN = 64
BATCH_ROWS = 64
MICRO_STEPS = 2
TOKENS = MICRO_STEPS * BATCH_ROWS * SEQ_LEN
REF_BLOCK = min(256, TOKENS)
NORM_EPS = 1e-6


def setup_inputs(seed: int = 0) -> dict:
    sub_keys = jax.random.split(jax.random.key(seed), 8)
    tok_shape = (MICRO_STEPS, BATCH_ROWS, SEQ_LEN)
    token_ids = jax.random.randint(sub_keys[0], tok_shape, 0, VOCAB_SIZE, dtype=jnp.int32)
    labels = jax.random.randint(sub_keys[1], tok_shape, 0, VOCAB_SIZE, dtype=jnp.int32)
    emb_table = (jax.random.normal(sub_keys[2], (VOCAB_SIZE, MODEL_DIM), jnp.float32) * MODEL_DIM ** -0.5).astype(jnp.bfloat16)
    w_gate = (jax.random.normal(sub_keys[3], (MODEL_DIM, FFN_DIM), jnp.float32) * MODEL_DIM ** -0.5).astype(jnp.bfloat16)
    w_up = (jax.random.normal(sub_keys[4], (MODEL_DIM, FFN_DIM), jnp.float32) * MODEL_DIM ** -0.5).astype(jnp.bfloat16)
    w_down = (jax.random.normal(sub_keys[5], (FFN_DIM, MODEL_DIM), jnp.float32) * (1.5 * (FFN_DIM * MODEL_DIM) ** -0.5)).astype(jnp.bfloat16)
    gain_in = 1.0 + 0.3 * jax.random.normal(sub_keys[6], (MODEL_DIM,), jnp.float32)
    gain_out = 1.0 + 0.3 * jax.random.normal(sub_keys[7], (MODEL_DIM,), jnp.float32)
    return {'token_ids': token_ids, 'labels': labels, 'emb_table': emb_table, 'w_gate': w_gate, 'w_up': w_up, 'w_down': w_down, 'gain_in': gain_in, 'gain_out': gain_out}


def rms_scale(values, gain_vec):
    vals32 = values.astype(jnp.float32)
    inv_rms = lax.rsqrt(jnp.mean(vals32 * vals32, axis=-1, keepdims=True) + NORM_EPS)
    return (vals32 * inv_rms * gain_vec).astype(jnp.bfloat16)


def block_loss(params, gain_in, gain_out, ids_blk, lab_blk):
    emb_table = params[0].astype(jnp.bfloat16)
    w_gate = params[1].astype(jnp.bfloat16)
    w_up = params[2].astype(jnp.bfloat16)
    w_down = params[3].astype(jnp.bfloat16)
    emb_rows = jnp.take(emb_table, ids_blk, axis=0)
    normed_in = rms_scale(emb_rows, gain_in)
    gate_pre = jnp.dot(normed_in, w_gate, preferred_element_type=jnp.float32).astype(jnp.bfloat16)
    up_proj = jnp.dot(normed_in, w_up, preferred_element_type=jnp.float32).astype(jnp.bfloat16)
    acts = (jax.nn.silu(gate_pre.astype(jnp.float32)) * up_proj.astype(jnp.float32)).astype(jnp.bfloat16)
    mlp_out = jnp.dot(acts, w_down, preferred_element_type=jnp.float32).astype(jnp.bfloat16)
    hidden = (emb_rows.astype(jnp.float32) + mlp_out.astype(jnp.float32)).astype(jnp.bfloat16)
    normed_out = rms_scale(hidden, gain_out)
    logits = jnp.dot(normed_out, emb_table.T, preferred_element_type=jnp.float32)
    log_norm = jax.nn.logsumexp(logits, axis=-1)
    is_label = jnp.arange(VOCAB_SIZE, dtype=jnp.int32)[None, :] == lab_blk[:, None]
    lab_logit = jnp.sum(jnp.where(is_label, logits, 0.0), axis=-1)
    return jnp.sum(log_norm - lab_logit)


def reference(token_ids, labels, emb_table, w_gate, w_up, w_down, gain_in, gain_out):
    params = (emb_table.astype(jnp.float32), w_gate.astype(jnp.float32), w_up.astype(jnp.float32), w_down.astype(jnp.float32))
    id_blocks = token_ids.reshape(-1, REF_BLOCK)
    lab_blocks = labels.reshape(-1, REF_BLOCK)
    ckpt_loss = jax.checkpoint(block_loss)

    def total_sum(weights):
        def one_block(block_pair):
            return ckpt_loss(weights, gain_in, gain_out, block_pair[0], block_pair[1])
        return jnp.sum(lax.map(one_block, (id_blocks, lab_blocks)))

    loss_sum, grad_sums = jax.value_and_grad(total_sum)(params)
    return (loss_sum / TOKENS, grad_sums[0], grad_sums[1], grad_sums[2], grad_sums[3])
```

```python
import functools
import jax
import jax.numpy as jnp
from jax import lax
from jax.experimental import pallas as pl
from jax.experimental.pallas import tpu as pltpu
from jax.sharding import PartitionSpec as P

NORM_EPS = 1e-6
SLOTS = 64
TOK_BLOCK = 256
VMEM_LIMIT = 60 * 1024 * 1024


def rms_scale(values, gain_vec):
    vals32 = values.astype(jnp.float32)
    inv_rms = lax.rsqrt(jnp.mean(vals32 * vals32, axis=-1, keepdims=True) + NORM_EPS)
    return (vals32 * inv_rms * gain_vec).astype(jnp.bfloat16), inv_rms


def rms_back(values, inv_rms, gain_vec, grad_out):
    vals32 = values.astype(jnp.float32)
    scaled = grad_out * gain_vec
    proj_mean = jnp.mean(scaled * vals32, axis=-1, keepdims=True)
    return inv_rms * scaled - vals32 * (inv_rms * inv_rms * inv_rms) * proj_mean


def mlp_forward(emb_rows, gain_in, gain_out, w_gate, w_up, w_down):
    normed_in, inv_in = rms_scale(emb_rows, gain_in)
    gate_pre = jnp.dot(normed_in, w_gate, preferred_element_type=jnp.float32).astype(jnp.bfloat16)
    up_proj = jnp.dot(normed_in, w_up, preferred_element_type=jnp.float32).astype(jnp.bfloat16)
    acts = (jax.nn.silu(gate_pre.astype(jnp.float32)) * up_proj.astype(jnp.float32)).astype(jnp.bfloat16)
    mlp_out = jnp.dot(acts, w_down, preferred_element_type=jnp.float32).astype(jnp.bfloat16)
    hidden = (emb_rows.astype(jnp.float32) + mlp_out.astype(jnp.float32)).astype(jnp.bfloat16)
    normed_out, inv_out = rms_scale(hidden, gain_out)
    return normed_out, (emb_rows, normed_in, inv_in, gate_pre, up_proj, acts, hidden, inv_out)


COLS_DIMS = (((1,), (1,)), ((), ()))
ROWS_DIMS = (((0,), (0,)), ((), ()))


def mlp_backward(saved, grad_normed, gain_in, gain_out, w_gate, w_up, w_down):
    emb_rows, normed_in, inv_in, gate_pre, up_proj, acts, hidden, inv_out = saved
    grad_hidden = rms_back(hidden, inv_out, gain_out, grad_normed)
    grad_mid = grad_hidden.astype(jnp.bfloat16)
    grad_acts = lax.dot_general(grad_mid, w_down, COLS_DIMS, preferred_element_type=jnp.float32)
    gate32 = gate_pre.astype(jnp.float32)
    gate_sig = jax.nn.sigmoid(gate32)
    grad_gate_pre = (grad_acts * up_proj.astype(jnp.float32) * gate_sig * (1.0 + gate32 * (1.0 - gate_sig))).astype(jnp.bfloat16)
    grad_up_proj = (grad_acts * gate32 * gate_sig).astype(jnp.bfloat16)
    grad_normed_in = (lax.dot_general(grad_gate_pre, w_gate, COLS_DIMS, preferred_element_type=jnp.float32)
                      + lax.dot_general(grad_up_proj, w_up, COLS_DIMS, preferred_element_type=jnp.float32))
    grad_rows = grad_hidden + rms_back(emb_rows, inv_in, gain_in, grad_normed_in)
    return grad_rows, grad_mid, grad_gate_pre, grad_up_proj


def stats_kernel(base_ref, z_ref, table_ref, lab_ref, logits_ref, stats_ref):
    logits = lax.dot_general(table_ref[...], z_ref[...], COLS_DIMS, preferred_element_type=jnp.float32)
    logits_ref[0] = logits
    col_max = jnp.max(logits, axis=0, keepdims=True)
    exp_sum = jnp.sum(jnp.exp(logits - col_max), axis=0, keepdims=True)
    row_ids = lax.broadcasted_iota(jnp.int32, logits.shape, 0)
    is_label = row_ids == (lab_ref[...] - base_ref[0])
    lab_logit = jnp.sum(jnp.where(is_label, logits, 0.0), axis=0, keepdims=True)
    stats_ref[...] = jnp.concatenate([col_max, exp_sum, lab_logit], axis=0)


def head_stats(base, z_all, table_shard, lab_row):
    tokens, dim = z_all.shape
    rows = table_shard.shape[0]
    blocks = tokens // TOK_BLOCK
    return pl.pallas_call(
        stats_kernel,
        grid=(blocks,),
        in_specs=[pl.BlockSpec(memory_space=pltpu.SMEM),
                  pl.BlockSpec((TOK_BLOCK, dim), lambda i: (i, 0)),
                  pl.BlockSpec((rows, dim), lambda i: (0, 0)),
                  pl.BlockSpec((1, TOK_BLOCK), lambda i: (0, i))],
        out_specs=[pl.BlockSpec((1, rows, TOK_BLOCK), lambda i: (i, 0, 0)),
                   pl.BlockSpec((3, TOK_BLOCK), lambda i: (0, i))],
        out_shape=[jax.ShapeDtypeStruct((blocks, rows, TOK_BLOCK), jnp.float32),
                   jax.ShapeDtypeStruct((3, tokens), jnp.float32)],
        compiler_params=pltpu.CompilerParams(vmem_limit_bytes=VMEM_LIMIT, dimension_semantics=("arbitrary",)),
        cost_estimate=pl.CostEstimate(flops=2 * tokens * rows * dim, bytes_accessed=tokens * rows * 4, transcendentals=tokens * rows),
        name="head_stats",
    )(base, z_all, table_shard, lab_row)


def grad_kernel(base_ref, logits_ref, z_ref, table_ref, lab_ref, norm_ref, init_ref, dz_ref, dtable_ref):
    logits = logits_ref[0]
    norm = norm_ref[...]
    row_ids = lax.broadcasted_iota(jnp.int32, logits.shape, 0)
    is_label = row_ids == (lab_ref[...] - base_ref[0])
    probs = jnp.exp(logits - norm[0:1]) * norm[1:2]
    grad_logits = (probs - is_label.astype(jnp.float32)).astype(jnp.bfloat16)
    dz_ref[...] = lax.dot_general(grad_logits, table_ref[...], ROWS_DIMS, preferred_element_type=jnp.float32)
    step_grad = jnp.dot(grad_logits, z_ref[...], preferred_element_type=jnp.float32)

    @pl.when(pl.program_id(0) == 0)
    def _():
        dtable_ref[...] = init_ref[...] + step_grad

    @pl.when(pl.program_id(0) > 0)
    def _():
        dtable_ref[...] += step_grad


def head_grad(base, logits, z_all, table_shard, lab_row, norm, init):
    tokens, dim = z_all.shape
    rows = table_shard.shape[0]
    blocks = tokens // TOK_BLOCK
    return pl.pallas_call(
        grad_kernel,
        grid=(blocks,),
        in_specs=[pl.BlockSpec(memory_space=pltpu.SMEM),
                  pl.BlockSpec((1, rows, TOK_BLOCK), lambda i: (i, 0, 0)),
                  pl.BlockSpec((TOK_BLOCK, dim), lambda i: (i, 0)),
                  pl.BlockSpec((rows, dim), lambda i: (0, 0)),
                  pl.BlockSpec((1, TOK_BLOCK), lambda i: (0, i)),
                  pl.BlockSpec((2, TOK_BLOCK), lambda i: (0, i)),
                  pl.BlockSpec((rows, dim), lambda i: (0, 0))],
        out_specs=[pl.BlockSpec((TOK_BLOCK, dim), lambda i: (i, 0)),
                   pl.BlockSpec((rows, dim), lambda i: (0, 0))],
        out_shape=[jax.ShapeDtypeStruct((tokens, dim), jnp.float32),
                   jax.ShapeDtypeStruct((rows, dim), jnp.float32)],
        compiler_params=pltpu.CompilerParams(vmem_limit_bytes=VMEM_LIMIT, dimension_semantics=("arbitrary",)),
        cost_estimate=pl.CostEstimate(flops=4 * tokens * rows * dim, bytes_accessed=tokens * rows * 4, transcendentals=tokens * rows),
        name="head_grad",
    )(base, logits, z_all, table_shard, lab_row, norm, init)


def split3(values):
    high = lax.reduce_precision(values, 8, 7)
    rest = values - high
    mid = lax.reduce_precision(rest, 8, 7)
    low = rest - mid
    return [part.astype(jnp.bfloat16) for part in (high, mid, low)]


def pick_rows(select, values):
    total = None
    for part in split3(values):
        term = jnp.dot(select, part, preferred_element_type=jnp.float32)
        total = term if total is None else total + term
    return total


def solution(mesh):
    groups = mesh.shape['fsdp']

    def device_step(token_ids, labels, table_shard, gate_shard, up_shard, down_shard, gain_in, gain_out):
        micro_count = token_ids.shape[0]
        tok_micro = token_ids.shape[1] * token_ids.shape[2]
        tok_dev = micro_count * tok_micro
        total_tokens = tok_dev * groups
        rows, dim = table_shard.shape
        me = lax.axis_index('fsdp')
        base = (me * rows).astype(jnp.int32)
        base_arr = base.reshape(1)

        packed = jnp.stack([token_ids.reshape(tok_dev), labels.reshape(tok_dev)])
        packed_all = lax.all_gather(packed, 'fsdp', axis=0, tiled=False)
        ids_all = packed_all[:, 0]
        lab_all = packed_all[:, 1].reshape(groups, micro_count, tok_micro)

        gate_rows, ffn = gate_shard.shape
        down_rows = down_shard.shape[0]
        w_all = lax.all_gather(jnp.concatenate([gate_shard, up_shard, down_shard.reshape(gate_rows, ffn)], axis=0), 'fsdp', axis=0, tiled=False)
        w_gate = w_all[:, :gate_rows].reshape(groups * gate_rows, ffn)
        w_up = w_all[:, gate_rows:2 * gate_rows].reshape(groups * gate_rows, ffn)
        w_down = w_all[:, 2 * gate_rows:].reshape(groups, down_rows, dim).reshape(groups * down_rows, dim)

        owner = ids_all // rows
        local = ids_all - owner * rows
        owner_hot = owner[:, :, None] == jnp.arange(groups, dtype=jnp.int32)
        tri = jnp.tril(jnp.ones((tok_dev, tok_dev), jnp.bfloat16), -1)
        before = jnp.einsum('tu,suo->sto', tri, owner_hot.astype(jnp.bfloat16), preferred_element_type=jnp.float32)
        rank = jnp.sum(jnp.where(owner_hot, before, 0.0), axis=-1).astype(jnp.int32)
        rounds = jnp.max(rank) // SLOTS + 1
        my_owner = lax.dynamic_index_in_dim(owner, me, 0, keepdims=False)
        my_rank = lax.dynamic_index_in_dim(rank, me, 0, keepdims=False)
        owned = owner == me
        slot_ids = jnp.arange(SLOTS, dtype=jnp.int32)

        def owned_rows(round_idx):
            hit = owned[:, None, :] & (rank[:, None, :] == slot_ids[None, :, None] + round_idx * SLOTS)
            return (jnp.sum(jnp.where(hit, local[:, None, :] + 1, 0), axis=-1) - 1).reshape(groups * SLOTS)

        def my_slots(round_idx):
            off = my_rank - round_idx * SLOTS
            return jnp.where((off >= 0) & (off < SLOTS), my_owner * SLOTS + off, -1)

        def fetch_round(round_idx):
            row_idx = owned_rows(round_idx)
            select = (row_idx[:, None] == jnp.arange(rows, dtype=jnp.int32)[None, :]).astype(jnp.bfloat16)
            send = jnp.dot(select, table_shard, preferred_element_type=jnp.float32).astype(jnp.bfloat16)
            got = lax.all_to_all(send.reshape(groups, SLOTS, dim), 'fsdp', 0, 0).reshape(groups * SLOTS, dim)
            place = (my_slots(round_idx)[:, None] == jnp.arange(groups * SLOTS, dtype=jnp.int32)[None, :]).astype(jnp.bfloat16)
            return jnp.dot(place, got, preferred_element_type=jnp.float32).astype(jnp.bfloat16)

        def return_round(round_idx, grad_rows):
            place = (jnp.arange(groups * SLOTS, dtype=jnp.int32)[:, None] == my_slots(round_idx)[None, :]).astype(jnp.bfloat16)
            send = pick_rows(place, grad_rows)
            got = lax.all_to_all(send.reshape(groups, SLOTS, dim), 'fsdp', 0, 0).reshape(groups * SLOTS, dim)
            select = (jnp.arange(rows, dtype=jnp.int32)[:, None] == owned_rows(round_idx)[None, :]).astype(jnp.bfloat16)
            return pick_rows(select, got)

        emb_rows = fetch_round(jnp.int32(0))
        emb_rows = lax.fori_loop(1, rounds, lambda r, acc: acc + fetch_round(r), emb_rows)

        normed, saved = [], []
        for m in range(micro_count):
            out, kept = mlp_forward(emb_rows[m * tok_micro:(m + 1) * tok_micro], gain_in, gain_out, w_gate, w_up, w_down)
            normed.append(out)
            saved.append(kept)

        lab_rows = [lab_all[:, m].reshape(1, groups * tok_micro) for m in range(micro_count)]
        z_all = [lax.all_gather(normed[m], 'fsdp', axis=0, tiled=True) for m in range(micro_count)]
        dtable = jnp.zeros((rows, dim), jnp.float32)
        loss_total = jnp.zeros((), jnp.float32)
        firsts = [head_stats(base_arr, z_all[m], table_shard, lab_rows[m]) for m in range(micro_count)]
        grad_normed = []
        for m in range(micro_count):
            logits, stats = firsts[m]
            stats_all = lax.all_gather(stats, 'fsdp', axis=0, tiled=False)
            top = jnp.max(stats_all[:, 0], axis=0)
            exp_total = jnp.sum(stats_all[:, 1] * jnp.exp(stats_all[:, 0] - top[None]), axis=0)
            loss_total = loss_total + jnp.sum(top + jnp.log(exp_total) - jnp.sum(stats_all[:, 2], axis=0))
            norm = jnp.stack([top, 1.0 / exp_total])
            dz, dtable = head_grad(base_arr, logits, z_all[m], table_shard, lab_rows[m], norm, dtable)
            grad_normed.append(lax.psum_scatter(dz, 'fsdp', scatter_dimension=0, tiled=True))

        backs = [mlp_backward(saved[m], grad_normed[m], gain_in, gain_out, w_gate, w_up, w_down) for m in range(micro_count)]
        grad_rows, grad_mid, grad_gate_pre, grad_up_proj = [jnp.concatenate(parts, axis=0) for parts in zip(*backs)]
        normed_in = jnp.concatenate([kept[1] for kept in saved], axis=0)
        acts = jnp.concatenate([kept[5] for kept in saved], axis=0)
        grad_down = lax.dot_general(acts, grad_mid, ROWS_DIMS, preferred_element_type=jnp.float32)
        grad_gate = lax.dot_general(normed_in, grad_gate_pre, ROWS_DIMS, preferred_element_type=jnp.float32)
        grad_up = lax.dot_general(normed_in, grad_up_proj, ROWS_DIMS, preferred_element_type=jnp.float32)
        w_grads = jnp.concatenate([grad_gate.reshape(groups, gate_rows, ffn), grad_up.reshape(groups, gate_rows, ffn),
                                   grad_down.reshape(groups, down_rows, dim).reshape(groups, gate_rows, ffn)], axis=1)
        w_grad = lax.psum_scatter(w_grads, 'fsdp', scatter_dimension=0, tiled=False)

        dtable = dtable + return_round(jnp.int32(0), grad_rows)
        dtable = lax.fori_loop(1, rounds, lambda r, acc: acc + return_round(r, grad_rows), dtable)
        return (loss_total / total_tokens, dtable, w_grad[:gate_rows], w_grad[gate_rows:2 * gate_rows],
                w_grad[2 * gate_rows:].reshape(down_rows, dim))

    row_spec = P('fsdp', None)
    tok_spec = P(None, 'fsdp', None)
    return jax.shard_map(device_step, mesh=mesh,
                         in_specs=(tok_spec, tok_spec, row_spec, row_spec, row_spec, row_spec, P(), P()),
                         out_specs=(P(), row_spec, row_spec, row_spec, row_spec), check_vma=False)
```

```python
import functools
import jax
import jax.numpy as jnp
from jax import lax
from jax.experimental import pallas as pl
from jax.experimental.pallas import tpu as pltpu
from jax.sharding import PartitionSpec as P

NORM_EPS = 1e-6
SLOTS = 64


def rms_scale(values, gain_vec):
    vals32 = values.astype(jnp.float32)
    inv_rms = lax.rsqrt(jnp.mean(vals32 * vals32, axis=-1, keepdims=True) + NORM_EPS)
    return (vals32 * inv_rms * gain_vec).astype(jnp.bfloat16), inv_rms


def rms_back(values, inv_rms, gain_vec, grad_out):
    vals32 = values.astype(jnp.float32)
    scaled = grad_out * gain_vec
    proj_mean = jnp.mean(scaled * vals32, axis=-1, keepdims=True)
    return inv_rms * scaled - vals32 * (inv_rms * inv_rms * inv_rms) * proj_mean


def mlp_forward(emb_rows, gain_in, gain_out, w_gate, w_up, w_down):
    normed_in, inv_in = rms_scale(emb_rows, gain_in)
    gate_pre = jnp.dot(normed_in, w_gate, preferred_element_type=jnp.float32).astype(jnp.bfloat16)
    up_proj = jnp.dot(normed_in, w_up, preferred_element_type=jnp.float32).astype(jnp.bfloat16)
    acts = (jax.nn.silu(gate_pre.astype(jnp.float32)) * up_proj.astype(jnp.float32)).astype(jnp.bfloat16)
    mlp_out = jnp.dot(acts, w_down, preferred_element_type=jnp.float32).astype(jnp.bfloat16)
    hidden = (emb_rows.astype(jnp.float32) + mlp_out.astype(jnp.float32)).astype(jnp.bfloat16)
    normed_out, inv_out = rms_scale(hidden, gain_out)
    return normed_out, (emb_rows, normed_in, inv_in, gate_pre, up_proj, acts, hidden, inv_out)


COLS_DIMS = (((1,), (1,)), ((), ()))
ROWS_DIMS = (((0,), (0,)), ((), ()))


def mlp_backward(saved, grad_normed, gain_in, gain_out, w_gate, w_up, w_down):
    emb_rows, normed_in, inv_in, gate_pre, up_proj, acts, hidden, inv_out = saved
    grad_hidden = rms_back(hidden, inv_out, gain_out, grad_normed)
    grad_mid = grad_hidden.astype(jnp.bfloat16)
    grad_acts = lax.dot_general(grad_mid, w_down, COLS_DIMS, preferred_element_type=jnp.float32)
    gate32 = gate_pre.astype(jnp.float32)
    gate_sig = jax.nn.sigmoid(gate32)
    grad_gate_pre = (grad_acts * up_proj.astype(jnp.float32) * gate_sig * (1.0 + gate32 * (1.0 - gate_sig))).astype(jnp.bfloat16)
    grad_up_proj = (grad_acts * gate32 * gate_sig).astype(jnp.bfloat16)
    grad_normed_in = (lax.dot_general(grad_gate_pre, w_gate, COLS_DIMS, preferred_element_type=jnp.float32)
                      + lax.dot_general(grad_up_proj, w_up, COLS_DIMS, preferred_element_type=jnp.float32))
    grad_rows = grad_hidden + rms_back(emb_rows, inv_in, gain_in, grad_normed_in)
    return grad_rows, grad_mid, grad_gate_pre, grad_up_proj


UNIT = 64
CUBE_BITS = 3
PARTS = 3
VOCAB_TILE = 256
STAT_ROWS = 8
MESH_ID = pl.DeviceIdType.MESH
PAD_LOGIT = -1e30


def head_kernel(vocab_rows, chunks, z_hbm, table_ref, lab_ref, dz_ref, dtable_ref, loss_ref,
                zbuf, lbuf, gbuf, dzbuf, got_core, got_one, got_two, got_three, stats, norm,
                local_sem, ag_send, ag_recv, rs_send, rs_recv, st_send, st_recv):
    me = lax.axis_index('fsdp')
    total = 16
    core = lax.rem(me, 2)
    pos = [lax.rem(me // 2, 2), lax.rem(me // 4, 2), me // 8]
    base = me * vocab_rows
    padded, dim = table_ref.shape
    part_cols = dim // PARTS
    half = 8 * UNIT
    tiles = padded // VOCAB_TILE

    def peer(axis):
        return me + (1 - 2 * pos[axis]) * (2 << axis)

    core_peer = me + 1 - 2 * core

    barrier = pltpu.get_barrier_semaphore()
    for step in range(1, total):
        pl.semaphore_signal(barrier, inc=1, device_id=(lax.rem(me + step, total),), device_id_type=MESH_ID)
    own = pltpu.make_async_copy(z_hbm, zbuf.at[:, pos[2], pos[1], pos[0], core], local_sem)
    own.start()
    dtable_ref[...] = jnp.zeros_like(dtable_ref)
    loss_ref[...] = jnp.zeros_like(loss_ref)
    own.wait()
    pl.semaphore_wait(barrier, total - 1)

    def where(choice):
        return choice.get(2, slice(None)), choice.get(1, slice(None)), choice.get(0, slice(None))

    def axes(part):
        return part % 3, (part + 1) % 3, (part + 2) % 3

    def cols(part):
        return pl.ds(part * part_cols, part_cols)

    def gather_copies(chunk, phase):
        if phase == 4:
            here = zbuf.at[chunk, :, :, :, core]
            return [pltpu.make_async_remote_copy(here, here, ag_send.at[chunk, 9], ag_recv.at[chunk, 9],
                                                 device_id=(core_peer,), device_id_type=MESH_ID)]
        copies = []
        for part in range(PARTS):
            order = axes(part)
            fixed = {axis: pos[axis] for axis in order[phase - 1:]}
            iz, iy, ix = where(fixed)
            here = zbuf.at[chunk, iz, iy, ix, core, :, cols(part)]
            sem = (phase - 1) * PARTS + part
            copies.append(pltpu.make_async_remote_copy(here, here, ag_send.at[chunk, sem], ag_recv.at[chunk, sem],
                                                       device_id=(peer(order[phase - 1]),), device_id_type=MESH_ID))
        return copies

    def reduce_copies(chunk, phase):
        slot = lax.rem(chunk, 2)
        if phase == 0:
            return [pltpu.make_async_remote_copy(dzbuf.at[slot, :, :, :, 1 - core], got_core.at[slot], rs_send.at[chunk, 9], rs_recv.at[chunk, 9],
                                                 device_id=(core_peer,), device_id_type=MESH_ID)]
        copies = []
        for part in range(PARTS):
            order = axes(part)
            fixed = {axis: pos[axis] for axis in order[:phase - 1]}
            fixed[order[phase - 1]] = 1 - pos[order[phase - 1]]
            iz, iy, ix = where(fixed)
            got = (got_one, got_two, got_three)[phase - 1]
            sem = (phase - 1) * PARTS + part
            copies.append(pltpu.make_async_remote_copy(dzbuf.at[slot, iz, iy, ix, core, :, cols(part)], got.at[slot, part],
                                                       rs_send.at[chunk, sem], rs_recv.at[chunk, sem],
                                                       device_id=(peer(order[phase - 1]),), device_id_type=MESH_ID))
        return copies

    def start(copies):
        for copy in copies:
            copy.start()

    def finish(copies):
        for copy in copies:
            copy.wait()

    def reduce_add(chunk, phase):
        slot = lax.rem(chunk, 2)
        if phase == 0:
            dzbuf[slot, :, :, :, core] += got_core[slot]
            return
        for part in range(PARTS):
            order = axes(part)
            iz, iy, ix = where({axis: pos[axis] for axis in order[:phase]})
            got = (got_one, got_two, got_three)[phase - 1]
            lanes = slice(part * part_cols, (part + 1) * part_cols)
            if phase == 3:
                rows = pl.ds(pl.multiple_of(chunk * UNIT, UNIT), UNIT)
                dz_ref[rows, lanes] = dzbuf[slot, iz, iy, ix, core, :, lanes] + got[slot, part]
            else:
                dzbuf[slot, iz, iy, ix, core, :, lanes] += got[slot, part]

    def stat_copies(chunk):
        copies = []
        for step in range(1, total):
            to = lax.rem(me + step, total)
            copies.append(pltpu.make_async_remote_copy(stats.at[chunk, me], stats.at[chunk, me], st_send.at[chunk, step], st_recv.at[chunk, step],
                                                       device_id=(to,), device_id_type=MESH_ID))
        return copies

    def label_row(chunk, part):
        lab = lab_ref[pl.ds(chunk * 2 + part, 1), :] - base
        return jnp.where(lab < vocab_rows, lab, -1)

    row_ids = lax.broadcasted_iota(jnp.int32, (VOCAB_TILE, half), 0)

    def forward_half(chunk, part):
        slot = lax.rem(chunk, 2)
        zb = zbuf[chunk, part].reshape(half, dim)
        lab = label_row(chunk, part)
        tops, sums, labs = [], [], []
        for tile in range(tiles):
            rows = slice(tile * VOCAB_TILE, (tile + 1) * VOCAB_TILE)
            logits = lax.dot_general(table_ref[rows, :], zb, COLS_DIMS, preferred_element_type=jnp.float32)
            if (tile + 1) * VOCAB_TILE > vocab_rows:
                logits = jnp.where(row_ids < vocab_rows - tile * VOCAB_TILE, logits, PAD_LOGIT)
            lbuf[slot, rows, part * half:(part + 1) * half] = logits
            top = jnp.max(logits, axis=0, keepdims=True)
            tops.append(top)
            sums.append(jnp.sum(jnp.exp(logits - top), axis=0, keepdims=True))
            labs.append(jnp.sum(jnp.where(row_ids == lab - tile * VOCAB_TILE, logits, 0.0), axis=0, keepdims=True))
        top = functools.reduce(jnp.maximum, tops)
        exp_sum = sum(s * jnp.exp(t - top) for s, t in zip(sums, tops))
        stats[chunk, me, part:part + 1, :] = top
        stats[chunk, me, 2 + part:3 + part, :] = exp_sum
        stats[chunk, me, 4 + part:5 + part, :] = sum(labs)

    def combine(chunk):
        for part in range(2):
            tops = stats[chunk, :, part, :]
            top = jnp.max(tops, axis=0, keepdims=True)
            exp_sum = jnp.sum(stats[chunk, :, 2 + part, :] * jnp.exp(tops - top), axis=0, keepdims=True)
            lab = jnp.sum(stats[chunk, :, 4 + part, :], axis=0, keepdims=True)
            norm[part:part + 1, :] = top
            norm[2 + part:3 + part, :] = 1.0 / exp_sum
            loss_ref[part:part + 1, :] += top + jnp.log(exp_sum) - lab

    def table_half(chunk, which):
        slot = lax.rem(chunk, 2)
        zc = zbuf[chunk].reshape(2 * half, dim)
        for tile in range(which * tiles // 2, (which + 1) * tiles // 2):
            rows = slice(tile * VOCAB_TILE, (tile + 1) * VOCAB_TILE)
            for part in range(2):
                lanes = slice(part * half, (part + 1) * half)
                probs = jnp.exp(lbuf[slot, rows, lanes] - norm[part:part + 1, :]) * norm[2 + part:3 + part, :]
                hot = row_ids == label_row(chunk, part) - tile * VOCAB_TILE
                gbuf[rows, lanes] = jnp.where(hot, probs - 1.0, probs).astype(jnp.bfloat16)
            dtable_ref[rows, :] += jnp.dot(gbuf[rows, :], zc, preferred_element_type=jnp.float32)

    def token_half(chunk, part):
        slot = lax.rem(chunk, 2)
        dz = lax.dot_general(gbuf[:, part * half:(part + 1) * half], table_ref[...], ROWS_DIMS, preferred_element_type=jnp.float32)
        dzbuf[slot, part] = dz.reshape(2, 2, 2, UNIT, dim)

    for phase in range(1, 5):
        first = gather_copies(0, phase)
        start(first)
        finish(first)

    def body(i, carry):
        fwd = i < chunks
        more = i < chunks - 1
        bwd = (i >= 1) & (i <= chunks)
        red = (i >= 2) & (i <= chunks + 1)
        last = i >= 3
        nxt = jnp.minimum(i + 1, chunks - 1)
        prev = jnp.maximum(i - 1, 0)
        old = jnp.maximum(i - 2, 0)
        older = jnp.maximum(i - 3, 0)

        pl.when(red)(lambda: start(reduce_copies(old, 0)))
        pl.when(more)(lambda: start(gather_copies(nxt, 1)))
        pl.when(fwd)(lambda: forward_half(i, 0))

        @pl.when(last)
        def _():
            finish(reduce_copies(older, 3))
            reduce_add(older, 3)

        @pl.when(red)
        def _():
            finish(reduce_copies(old, 0))
            reduce_add(old, 0)
            start(reduce_copies(old, 1))

        @pl.when(more)
        def _():
            finish(gather_copies(nxt, 1))
            start(gather_copies(nxt, 2))
        pl.when(fwd)(lambda: forward_half(i, 1))

        @pl.when(more)
        def _():
            finish(gather_copies(nxt, 2))
            start(gather_copies(nxt, 3))

        @pl.when(bwd)
        def _():
            finish(stat_copies(prev))
            combine(prev)
            table_half(prev, 0)

        pl.when(fwd)(lambda: start(stat_copies(i)))

        @pl.when(more)
        def _():
            finish(gather_copies(nxt, 3))
            start(gather_copies(nxt, 4))
        pl.when(bwd)(lambda: table_half(prev, 1))

        @pl.when(red)
        def _():
            finish(reduce_copies(old, 1))
            reduce_add(old, 1)
            start(reduce_copies(old, 2))

        @pl.when(bwd)
        def _():
            token_half(prev, 0)
            token_half(prev, 1)

        @pl.when(red)
        def _():
            finish(reduce_copies(old, 2))
            reduce_add(old, 2)
            start(reduce_copies(old, 3))
        pl.when(more)(lambda: finish(gather_copies(nxt, 4)))
        return carry

    lax.fori_loop(0, chunks + 3, body, 0)


def head(z_local, table_padded, lab_rows, vocab_rows):
    tokens, dim = z_local.shape
    chunks = tokens // UNIT
    padded = table_padded.shape[0]
    chunk_tokens = 16 * UNIT
    part_cols = dim // PARTS
    f32, bf16 = jnp.float32, jnp.bfloat16
    sems = pltpu.SemaphoreType.DMA
    vmem = pl.BlockSpec(memory_space=pltpu.VMEM)
    cost = 6 * tokens * 16 * padded * dim
    return pl.pallas_call(
        functools.partial(head_kernel, vocab_rows, chunks),
        in_specs=[pl.BlockSpec(memory_space=pl.ANY), vmem, vmem],
        out_specs=[vmem, vmem, vmem],
        out_shape=[jax.ShapeDtypeStruct((tokens, dim), f32),
                   jax.ShapeDtypeStruct((padded, dim), f32),
                   jax.ShapeDtypeStruct((2, 8 * UNIT), f32)],
        scratch_shapes=[pltpu.VMEM((chunks, 2, 2, 2, 2, UNIT, dim), bf16),
                        pltpu.VMEM((2, padded, chunk_tokens), f32),
                        pltpu.VMEM((padded, chunk_tokens), bf16),
                        pltpu.VMEM((2, 2, 2, 2, 2, UNIT, dim), f32),
                        pltpu.VMEM((2, 2, 2, 2, UNIT, dim), f32),
                        pltpu.VMEM((2, PARTS, 2, 2, UNIT, part_cols), f32),
                        pltpu.VMEM((2, PARTS, 2, UNIT, part_cols), f32),
                        pltpu.VMEM((2, PARTS, UNIT, part_cols), f32),
                        pltpu.VMEM((chunks, 16, STAT_ROWS, 8 * UNIT), f32),
                        pltpu.VMEM((8, 8 * UNIT), f32),
                        sems(()),
                        sems((chunks, 10)), sems((chunks, 10)),
                        sems((chunks, 10)), sems((chunks, 10)),
                        sems((chunks, 16)), sems((chunks, 16))],
        compiler_params=pltpu.CompilerParams(vmem_limit_bytes=67043328, collective_id=1, has_side_effects=True),
        cost_estimate=pl.CostEstimate(flops=cost, bytes_accessed=4 * padded * dim, transcendentals=2 * tokens * 16 * padded),
        name="head_all",
    )(z_local.reshape(chunks, UNIT, dim), table_padded, lab_rows)


def split3(values):
    high = lax.reduce_precision(values, 8, 7)
    rest = values - high
    mid = lax.reduce_precision(rest, 8, 7)
    low = rest - mid
    return [part.astype(jnp.bfloat16) for part in (high, mid, low)]


def pick_rows(select, values):
    total = None
    for part in split3(values):
        term = jnp.dot(select, part, preferred_element_type=jnp.float32)
        total = term if total is None else total + term
    return total


def solution(mesh):
    groups = mesh.shape['fsdp']

    def device_step(token_ids, labels, table_shard, gate_shard, up_shard, down_shard, gain_in, gain_out):
        micro_count = token_ids.shape[0]
        tok_micro = token_ids.shape[1] * token_ids.shape[2]
        tok_dev = micro_count * tok_micro
        total_tokens = tok_dev * groups
        rows, dim = table_shard.shape
        me = lax.axis_index('fsdp')

        packed = jnp.stack([token_ids.reshape(tok_dev), labels.reshape(tok_dev)])
        packed_all = lax.all_gather(packed, 'fsdp', axis=0, tiled=False)
        ids_all = packed_all[:, 0]

        gate_rows, ffn = gate_shard.shape
        down_rows = down_shard.shape[0]
        w_all = lax.all_gather(jnp.concatenate([gate_shard, up_shard, down_shard.reshape(gate_rows, ffn)], axis=0), 'fsdp', axis=0, tiled=False)
        w_gate = w_all[:, :gate_rows].reshape(groups * gate_rows, ffn)
        w_up = w_all[:, gate_rows:2 * gate_rows].reshape(groups * gate_rows, ffn)
        w_down = w_all[:, 2 * gate_rows:].reshape(groups, down_rows, dim).reshape(groups * down_rows, dim)

        owner = ids_all // rows
        local = ids_all - owner * rows
        owner_hot = owner[:, :, None] == jnp.arange(groups, dtype=jnp.int32)
        tri = jnp.tril(jnp.ones((tok_dev, tok_dev), jnp.bfloat16), -1)
        before = jnp.einsum('tu,suo->sto', tri, owner_hot.astype(jnp.bfloat16), preferred_element_type=jnp.float32)
        rank = jnp.sum(jnp.where(owner_hot, before, 0.0), axis=-1).astype(jnp.int32)
        rounds = jnp.max(rank) // SLOTS + 1
        my_owner = lax.dynamic_index_in_dim(owner, me, 0, keepdims=False)
        my_rank = lax.dynamic_index_in_dim(rank, me, 0, keepdims=False)
        owned = owner == me
        slot_ids = jnp.arange(SLOTS, dtype=jnp.int32)

        def owned_rows(round_idx):
            hit = owned[:, None, :] & (rank[:, None, :] == slot_ids[None, :, None] + round_idx * SLOTS)
            return (jnp.sum(jnp.where(hit, local[:, None, :] + 1, 0), axis=-1) - 1).reshape(groups * SLOTS)

        def my_slots(round_idx):
            off = my_rank - round_idx * SLOTS
            return jnp.where((off >= 0) & (off < SLOTS), my_owner * SLOTS + off, -1)

        def fetch_round(round_idx):
            row_idx = owned_rows(round_idx)
            select = (row_idx[:, None] == jnp.arange(rows, dtype=jnp.int32)[None, :]).astype(jnp.bfloat16)
            send = jnp.dot(select, table_shard, preferred_element_type=jnp.float32).astype(jnp.bfloat16)
            got = lax.all_to_all(send.reshape(groups, SLOTS, dim), 'fsdp', 0, 0).reshape(groups * SLOTS, dim)
            place = (my_slots(round_idx)[:, None] == jnp.arange(groups * SLOTS, dtype=jnp.int32)[None, :]).astype(jnp.bfloat16)
            return jnp.dot(place, got, preferred_element_type=jnp.float32).astype(jnp.bfloat16)

        def return_round(round_idx, grad_rows):
            place = (jnp.arange(groups * SLOTS, dtype=jnp.int32)[:, None] == my_slots(round_idx)[None, :]).astype(jnp.bfloat16)
            send = pick_rows(place, grad_rows)
            got = lax.all_to_all(send.reshape(groups, SLOTS, dim), 'fsdp', 0, 0).reshape(groups * SLOTS, dim)
            select = (jnp.arange(rows, dtype=jnp.int32)[:, None] == owned_rows(round_idx)[None, :]).astype(jnp.bfloat16)
            return pick_rows(select, got)

        emb_rows = fetch_round(jnp.int32(0))
        emb_rows = lax.fori_loop(1, rounds, lambda r, acc: acc + fetch_round(r), emb_rows)

        normed, saved = [], []
        for m in range(micro_count):
            out, kept = mlp_forward(emb_rows[m * tok_micro:(m + 1) * tok_micro], gain_in, gain_out, w_gate, w_up, w_down)
            normed.append(out)
            saved.append(kept)

        chunks = tok_dev // UNIT
        lab_rows = jnp.transpose(packed_all[:, 1].reshape(groups, chunks, UNIT), (1, 0, 2)).reshape(2 * chunks, groups * UNIT // 2)
        padded = -(-rows // VOCAB_TILE) * VOCAB_TILE
        table_padded = jnp.pad(table_shard, ((0, padded - rows), (0, 0)))
        dz, dtable, loss_rows = head(jnp.concatenate(normed, axis=0), table_padded, lab_rows, rows)
        dtable = dtable[:rows]
        loss_total = jnp.sum(loss_rows)
        grad_normed = [dz[m * tok_micro:(m + 1) * tok_micro] for m in range(micro_count)]

        backs = [mlp_backward(saved[m], grad_normed[m], gain_in, gain_out, w_gate, w_up, w_down) for m in range(micro_count)]
        grad_rows, grad_mid, grad_gate_pre, grad_up_proj = [jnp.concatenate(parts, axis=0) for parts in zip(*backs)]
        normed_in = jnp.concatenate([kept[1] for kept in saved], axis=0)
        acts = jnp.concatenate([kept[5] for kept in saved], axis=0)
        grad_down = lax.dot_general(acts, grad_mid, ROWS_DIMS, preferred_element_type=jnp.float32)
        grad_gate = lax.dot_general(normed_in, grad_gate_pre, ROWS_DIMS, preferred_element_type=jnp.float32)
        grad_up = lax.dot_general(normed_in, grad_up_proj, ROWS_DIMS, preferred_element_type=jnp.float32)
        w_grads = jnp.concatenate([grad_gate.reshape(groups, gate_rows, ffn), grad_up.reshape(groups, gate_rows, ffn),
                                   grad_down.reshape(groups, down_rows, dim).reshape(groups, gate_rows, ffn)], axis=1)
        w_grad = lax.psum_scatter(w_grads, 'fsdp', scatter_dimension=0, tiled=False)

        dtable = dtable + return_round(jnp.int32(0), grad_rows)
        dtable = lax.fori_loop(1, rounds, lambda r, acc: acc + return_round(r, grad_rows), dtable)
        return (loss_total / total_tokens, dtable, w_grad[:gate_rows], w_grad[gate_rows:2 * gate_rows],
                w_grad[2 * gate_rows:].reshape(down_rows, dim))

    row_spec = P('fsdp', None)
    tok_spec = P(None, 'fsdp', None)
    return jax.shard_map(device_step, mesh=mesh,
                         in_specs=(tok_spec, tok_spec, row_spec, row_spec, row_spec, row_spec, P(), P()),
                         out_specs=(P(), row_spec, row_spec, row_spec, row_spec), check_vma=False)
```

```python
import functools
import jax
import jax.numpy as jnp
from jax import lax
from jax.experimental import pallas as pl
from jax.experimental.pallas import tpu as pltpu
from jax.sharding import PartitionSpec as P

NORM_EPS = 1e-6
SLOTS = 64


def rms_scale(values, gain_vec):
    vals32 = values.astype(jnp.float32)
    inv_rms = lax.rsqrt(jnp.mean(vals32 * vals32, axis=-1, keepdims=True) + NORM_EPS)
    return (vals32 * inv_rms * gain_vec).astype(jnp.bfloat16), inv_rms


def rms_back(values, inv_rms, gain_vec, grad_out):
    vals32 = values.astype(jnp.float32)
    scaled = grad_out * gain_vec
    proj_mean = jnp.mean(scaled * vals32, axis=-1, keepdims=True)
    return inv_rms * scaled - vals32 * (inv_rms * inv_rms * inv_rms) * proj_mean


def mlp_forward(emb_rows, gain_in, gain_out, w_gate, w_up, w_down):
    normed_in, inv_in = rms_scale(emb_rows, gain_in)
    gate_pre = jnp.dot(normed_in, w_gate, preferred_element_type=jnp.float32).astype(jnp.bfloat16)
    up_proj = jnp.dot(normed_in, w_up, preferred_element_type=jnp.float32).astype(jnp.bfloat16)
    acts = (jax.nn.silu(gate_pre.astype(jnp.float32)) * up_proj.astype(jnp.float32)).astype(jnp.bfloat16)
    mlp_out = jnp.dot(acts, w_down, preferred_element_type=jnp.float32).astype(jnp.bfloat16)
    hidden = (emb_rows.astype(jnp.float32) + mlp_out.astype(jnp.float32)).astype(jnp.bfloat16)
    normed_out, inv_out = rms_scale(hidden, gain_out)
    return normed_out, (emb_rows, normed_in, inv_in, gate_pre, up_proj, acts, hidden, inv_out)


COLS_DIMS = (((1,), (1,)), ((), ()))
ROWS_DIMS = (((0,), (0,)), ((), ()))


def mlp_backward(saved, grad_normed, gain_in, gain_out, w_gate, w_up, w_down):
    emb_rows, normed_in, inv_in, gate_pre, up_proj, acts, hidden, inv_out = saved
    grad_hidden = rms_back(hidden, inv_out, gain_out, grad_normed)
    grad_mid = grad_hidden.astype(jnp.bfloat16)
    grad_acts = lax.dot_general(grad_mid, w_down, COLS_DIMS, preferred_element_type=jnp.float32)
    gate32 = gate_pre.astype(jnp.float32)
    gate_sig = jax.nn.sigmoid(gate32)
    grad_gate_pre = (grad_acts * up_proj.astype(jnp.float32) * gate_sig * (1.0 + gate32 * (1.0 - gate_sig))).astype(jnp.bfloat16)
    grad_up_proj = (grad_acts * gate32 * gate_sig).astype(jnp.bfloat16)
    grad_normed_in = (lax.dot_general(grad_gate_pre, w_gate, COLS_DIMS, preferred_element_type=jnp.float32)
                      + lax.dot_general(grad_up_proj, w_up, COLS_DIMS, preferred_element_type=jnp.float32))
    grad_rows = grad_hidden + rms_back(emb_rows, inv_in, gain_in, grad_normed_in)
    return grad_rows, grad_mid, grad_gate_pre, grad_up_proj


UNIT = 64
CUBE_BITS = 3
PARTS = 3
VOCAB_TILE = 256
STAT_ROWS = 4
MESH_ID = pl.DeviceIdType.MESH
PAD_LOGIT = -1e30


def head_kernel(vocab_rows, chunks, z_hbm, table_ref, lab_ref, dz_ref, dtable_ref, loss_ref,
                zbuf, lbuf, gbuf, dzbuf, got_core, got_one, got_two, got_three, stats, labs, norm,
                local_sem, ag_send, ag_recv, rs_send, rs_recv, st_send, st_recv, lab_send, lab_recv):
    me = lax.axis_index('fsdp')
    total = 16
    core = lax.rem(me, 2)
    pos = [lax.rem(me // 2, 2), lax.rem(me // 4, 2), me // 8]
    base = me * vocab_rows
    padded, dim = table_ref.shape
    part_cols = dim // PARTS
    half = 8 * UNIT
    tiles = padded // VOCAB_TILE

    def peer(axis):
        return me + (1 - 2 * pos[axis]) * (2 << axis)

    core_peer = me + 1 - 2 * core

    barrier = pltpu.get_barrier_semaphore()
    for step in range(1, total):
        pl.semaphore_signal(barrier, inc=1, device_id=(lax.rem(me + step, total),), device_id_type=MESH_ID)
    own = pltpu.make_async_copy(z_hbm, zbuf.at[:, pos[2], pos[1], pos[0], core], local_sem)
    own.start()
    dtable_ref[...] = jnp.zeros_like(dtable_ref)
    loss_ref[...] = jnp.zeros_like(loss_ref)
    labs[me] = jnp.zeros((1, half), jnp.float32)
    own.wait()
    pl.semaphore_wait(barrier, total - 1)

    def where(choice):
        return choice.get(2, slice(None)), choice.get(1, slice(None)), choice.get(0, slice(None))

    def axes(part):
        return part % 3, (part + 1) % 3, (part + 2) % 3

    def cols(part):
        return pl.ds(part * part_cols, part_cols)

    def gather_copies(chunk, phase):
        if phase == 4:
            here = zbuf.at[chunk, :, :, :, core]
            return [pltpu.make_async_remote_copy(here, here, ag_send.at[chunk, 9], ag_recv.at[chunk, 9],
                                                 device_id=(core_peer,), device_id_type=MESH_ID)]
        copies = []
        for part in range(PARTS):
            order = axes(part)
            fixed = {axis: pos[axis] for axis in order[phase - 1:]}
            iz, iy, ix = where(fixed)
            here = zbuf.at[chunk, iz, iy, ix, core, :, cols(part)]
            sem = (phase - 1) * PARTS + part
            copies.append(pltpu.make_async_remote_copy(here, here, ag_send.at[chunk, sem], ag_recv.at[chunk, sem],
                                                       device_id=(peer(order[phase - 1]),), device_id_type=MESH_ID))
        return copies

    def reduce_copies(chunk, phase):
        slot, dzs = lax.rem(chunk, 2), lax.rem(chunk, 3)
        if phase == 0:
            return [pltpu.make_async_remote_copy(dzbuf.at[dzs, :, :, :, 1 - core], got_core.at[slot], rs_send.at[chunk, 9], rs_recv.at[chunk, 9],
                                                 device_id=(core_peer,), device_id_type=MESH_ID)]
        copies = []
        for part in range(PARTS):
            order = axes(part)
            fixed = {axis: pos[axis] for axis in order[:phase - 1]}
            fixed[order[phase - 1]] = 1 - pos[order[phase - 1]]
            iz, iy, ix = where(fixed)
            got = (got_one, got_two, got_three)[phase - 1]
            sem = (phase - 1) * PARTS + part
            copies.append(pltpu.make_async_remote_copy(dzbuf.at[dzs, iz, iy, ix, core, :, cols(part)], got.at[slot, part],
                                                       rs_send.at[chunk, sem], rs_recv.at[chunk, sem],
                                                       device_id=(peer(order[phase - 1]),), device_id_type=MESH_ID))
        return copies

    def start(copies):
        for copy in copies:
            copy.start()

    def finish(copies):
        for copy in copies:
            copy.wait()

    def reduce_add(chunk, phase):
        slot, dzs = lax.rem(chunk, 2), lax.rem(chunk, 3)
        if phase == 0:
            dzbuf[dzs, :, :, :, core] += got_core[slot]
            return
        for part in range(PARTS):
            order = axes(part)
            iz, iy, ix = where({axis: pos[axis] for axis in order[:phase]})
            got = (got_one, got_two, got_three)[phase - 1]
            lanes = slice(part * part_cols, (part + 1) * part_cols)
            if phase == 3:
                rows = pl.ds(pl.multiple_of(chunk * UNIT, UNIT), UNIT)
                dz_ref[rows, lanes] = dzbuf[dzs, iz, iy, ix, core, :, lanes] + got[slot, part]
            else:
                dzbuf[dzs, iz, iy, ix, core, :, lanes] += got[slot, part]

    def stat_copies(chunk):
        copies = []
        for step in range(1, total):
            to = lax.rem(me + step, total)
            copies.append(pltpu.make_async_remote_copy(stats.at[chunk, me], stats.at[chunk, me], st_send.at[chunk, step], st_recv.at[chunk, step],
                                                       device_id=(to,), device_id_type=MESH_ID))
        return copies

    def lab_copies():
        return [pltpu.make_async_remote_copy(labs.at[me], labs.at[me], lab_send.at[step], lab_recv.at[step],
                                             device_id=(lax.rem(me + step, total),), device_id_type=MESH_ID) for step in range(1, total)]

    def label_row(chunk, part):
        lab = lab_ref[pl.ds(chunk * 2 + part, 1), :] - base
        return jnp.where(lab < vocab_rows, lab, -1)

    row_ids = lax.broadcasted_iota(jnp.int32, (VOCAB_TILE, half), 0)

    def forward_half(chunk, part):
        slot = lax.rem(chunk, 2)
        zb = zbuf[chunk, part].reshape(half, dim)
        lab = label_row(chunk, part)
        tops, sums, hits = [], [], []
        for tile in range(tiles):
            rows = slice(tile * VOCAB_TILE, (tile + 1) * VOCAB_TILE)
            logits = lax.dot_general(table_ref[rows, :], zb, COLS_DIMS, preferred_element_type=jnp.float32)
            if (tile + 1) * VOCAB_TILE > vocab_rows:
                logits = jnp.where(row_ids < vocab_rows - tile * VOCAB_TILE, logits, PAD_LOGIT)
            lbuf[slot, rows, part * half:(part + 1) * half] = logits
            top = jnp.max(logits, axis=0, keepdims=True)
            tops.append(top)
            sums.append(jnp.sum(jnp.exp(logits - top), axis=0, keepdims=True))
            hits.append(jnp.sum(jnp.where(row_ids == lab - tile * VOCAB_TILE, logits, 0.0), axis=0, keepdims=True))
        top = functools.reduce(jnp.maximum, tops)
        exp_sum = sum(s * jnp.exp(t - top) for s, t in zip(sums, tops))
        stats[chunk, me, part:part + 1, :] = top
        stats[chunk, me, 2 + part:3 + part, :] = exp_sum
        labs[me] += sum(hits)

    def combine(chunk):
        for part in range(2):
            tops = stats[chunk, :, part, :]
            top = jnp.max(tops, axis=0, keepdims=True)
            exp_sum = jnp.sum(stats[chunk, :, 2 + part, :] * jnp.exp(tops - top), axis=0, keepdims=True)
            norm[part:part + 1, :] = top
            norm[2 + part:3 + part, :] = 1.0 / exp_sum
            loss_ref[part:part + 1, :] += top + jnp.log(exp_sum)

    def table_half(chunk, which):
        slot = lax.rem(chunk, 2)
        zc = zbuf[chunk].reshape(2 * half, dim)
        for tile in range(which * tiles // 2, (which + 1) * tiles // 2):
            rows = slice(tile * VOCAB_TILE, (tile + 1) * VOCAB_TILE)
            for part in range(2):
                lanes = slice(part * half, (part + 1) * half)
                probs = jnp.exp(lbuf[slot, rows, lanes] - norm[part:part + 1, :]) * norm[2 + part:3 + part, :]
                hot = row_ids == label_row(chunk, part) - tile * VOCAB_TILE
                gbuf[rows, lanes] = jnp.where(hot, probs - 1.0, probs).astype(jnp.bfloat16)
            dtable_ref[rows, :] += jnp.dot(gbuf[rows, :], zc, preferred_element_type=jnp.float32)

    def token_half(chunk, part):
        dz = lax.dot_general(gbuf[:, part * half:(part + 1) * half], table_ref[...], ROWS_DIMS, preferred_element_type=jnp.float32)
        dzbuf[lax.rem(chunk, 3), part] = dz.reshape(2, 2, 2, UNIT, dim)

    start(gather_copies(0, 1))
    start(gather_copies(1, 1))
    start(gather_copies(2, 1))
    for chunk in range(3):
        finish(gather_copies(chunk, 1))
        start(gather_copies(chunk, 2))
    for chunk in range(2):
        finish(gather_copies(chunk, 2))
        start(gather_copies(chunk, 3))
    finish(gather_copies(0, 3))
    start(gather_copies(0, 4))
    finish(gather_copies(0, 4))

    def body(i, carry):
        def inside(offset, action):
            chunk = i + offset
            pl.when((chunk >= 0) & (chunk < chunks))(lambda: action(jnp.clip(chunk, 0, chunks - 1)))

        def step_reduce(phase, follow):
            def action(chunk):
                finish(reduce_copies(chunk, phase))
                reduce_add(chunk, phase)
                if follow:
                    start(reduce_copies(chunk, phase + 1))
            return action

        def step_gather(phase):
            def action(chunk):
                finish(gather_copies(chunk, phase))
                start(gather_copies(chunk, phase + 1))
            return action

        inside(-4, step_reduce(2, True))
        inside(-2, lambda chunk: start(reduce_copies(chunk, 0)))
        inside(1, step_gather(3))
        inside(3, lambda chunk: start(gather_copies(chunk, 1)))
        inside(2, step_gather(2))

        @pl.when(i < chunks)
        def _():
            forward_half(i, 0)
            forward_half(i, 1)

        inside(-2, step_reduce(0, False))
        inside(-3, step_reduce(1, True))
        inside(-4, step_reduce(3, False))
        inside(3, step_gather(1))
        inside(1, lambda chunk: finish(gather_copies(chunk, 4)))
        inside(-2, lambda chunk: start(reduce_copies(chunk, 1)))
        inside(0, lambda chunk: start(stat_copies(chunk)))

        @pl.when(i == chunks - 1)
        def _():
            start(lab_copies())

        def backward(chunk):
            finish(stat_copies(chunk))
            combine(chunk)
            table_half(chunk, 0)
            table_half(chunk, 1)
            token_half(chunk, 0)
            token_half(chunk, 1)

        inside(-1, backward)
        return carry

    lax.fori_loop(0, chunks + 4, body, 0)
    finish(lab_copies())
    loss_ref[2:3, :] = -jnp.sum(labs[...], axis=0)


def head(z_local, table_padded, lab_rows, vocab_rows):
    tokens, dim = z_local.shape
    chunks = tokens // UNIT
    padded = table_padded.shape[0]
    chunk_tokens = 16 * UNIT
    part_cols = dim // PARTS
    f32, bf16 = jnp.float32, jnp.bfloat16
    sems = pltpu.SemaphoreType.DMA
    vmem = pl.BlockSpec(memory_space=pltpu.VMEM)
    cost = 6 * tokens * 16 * padded * dim
    return pl.pallas_call(
        functools.partial(head_kernel, vocab_rows, chunks),
        in_specs=[pl.BlockSpec(memory_space=pl.ANY), vmem, vmem],
        out_specs=[vmem, vmem, vmem],
        out_shape=[jax.ShapeDtypeStruct((tokens, dim), f32),
                   jax.ShapeDtypeStruct((padded, dim), f32),
                   jax.ShapeDtypeStruct((3, 8 * UNIT), f32)],
        scratch_shapes=[pltpu.VMEM((chunks, 2, 2, 2, 2, UNIT, dim), bf16),
                        pltpu.VMEM((2, padded, chunk_tokens), f32),
                        pltpu.VMEM((padded, chunk_tokens), bf16),
                        pltpu.VMEM((3, 2, 2, 2, 2, UNIT, dim), f32),
                        pltpu.VMEM((2, 2, 2, 2, UNIT, dim), f32),
                        pltpu.VMEM((2, PARTS, 2, 2, UNIT, part_cols), f32),
                        pltpu.VMEM((2, PARTS, 2, UNIT, part_cols), f32),
                        pltpu.VMEM((2, PARTS, UNIT, part_cols), f32),
                        pltpu.VMEM((chunks, 16, STAT_ROWS, 8 * UNIT), f32),
                        pltpu.VMEM((16, 1, 8 * UNIT), f32),
                        pltpu.VMEM((8, 8 * UNIT), f32),
                        sems(()),
                        sems((chunks, 10)), sems((chunks, 10)),
                        sems((chunks, 10)), sems((chunks, 10)),
                        sems((chunks, 16)), sems((chunks, 16)),
                        sems((16,)), sems((16,))],
        compiler_params=pltpu.CompilerParams(vmem_limit_bytes=67043328, collective_id=1, has_side_effects=True),
        cost_estimate=pl.CostEstimate(flops=cost, bytes_accessed=4 * padded * dim, transcendentals=2 * tokens * 16 * padded),
        name="head_all",
    )(z_local.reshape(chunks, UNIT, dim), table_padded, lab_rows)


def split3(values):
    high = lax.reduce_precision(values, 8, 7)
    rest = values - high
    mid = lax.reduce_precision(rest, 8, 7)
    low = rest - mid
    return [part.astype(jnp.bfloat16) for part in (high, mid, low)]


def pick_rows(select, values):
    total = None
    for part in split3(values):
        term = jnp.dot(select, part, preferred_element_type=jnp.float32)
        total = term if total is None else total + term
    return total


def solution(mesh):
    groups = mesh.shape['fsdp']

    def device_step(token_ids, labels, table_shard, gate_shard, up_shard, down_shard, gain_in, gain_out):
        micro_count = token_ids.shape[0]
        tok_micro = token_ids.shape[1] * token_ids.shape[2]
        tok_dev = micro_count * tok_micro
        total_tokens = tok_dev * groups
        rows, dim = table_shard.shape
        me = lax.axis_index('fsdp')

        packed = jnp.stack([token_ids.reshape(tok_dev), labels.reshape(tok_dev)])
        packed_all = lax.all_gather(packed, 'fsdp', axis=0, tiled=False)
        ids_all = packed_all[:, 0]

        gate_rows, ffn = gate_shard.shape
        down_rows = down_shard.shape[0]
        w_all = lax.all_gather(jnp.concatenate([gate_shard, up_shard, down_shard.reshape(gate_rows, ffn)], axis=0), 'fsdp', axis=0, tiled=False)
        w_gate = w_all[:, :gate_rows].reshape(groups * gate_rows, ffn)
        w_up = w_all[:, gate_rows:2 * gate_rows].reshape(groups * gate_rows, ffn)
        w_down = w_all[:, 2 * gate_rows:].reshape(groups, down_rows, dim).reshape(groups * down_rows, dim)

        owner = ids_all // rows
        local = ids_all - owner * rows
        owner_hot = owner[:, :, None] == jnp.arange(groups, dtype=jnp.int32)
        tri = jnp.tril(jnp.ones((tok_dev, tok_dev), jnp.bfloat16), -1)
        before = jnp.einsum('tu,suo->sto', tri, owner_hot.astype(jnp.bfloat16), preferred_element_type=jnp.float32)
        rank = jnp.sum(jnp.where(owner_hot, before, 0.0), axis=-1).astype(jnp.int32)
        rounds = jnp.max(rank) // SLOTS + 1
        my_owner = lax.dynamic_index_in_dim(owner, me, 0, keepdims=False)
        my_rank = lax.dynamic_index_in_dim(rank, me, 0, keepdims=False)
        owned = owner == me
        slot_ids = jnp.arange(SLOTS, dtype=jnp.int32)

        def owned_rows(round_idx):
            hit = owned[:, None, :] & (rank[:, None, :] == slot_ids[None, :, None] + round_idx * SLOTS)
            return (jnp.sum(jnp.where(hit, local[:, None, :] + 1, 0), axis=-1) - 1).reshape(groups * SLOTS)

        def my_slots(round_idx):
            off = my_rank - round_idx * SLOTS
            return jnp.where((off >= 0) & (off < SLOTS), my_owner * SLOTS + off, -1)

        def fetch_round(round_idx):
            row_idx = owned_rows(round_idx)
            select = (row_idx[:, None] == jnp.arange(rows, dtype=jnp.int32)[None, :]).astype(jnp.bfloat16)
            send = jnp.dot(select, table_shard, preferred_element_type=jnp.float32).astype(jnp.bfloat16)
            got = lax.all_to_all(send.reshape(groups, SLOTS, dim), 'fsdp', 0, 0).reshape(groups * SLOTS, dim)
            place = (my_slots(round_idx)[:, None] == jnp.arange(groups * SLOTS, dtype=jnp.int32)[None, :]).astype(jnp.bfloat16)
            return jnp.dot(place, got, preferred_element_type=jnp.float32).astype(jnp.bfloat16)

        def return_round(round_idx, grad_rows):
            place = (jnp.arange(groups * SLOTS, dtype=jnp.int32)[:, None] == my_slots(round_idx)[None, :]).astype(jnp.bfloat16)
            send = pick_rows(place, grad_rows)
            got = lax.all_to_all(send.reshape(groups, SLOTS, dim), 'fsdp', 0, 0).reshape(groups * SLOTS, dim)
            select = (jnp.arange(rows, dtype=jnp.int32)[:, None] == owned_rows(round_idx)[None, :]).astype(jnp.bfloat16)
            return pick_rows(select, got)

        emb_rows = fetch_round(jnp.int32(0))
        emb_rows = lax.fori_loop(1, rounds, lambda r, acc: acc + fetch_round(r), emb_rows)

        normed, saved = [], []
        for m in range(micro_count):
            out, kept = mlp_forward(emb_rows[m * tok_micro:(m + 1) * tok_micro], gain_in, gain_out, w_gate, w_up, w_down)
            normed.append(out)
            saved.append(kept)

        chunks = tok_dev // UNIT
        lab_rows = jnp.transpose(packed_all[:, 1].reshape(groups, chunks, UNIT), (1, 0, 2)).reshape(2 * chunks, groups * UNIT // 2)
        padded = -(-rows // VOCAB_TILE) * VOCAB_TILE
        table_padded = jnp.pad(table_shard, ((0, padded - rows), (0, 0)))
        dz, dtable, loss_rows = head(jnp.concatenate(normed, axis=0), table_padded, lab_rows, rows)
        dtable = dtable[:rows]
        loss_total = jnp.sum(loss_rows)
        grad_normed = [dz[m * tok_micro:(m + 1) * tok_micro] for m in range(micro_count)]

        backs = [mlp_backward(saved[m], grad_normed[m], gain_in, gain_out, w_gate, w_up, w_down) for m in range(micro_count)]
        grad_rows, grad_mid, grad_gate_pre, grad_up_proj = [jnp.concatenate(parts, axis=0) for parts in zip(*backs)]
        normed_in = jnp.concatenate([kept[1] for kept in saved], axis=0)
        acts = jnp.concatenate([kept[5] for kept in saved], axis=0)
        grad_down = lax.dot_general(acts, grad_mid, ROWS_DIMS, preferred_element_type=jnp.float32)
        grad_gate = lax.dot_general(normed_in, grad_gate_pre, ROWS_DIMS, preferred_element_type=jnp.float32)
        grad_up = lax.dot_general(normed_in, grad_up_proj, ROWS_DIMS, preferred_element_type=jnp.float32)
        w_grads = jnp.concatenate([grad_gate.reshape(groups, gate_rows, ffn), grad_up.reshape(groups, gate_rows, ffn),
                                   grad_down.reshape(groups, down_rows, dim).reshape(groups, gate_rows, ffn)], axis=1)
        w_grad = lax.psum_scatter(w_grads, 'fsdp', scatter_dimension=0, tiled=False)

        dtable = dtable + return_round(jnp.int32(0), grad_rows)
        dtable = lax.fori_loop(1, rounds, lambda r, acc: acc + return_round(r, grad_rows), dtable)
        return (loss_total / total_tokens, dtable, w_grad[:gate_rows], w_grad[gate_rows:2 * gate_rows],
                w_grad[2 * gate_rows:].reshape(down_rows, dim))

    row_spec = P('fsdp', None)
    tok_spec = P(None, 'fsdp', None)
    return jax.shard_map(device_step, mesh=mesh,
                         in_specs=(tok_spec, tok_spec, row_spec, row_spec, row_spec, row_spec, P(), P()),
                         out_specs=(P(), row_spec, row_spec, row_spec, row_spec), check_vma=False)
```

```python
import functools
import jax
import jax.numpy as jnp
from jax import lax
from jax.experimental import pallas as pl
from jax.experimental.pallas import tpu as pltpu
from jax.sharding import PartitionSpec as P

NORM_EPS = 1e-6
SLOTS = 64


def rms_scale(values, gain_vec):
    vals32 = values.astype(jnp.float32)
    inv_rms = lax.rsqrt(jnp.mean(vals32 * vals32, axis=-1, keepdims=True) + NORM_EPS)
    return (vals32 * inv_rms * gain_vec).astype(jnp.bfloat16), inv_rms


def rms_back(values, inv_rms, gain_vec, grad_out):
    vals32 = values.astype(jnp.float32)
    scaled = grad_out * gain_vec
    proj_mean = jnp.mean(scaled * vals32, axis=-1, keepdims=True)
    return inv_rms * scaled - vals32 * (inv_rms * inv_rms * inv_rms) * proj_mean


def mlp_forward(emb_rows, gain_in, gain_out, w_gate, w_up, w_down):
    normed_in, inv_in = rms_scale(emb_rows, gain_in)
    gate_pre = jnp.dot(normed_in, w_gate, preferred_element_type=jnp.float32).astype(jnp.bfloat16)
    up_proj = jnp.dot(normed_in, w_up, preferred_element_type=jnp.float32).astype(jnp.bfloat16)
    acts = (jax.nn.silu(gate_pre.astype(jnp.float32)) * up_proj.astype(jnp.float32)).astype(jnp.bfloat16)
    mlp_out = jnp.dot(acts, w_down, preferred_element_type=jnp.float32).astype(jnp.bfloat16)
    hidden = (emb_rows.astype(jnp.float32) + mlp_out.astype(jnp.float32)).astype(jnp.bfloat16)
    normed_out, inv_out = rms_scale(hidden, gain_out)
    return normed_out, (emb_rows, normed_in, inv_in, gate_pre, up_proj, acts, hidden, inv_out)


COLS_DIMS = (((1,), (1,)), ((), ()))
ROWS_DIMS = (((0,), (0,)), ((), ()))


def mlp_backward(saved, grad_normed, gain_in, gain_out, w_gate, w_up, w_down):
    emb_rows, normed_in, inv_in, gate_pre, up_proj, acts, hidden, inv_out = saved
    grad_hidden = rms_back(hidden, inv_out, gain_out, grad_normed)
    grad_mid = grad_hidden.astype(jnp.bfloat16)
    grad_acts = lax.dot_general(grad_mid, w_down, COLS_DIMS, preferred_element_type=jnp.float32)
    gate32 = gate_pre.astype(jnp.float32)
    gate_sig = jax.nn.sigmoid(gate32)
    grad_gate_pre = (grad_acts * up_proj.astype(jnp.float32) * gate_sig * (1.0 + gate32 * (1.0 - gate_sig))).astype(jnp.bfloat16)
    grad_up_proj = (grad_acts * gate32 * gate_sig).astype(jnp.bfloat16)
    grad_normed_in = (lax.dot_general(grad_gate_pre, w_gate, COLS_DIMS, preferred_element_type=jnp.float32)
                      + lax.dot_general(grad_up_proj, w_up, COLS_DIMS, preferred_element_type=jnp.float32))
    grad_rows = grad_hidden + rms_back(emb_rows, inv_in, gain_in, grad_normed_in)
    return grad_rows, grad_mid, grad_gate_pre, grad_up_proj


UNIT = 64
CUBE_BITS = 3
PARTS = 3
VOCAB_TILE = 256
STAT_ROWS = 4
MESH_ID = pl.DeviceIdType.MESH
PAD_LOGIT = -1e30


def head_kernel(vocab_rows, chunks, z_hbm, table_ref, lab_ref, dz_ref, dtable_ref, loss_ref,
                zbuf, lbuf, gbuf, dzbuf, got_core, got_one, got_two, got_three, stats, labs, norm,
                local_sem, ag_send, ag_recv, rs_send, rs_recv, st_send, st_recv, lab_send, lab_recv):
    me = lax.axis_index('fsdp')
    total = 16
    core = lax.rem(me, 2)
    pos = [lax.rem(me // 2, 2), lax.rem(me // 4, 2), me // 8]
    base = me * vocab_rows
    padded, dim = table_ref.shape
    part_cols = dim // PARTS
    half = 8 * UNIT
    tiles = padded // VOCAB_TILE

    def peer(axis):
        return me + (1 - 2 * pos[axis]) * (2 << axis)

    core_peer = me + 1 - 2 * core

    barrier = pltpu.get_barrier_semaphore()
    for step in range(1, total):
        pl.semaphore_signal(barrier, inc=1, device_id=(lax.rem(me + step, total),), device_id_type=MESH_ID)
    own = pltpu.make_async_copy(z_hbm, zbuf.at[:, pos[2], pos[1], pos[0], core], local_sem)
    own.start()
    dtable_ref[...] = jnp.zeros_like(dtable_ref)
    loss_ref[...] = jnp.zeros_like(loss_ref)
    labs[me] = jnp.zeros((1, half), jnp.float32)
    own.wait()
    pl.semaphore_wait(barrier, total - 1)

    def where(choice):
        return choice.get(2, slice(None)), choice.get(1, slice(None)), choice.get(0, slice(None))

    def axes(part):
        return part % 3, (part + 1) % 3, (part + 2) % 3

    def cols(part):
        return pl.ds(part * part_cols, part_cols)

    def gather_copies(chunk, phase):
        if phase == 4:
            here = zbuf.at[chunk, :, :, :, core]
            return [pltpu.make_async_remote_copy(here, here, ag_send.at[chunk, 9], ag_recv.at[chunk, 9],
                                                 device_id=(core_peer,), device_id_type=MESH_ID)]
        copies = []
        for part in range(PARTS):
            order = axes(part)
            fixed = {axis: pos[axis] for axis in order[phase - 1:]}
            iz, iy, ix = where(fixed)
            here = zbuf.at[chunk, iz, iy, ix, core, :, cols(part)]
            sem = (phase - 1) * PARTS + part
            copies.append(pltpu.make_async_remote_copy(here, here, ag_send.at[chunk, sem], ag_recv.at[chunk, sem],
                                                       device_id=(peer(order[phase - 1]),), device_id_type=MESH_ID))
        return copies

    def reduce_copies(chunk, phase):
        slot, dzs = lax.rem(chunk, 2), lax.rem(chunk, 3)
        if phase == 0:
            return [pltpu.make_async_remote_copy(dzbuf.at[dzs, :, :, :, 1 - core], got_core.at[slot], rs_send.at[chunk, 9], rs_recv.at[chunk, 9],
                                                 device_id=(core_peer,), device_id_type=MESH_ID)]
        copies = []
        for part in range(PARTS):
            order = axes(part)
            fixed = {axis: pos[axis] for axis in order[:phase - 1]}
            fixed[order[phase - 1]] = 1 - pos[order[phase - 1]]
            iz, iy, ix = where(fixed)
            got = (got_one, got_two, got_three)[phase - 1]
            sem = (phase - 1) * PARTS + part
            copies.append(pltpu.make_async_remote_copy(dzbuf.at[dzs, iz, iy, ix, core, :, cols(part)], got.at[slot, part],
                                                       rs_send.at[chunk, sem], rs_recv.at[chunk, sem],
                                                       device_id=(peer(order[phase - 1]),), device_id_type=MESH_ID))
        return copies

    def start(copies):
        for copy in copies:
            copy.start()

    def finish(copies):
        for copy in copies:
            copy.wait()

    def reduce_add(chunk, phase):
        slot, dzs = lax.rem(chunk, 2), lax.rem(chunk, 3)
        if phase == 0:
            dzbuf[dzs, :, :, :, core] += got_core[slot]
            return
        for part in range(PARTS):
            order = axes(part)
            iz, iy, ix = where({axis: pos[axis] for axis in order[:phase]})
            got = (got_one, got_two, got_three)[phase - 1]
            lanes = slice(part * part_cols, (part + 1) * part_cols)
            if phase == 3:
                rows = pl.ds(pl.multiple_of(chunk * UNIT, UNIT), UNIT)
                dz_ref[rows, lanes] = dzbuf[dzs, iz, iy, ix, core, :, lanes] + got[slot, part]
            else:
                dzbuf[dzs, iz, iy, ix, core, :, lanes] += got[slot, part]

    def stat_copies(chunk):
        copies = []
        for step in range(1, total):
            to = lax.rem(me + step, total)
            copies.append(pltpu.make_async_remote_copy(stats.at[chunk, me], stats.at[chunk, me], st_send.at[chunk, step], st_recv.at[chunk, step],
                                                       device_id=(to,), device_id_type=MESH_ID))
        return copies

    def lab_copies():
        return [pltpu.make_async_remote_copy(labs.at[me], labs.at[me], lab_send.at[step], lab_recv.at[step],
                                             device_id=(lax.rem(me + step, total),), device_id_type=MESH_ID) for step in range(1, total)]

    def label_row(chunk, part):
        lab = lab_ref[pl.ds(chunk * 2 + part, 1), :] - base
        return jnp.where(lab < vocab_rows, lab, -1)

    row_ids = lax.broadcasted_iota(jnp.int32, (VOCAB_TILE, half), 0)

    def forward_half(chunk, part):
        slot = lax.rem(chunk, 2)
        zb = zbuf[chunk, part].reshape(half, dim)
        lab = label_row(chunk, part)
        tops, sums, hits = [], [], []
        for tile in range(tiles):
            rows = slice(tile * VOCAB_TILE, (tile + 1) * VOCAB_TILE)
            logits = lax.dot_general(table_ref[rows, :], zb, COLS_DIMS, preferred_element_type=jnp.float32)
            if (tile + 1) * VOCAB_TILE > vocab_rows:
                logits = jnp.where(row_ids < vocab_rows - tile * VOCAB_TILE, logits, PAD_LOGIT)
            lbuf[slot, rows, part * half:(part + 1) * half] = logits
            top = jnp.max(logits, axis=0, keepdims=True)
            tops.append(top)
            sums.append(jnp.sum(jnp.exp(logits - top), axis=0, keepdims=True))
            hits.append(jnp.sum(jnp.where(row_ids == lab - tile * VOCAB_TILE, logits, 0.0), axis=0, keepdims=True))
        top = functools.reduce(jnp.maximum, tops)
        exp_sum = sum(s * jnp.exp(t - top) for s, t in zip(sums, tops))
        stats[chunk, me, part:part + 1, :] = top
        stats[chunk, me, 2 + part:3 + part, :] = exp_sum
        labs[me] += sum(hits)

    def combine(chunk):
        for part in range(2):
            tops = stats[chunk, :, part, :]
            top = jnp.max(tops, axis=0, keepdims=True)
            exp_sum = jnp.sum(stats[chunk, :, 2 + part, :] * jnp.exp(tops - top), axis=0, keepdims=True)
            norm[part:part + 1, :] = top
            norm[2 + part:3 + part, :] = 1.0 / exp_sum
            loss_ref[part:part + 1, :] += top + jnp.log(exp_sum)

    def table_half(chunk, which):
        slot = lax.rem(chunk, 2)
        zc = zbuf[chunk].reshape(2 * half, dim)
        for tile in range(which * tiles // 2, (which + 1) * tiles // 2):
            rows = slice(tile * VOCAB_TILE, (tile + 1) * VOCAB_TILE)
            for part in range(2):
                lanes = slice(part * half, (part + 1) * half)
                probs = jnp.exp(lbuf[slot, rows, lanes] - norm[part:part + 1, :]) * norm[2 + part:3 + part, :]
                hot = row_ids == label_row(chunk, part) - tile * VOCAB_TILE
                gbuf[rows, lanes] = jnp.where(hot, probs - 1.0, probs).astype(jnp.bfloat16)
            dtable_ref[rows, :] += jnp.dot(gbuf[rows, :], zc, preferred_element_type=jnp.float32)

    def token_half(chunk, part):
        dz = lax.dot_general(gbuf[:, part * half:(part + 1) * half], table_ref[...], ROWS_DIMS, preferred_element_type=jnp.float32)
        dzbuf[lax.rem(chunk, 3), part] = dz.reshape(2, 2, 2, UNIT, dim)

    start(gather_copies(0, 1))
    start(gather_copies(1, 1))
    start(gather_copies(2, 1))
    for chunk in range(3):
        finish(gather_copies(chunk, 1))
        start(gather_copies(chunk, 2))
    for chunk in range(2):
        finish(gather_copies(chunk, 2))
        start(gather_copies(chunk, 3))
    finish(gather_copies(0, 3))
    start(gather_copies(0, 4))
    finish(gather_copies(0, 4))

    def body(i, carry):
        def inside(offset, action):
            chunk = i + offset
            pl.when((chunk >= 0) & (chunk < chunks))(lambda: action(jnp.clip(chunk, 0, chunks - 1)))

        def step_reduce(phase, follow):
            def action(chunk):
                finish(reduce_copies(chunk, phase))
                reduce_add(chunk, phase)
                if follow:
                    start(reduce_copies(chunk, phase + 1))
            return action

        def step_gather(phase):
            def action(chunk):
                finish(gather_copies(chunk, phase))
                start(gather_copies(chunk, phase + 1))
            return action

        inside(-4, step_reduce(2, True))
        inside(-2, lambda chunk: start(reduce_copies(chunk, 0)))
        inside(1, step_gather(3))
        inside(3, lambda chunk: start(gather_copies(chunk, 1)))
        inside(2, step_gather(2))

        @pl.when(i < chunks)
        def _():
            forward_half(i, 0)
            forward_half(i, 1)

        inside(-2, step_reduce(0, False))
        inside(-3, step_reduce(1, True))
        inside(-4, step_reduce(3, False))
        inside(3, step_gather(1))
        inside(1, lambda chunk: finish(gather_copies(chunk, 4)))
        inside(-2, lambda chunk: start(reduce_copies(chunk, 1)))
        inside(0, lambda chunk: start(stat_copies(chunk)))

        @pl.when(i == chunks - 1)
        def _():
            start(lab_copies())

        def backward(chunk):
            finish(stat_copies(chunk))
            combine(chunk)
            table_half(chunk, 0)
            table_half(chunk, 1)
            token_half(chunk, 0)
            token_half(chunk, 1)

        inside(-1, backward)
        return carry

    lax.fori_loop(0, chunks + 4, body, 0)
    finish(lab_copies())
    loss_ref[2:3, :] = -jnp.sum(labs[...], axis=0)


def head(z_local, table_padded, lab_rows, vocab_rows):
    tokens, dim = z_local.shape
    chunks = tokens // UNIT
    padded = table_padded.shape[0]
    chunk_tokens = 16 * UNIT
    part_cols = dim // PARTS
    f32, bf16 = jnp.float32, jnp.bfloat16
    sems = pltpu.SemaphoreType.DMA
    vmem = pl.BlockSpec(memory_space=pltpu.VMEM)
    cost = 6 * tokens * 16 * padded * dim
    return pl.pallas_call(
        functools.partial(head_kernel, vocab_rows, chunks),
        in_specs=[pl.BlockSpec(memory_space=pl.ANY), vmem, vmem],
        out_specs=[vmem, vmem, vmem],
        out_shape=[jax.ShapeDtypeStruct((tokens, dim), f32),
                   jax.ShapeDtypeStruct((padded, dim), f32),
                   jax.ShapeDtypeStruct((3, 8 * UNIT), f32)],
        scratch_shapes=[pltpu.VMEM((chunks, 2, 2, 2, 2, UNIT, dim), bf16),
                        pltpu.VMEM((2, padded, chunk_tokens), f32),
                        pltpu.VMEM((padded, chunk_tokens), bf16),
                        pltpu.VMEM((3, 2, 2, 2, 2, UNIT, dim), f32),
                        pltpu.VMEM((2, 2, 2, 2, UNIT, dim), f32),
                        pltpu.VMEM((2, PARTS, 2, 2, UNIT, part_cols), f32),
                        pltpu.VMEM((2, PARTS, 2, UNIT, part_cols), f32),
                        pltpu.VMEM((2, PARTS, UNIT, part_cols), f32),
                        pltpu.VMEM((chunks, 16, STAT_ROWS, 8 * UNIT), f32),
                        pltpu.VMEM((16, 1, 8 * UNIT), f32),
                        pltpu.VMEM((8, 8 * UNIT), f32),
                        sems(()),
                        sems((chunks, 10)), sems((chunks, 10)),
                        sems((chunks, 10)), sems((chunks, 10)),
                        sems((chunks, 16)), sems((chunks, 16)),
                        sems((16,)), sems((16,))],
        compiler_params=pltpu.CompilerParams(vmem_limit_bytes=67043328, collective_id=1, has_side_effects=True),
        cost_estimate=pl.CostEstimate(flops=cost, bytes_accessed=4 * padded * dim, transcendentals=2 * tokens * 16 * padded),
        name="head_all",
    )(z_local.reshape(chunks, UNIT, dim), table_padded, lab_rows)


PIECES = 4


def axes(part):
    return part % 3, (part + 1) % 3, (part + 2) % 3


def cube_index(choice):
    return choice.get(2, slice(None)), choice.get(1, slice(None)), choice.get(0, slice(None))


def tail_kernel(table_rows, gate_hbm, up_hbm, down_hbm, send_hbm, row_ref, dtable_hbm, gate_out, up_out, down_out, dtable_out,
                acc_g, acc_u, acc_d, core_g, core_u, core_d, one_g, one_u, one_d, two_g, two_u, two_d, three_g, three_u, three_d,
                rows_got, split, local_sem, send_sem, recv_sem, row_send, row_recv):
    me = lax.axis_index('fsdp')
    total = 16
    core = lax.rem(me, 2)
    pos = [lax.rem(me // 2, 2), lax.rem(me // 4, 2), me // 8]
    core_peer = me + 1 - 2 * core
    whole = (gate_hbm, up_hbm, down_hbm)
    accs = (acc_g, acc_u, acc_d)
    gots = ((core_g, core_u, core_d), (one_g, one_u, one_d), (two_g, two_u, two_d), (three_g, three_u, three_d))
    outs = (gate_out, up_out, down_out)

    barrier = pltpu.get_barrier_semaphore()
    for step in range(1, total):
        pl.semaphore_signal(barrier, inc=1, device_id=(lax.rem(me + step, total),), device_id_type=MESH_ID)
    loads = [pltpu.make_async_copy(whole[part].at[:, :, :, core], accs[part], local_sem.at[part]) for part in range(3)]
    loads.append(pltpu.make_async_copy(dtable_hbm.at[pl.ds(0, table_rows)], dtable_out, local_sem.at[3]))
    loads.append(pltpu.make_async_copy(send_hbm.at[me], rows_got.at[me], local_sem.at[4]))
    for load in loads:
        load.start()
    pl.semaphore_wait(barrier, total - 1)

    def piece(part, q):
        if part == 2:
            size = acc_d.shape[3] // PIECES
            return pl.ds(q * size, size), slice(None)
        size = acc_g.shape[4] // PIECES
        return slice(None), pl.ds(q * size, size)

    def copies(phase, q):
        made = []
        for part in range(3):
            rows, lanes = piece(part, q)
            order = axes(part)
            if phase == 0:
                src = whole[part].at[:, :, :, 1 - core, rows, lanes]
                dst = gots[0][part].at[:, :, :, rows, lanes]
                to = core_peer
            else:
                fixed = {axis: pos[axis] for axis in order[:phase - 1]}
                fixed[order[phase - 1]] = 1 - pos[order[phase - 1]]
                iz, iy, ix = cube_index(fixed)
                src = accs[part].at[iz, iy, ix, rows, lanes]
                lead = (slice(None),) * (3 - phase)
                dst = gots[phase][part].at[lead + (rows, lanes)]
                axis = order[phase - 1]
                to = me + (1 - 2 * pos[axis]) * (2 << axis)
            made.append(pltpu.make_async_remote_copy(src, dst, send_sem.at[phase, part, q], recv_sem.at[phase, part, q],
                                                     device_id=(to,), device_id_type=MESH_ID))
        return made

    def start(made):
        for copy in made:
            copy.start()

    def finish_add(phase, q):
        for copy in copies(phase, q):
            copy.wait()
        for part in range(3):
            rows, lanes = piece(part, q)
            iz, iy, ix = cube_index({axis: pos[axis] for axis in axes(part)[:phase]})
            got = gots[phase][part][(slice(None),) * (3 - phase) + (rows, lanes)]
            if phase == 3:
                outs[part][rows, lanes] = accs[part][iz, iy, ix, rows, lanes] + got
            else:
                accs[part][iz, iy, ix, rows, lanes] += got

    row_copies = []
    for step in range(1, total):
        to = lax.rem(me + step, total)
        row_copies.append(pltpu.make_async_remote_copy(send_hbm.at[to], rows_got.at[me], row_send.at[step], row_recv.at[step],
                                                       device_id=(to,), device_id_type=MESH_ID))
    for q in range(PIECES):
        start(copies(0, q))
    start(row_copies)
    for load in loads:
        load.wait()
    for q in range(PIECES):
        finish_add(0, q)
        start(copies(1, q))
    for copy in row_copies:
        copy.wait()
    slots, dim = rows_got.shape[0] * rows_got.shape[1], rows_got.shape[2]

    def split_rows(s, carry):
        vals = rows_got[s]
        at = pl.multiple_of(s * SLOTS, SLOTS)
        high = vals.astype(jnp.bfloat16)
        rest = vals - high.astype(jnp.float32)
        mid = rest.astype(jnp.bfloat16)
        split[pl.ds(at, SLOTS), :] = high
        split[pl.ds(slots + at, SLOTS), :] = mid
        split[pl.ds(2 * slots + at, SLOTS), :] = (rest - mid.astype(jnp.float32)).astype(jnp.bfloat16)
        return carry

    lax.fori_loop(0, total, split_rows, 0)

    def add_rows(first, count):
        ids = lax.broadcasted_iota(jnp.int32, (count, slots), 0) + first
        hot = jnp.where(ids == row_ref[...], 1.0, 0.0).astype(jnp.bfloat16)
        dtable_out[pl.ds(first, count), :] += jnp.dot(jnp.concatenate([hot, hot, hot], axis=1), split[...], preferred_element_type=jnp.float32)

    full = table_rows // VOCAB_TILE

    def add_tile(tile, carry):
        add_rows(pl.multiple_of(tile * VOCAB_TILE, VOCAB_TILE), VOCAB_TILE)
        return carry

    lax.fori_loop(0, full, add_tile, 0)
    if table_rows % VOCAB_TILE:
        add_rows(full * VOCAB_TILE, table_rows % VOCAB_TILE)

    for q in range(PIECES + 2):
        if q < PIECES:
            finish_add(1, q)
            start(copies(2, q))
        if 1 <= q <= PIECES:
            finish_add(2, q - 1)
            start(copies(3, q - 1))
        if q >= 2:
            finish_add(3, q - 2)


def tail(grad_gate, grad_up, grad_down, send, row_idx, dtable, table_rows):
    f32 = jnp.float32
    vmem = pl.BlockSpec(memory_space=pltpu.VMEM)
    anywhere = pl.BlockSpec(memory_space=pl.ANY)
    sems = pltpu.SemaphoreType.DMA
    blocks = [tuple(array.shape[4:]) for array in (grad_gate, grad_up, grad_down)]
    scratch = [pltpu.VMEM(lead + block, f32) for lead in ((2, 2, 2), (2, 2, 2), (2, 2), (2,), ()) for block in blocks]
    slots = send.shape[0] * send.shape[1]
    dim = send.shape[2]
    return pl.pallas_call(
        functools.partial(tail_kernel, table_rows),
        in_specs=[anywhere, anywhere, anywhere, anywhere, vmem, anywhere],
        out_specs=[vmem] * 4,
        out_shape=[jax.ShapeDtypeStruct(block, f32) for block in blocks] + [jax.ShapeDtypeStruct((table_rows, dim), f32)],
        scratch_shapes=scratch + [pltpu.VMEM(send.shape, f32), pltpu.VMEM((3 * slots, dim), jnp.bfloat16),
                                  sems((5,)), sems((4, 3, PIECES)), sems((4, 3, PIECES)), sems((16,)), sems((16,))],
        compiler_params=pltpu.CompilerParams(vmem_limit_bytes=60 * 1024 * 1024, collective_id=2, has_side_effects=True),
        cost_estimate=pl.CostEstimate(flops=6 * slots * table_rows * dim, bytes_accessed=40 * 1024 * 1024, transcendentals=0),
        name="tail_all",
    )(grad_gate, grad_up, grad_down, send, row_idx, dtable)


def split3(values):
    high = lax.reduce_precision(values, 8, 7)
    rest = values - high
    mid = lax.reduce_precision(rest, 8, 7)
    low = rest - mid
    return [part.astype(jnp.bfloat16) for part in (high, mid, low)]


def pick_rows(select, values):
    total = None
    for part in split3(values):
        term = jnp.dot(select, part, preferred_element_type=jnp.float32)
        total = term if total is None else total + term
    return total


def solution(mesh):
    groups = mesh.shape['fsdp']

    def device_step(token_ids, labels, table_shard, gate_shard, up_shard, down_shard, gain_in, gain_out):
        micro_count = token_ids.shape[0]
        tok_micro = token_ids.shape[1] * token_ids.shape[2]
        tok_dev = micro_count * tok_micro
        total_tokens = tok_dev * groups
        rows, dim = table_shard.shape
        me = lax.axis_index('fsdp')

        packed = jnp.stack([token_ids.reshape(tok_dev), labels.reshape(tok_dev)])
        packed_all = lax.all_gather(packed, 'fsdp', axis=0, tiled=False)
        ids_all = packed_all[:, 0]

        gate_rows, ffn = gate_shard.shape
        down_rows = down_shard.shape[0]
        w_all = lax.all_gather(jnp.concatenate([gate_shard, up_shard, down_shard.reshape(gate_rows, ffn)], axis=0), 'fsdp', axis=0, tiled=False)
        w_gate = w_all[:, :gate_rows].reshape(groups * gate_rows, ffn)
        w_up = w_all[:, gate_rows:2 * gate_rows].reshape(groups * gate_rows, ffn)
        w_down = w_all[:, 2 * gate_rows:].reshape(groups, down_rows, dim).reshape(groups * down_rows, dim)

        owner = ids_all // rows
        local = ids_all - owner * rows
        owner_hot = owner[:, :, None] == jnp.arange(groups, dtype=jnp.int32)
        tri = jnp.tril(jnp.ones((tok_dev, tok_dev), jnp.bfloat16), -1)
        before = jnp.einsum('tu,suo->sto', tri, owner_hot.astype(jnp.bfloat16), preferred_element_type=jnp.float32)
        rank = jnp.sum(jnp.where(owner_hot, before, 0.0), axis=-1).astype(jnp.int32)
        rounds = jnp.max(rank) // SLOTS + 1
        my_owner = lax.dynamic_index_in_dim(owner, me, 0, keepdims=False)
        my_rank = lax.dynamic_index_in_dim(rank, me, 0, keepdims=False)
        owned = owner == me
        slot_ids = jnp.arange(SLOTS, dtype=jnp.int32)

        def owned_rows(round_idx):
            hit = owned[:, None, :] & (rank[:, None, :] == slot_ids[None, :, None] + round_idx * SLOTS)
            return (jnp.sum(jnp.where(hit, local[:, None, :] + 1, 0), axis=-1) - 1).reshape(groups * SLOTS)

        def my_slots(round_idx):
            off = my_rank - round_idx * SLOTS
            return jnp.where((off >= 0) & (off < SLOTS), my_owner * SLOTS + off, -1)

        def fetch_round(round_idx):
            row_idx = owned_rows(round_idx)
            select = (row_idx[:, None] == jnp.arange(rows, dtype=jnp.int32)[None, :]).astype(jnp.bfloat16)
            send = jnp.dot(select, table_shard, preferred_element_type=jnp.float32).astype(jnp.bfloat16)
            got = lax.all_to_all(send.reshape(groups, SLOTS, dim), 'fsdp', 0, 0).reshape(groups * SLOTS, dim)
            place = (my_slots(round_idx)[:, None] == jnp.arange(groups * SLOTS, dtype=jnp.int32)[None, :]).astype(jnp.bfloat16)
            return jnp.dot(place, got, preferred_element_type=jnp.float32).astype(jnp.bfloat16)

        def slot_place(round_idx):
            return (jnp.arange(groups * SLOTS, dtype=jnp.int32)[:, None] == my_slots(round_idx)[None, :]).astype(jnp.bfloat16)

        def return_round(round_idx, grad_rows):
            send = pick_rows(slot_place(round_idx), grad_rows)
            got = lax.all_to_all(send.reshape(groups, SLOTS, dim), 'fsdp', 0, 0).reshape(groups * SLOTS, dim)
            select = (jnp.arange(rows, dtype=jnp.int32)[:, None] == owned_rows(round_idx)[None, :]).astype(jnp.bfloat16)
            return pick_rows(select, got)

        emb_rows = fetch_round(jnp.int32(0))
        emb_rows = lax.fori_loop(1, rounds, lambda r, acc: acc + fetch_round(r), emb_rows)

        normed, saved = [], []
        for m in range(micro_count):
            out, kept = mlp_forward(emb_rows[m * tok_micro:(m + 1) * tok_micro], gain_in, gain_out, w_gate, w_up, w_down)
            normed.append(out)
            saved.append(kept)

        chunks = tok_dev // UNIT
        lab_rows = jnp.transpose(packed_all[:, 1].reshape(groups, chunks, UNIT), (1, 0, 2)).reshape(2 * chunks, groups * UNIT // 2)
        padded = -(-rows // VOCAB_TILE) * VOCAB_TILE
        table_padded = jnp.pad(table_shard, ((0, padded - rows), (0, 0)))
        dz, dtable, loss_rows = head(jnp.concatenate(normed, axis=0), table_padded, lab_rows, rows)
        loss_total = jnp.sum(loss_rows)
        grad_normed = [dz[m * tok_micro:(m + 1) * tok_micro] for m in range(micro_count)]

        backs = [mlp_backward(saved[m], grad_normed[m], gain_in, gain_out, w_gate, w_up, w_down) for m in range(micro_count)]
        grad_rows, grad_mid, grad_gate_pre, grad_up_proj = [jnp.concatenate(parts, axis=0) for parts in zip(*backs)]
        normed_in = jnp.concatenate([kept[1] for kept in saved], axis=0)
        acts = jnp.concatenate([kept[5] for kept in saved], axis=0)
        grad_down = lax.dot_general(acts, grad_mid, ROWS_DIMS, preferred_element_type=jnp.float32)
        grad_gate = lax.dot_general(normed_in, grad_gate_pre, ROWS_DIMS, preferred_element_type=jnp.float32)
        grad_up = lax.dot_general(normed_in, grad_up_proj, ROWS_DIMS, preferred_element_type=jnp.float32)
        cube = (2, 2, 2, 2)
        send = pick_rows(slot_place(0), grad_rows).reshape(groups, SLOTS, dim)
        out_gate, out_up, out_down, dtable = tail(grad_gate.reshape(cube + (gate_rows, ffn)), grad_up.reshape(cube + (gate_rows, ffn)),
                                                  grad_down.reshape(cube + (down_rows, dim)), send, owned_rows(0).reshape(1, groups * SLOTS), dtable, rows)
        dtable = lax.fori_loop(1, rounds, lambda r, acc: acc + return_round(r, grad_rows), dtable)
        return (loss_total / total_tokens, dtable, out_gate, out_up, out_down)

    row_spec = P('fsdp', None)
    tok_spec = P(None, 'fsdp', None)
    return jax.shard_map(device_step, mesh=mesh,
                         in_specs=(tok_spec, tok_spec, row_spec, row_spec, row_spec, row_spec, P(), P()),
                         out_specs=(P(), row_spec, row_spec, row_spec, row_spec), check_vma=False)
```

```python
import functools
import jax
import jax.numpy as jnp
from jax import lax
from jax.experimental import pallas as pl
from jax.experimental.pallas import tpu as pltpu
from jax.sharding import PartitionSpec as P

NORM_EPS = 1e-6
SLOTS = 64


def rms_scale(values, gain_vec):
    vals32 = values.astype(jnp.float32)
    inv_rms = lax.rsqrt(jnp.mean(vals32 * vals32, axis=-1, keepdims=True) + NORM_EPS)
    return (vals32 * inv_rms * gain_vec).astype(jnp.bfloat16), inv_rms


def rms_back(values, inv_rms, gain_vec, grad_out):
    vals32 = values.astype(jnp.float32)
    scaled = grad_out * gain_vec
    proj_mean = jnp.mean(scaled * vals32, axis=-1, keepdims=True)
    return inv_rms * scaled - vals32 * (inv_rms * inv_rms * inv_rms) * proj_mean


def mlp_forward(emb_rows, gain_in, gain_out, w_gate, w_up, w_down):
    normed_in, inv_in = rms_scale(emb_rows, gain_in)
    gate_pre = jnp.dot(normed_in, w_gate, preferred_element_type=jnp.float32).astype(jnp.bfloat16)
    up_proj = jnp.dot(normed_in, w_up, preferred_element_type=jnp.float32).astype(jnp.bfloat16)
    acts = (jax.nn.silu(gate_pre.astype(jnp.float32)) * up_proj.astype(jnp.float32)).astype(jnp.bfloat16)
    mlp_out = jnp.dot(acts, w_down, preferred_element_type=jnp.float32).astype(jnp.bfloat16)
    hidden = (emb_rows.astype(jnp.float32) + mlp_out.astype(jnp.float32)).astype(jnp.bfloat16)
    normed_out, inv_out = rms_scale(hidden, gain_out)
    return normed_out, (emb_rows, normed_in, inv_in, gate_pre, up_proj, acts, hidden, inv_out)


COLS_DIMS = (((1,), (1,)), ((), ()))
ROWS_DIMS = (((0,), (0,)), ((), ()))


def mlp_backward(saved, grad_normed, gain_in, gain_out, w_gate, w_up, w_down):
    emb_rows, normed_in, inv_in, gate_pre, up_proj, acts, hidden, inv_out = saved
    grad_hidden = rms_back(hidden, inv_out, gain_out, grad_normed)
    grad_mid = grad_hidden.astype(jnp.bfloat16)
    grad_acts = lax.dot_general(grad_mid, w_down, COLS_DIMS, preferred_element_type=jnp.float32)
    gate32 = gate_pre.astype(jnp.float32)
    gate_sig = jax.nn.sigmoid(gate32)
    grad_gate_pre = (grad_acts * up_proj.astype(jnp.float32) * gate_sig * (1.0 + gate32 * (1.0 - gate_sig))).astype(jnp.bfloat16)
    grad_up_proj = (grad_acts * gate32 * gate_sig).astype(jnp.bfloat16)
    grad_normed_in = (lax.dot_general(grad_gate_pre, w_gate, COLS_DIMS, preferred_element_type=jnp.float32)
                      + lax.dot_general(grad_up_proj, w_up, COLS_DIMS, preferred_element_type=jnp.float32))
    grad_rows = grad_hidden + rms_back(emb_rows, inv_in, gain_in, grad_normed_in)
    return grad_rows, grad_mid, grad_gate_pre, grad_up_proj


UNIT = 64
CUBE_BITS = 3
PARTS = 3
VOCAB_TILE = 256
STAT_ROWS = 4
MESH_ID = pl.DeviceIdType.MESH
PAD_LOGIT = -1e30


def head_kernel(vocab_rows, chunks, z_hbm, table_ref, lab_ref, dz_ref, dtable_ref, loss_ref,
                zbuf, lbuf, gbuf, dzbuf, got_core, got_one, got_two, got_three, stats, labs, norm,
                local_sem, ag_send, ag_recv, rs_send, rs_recv, st_send, st_recv, lab_send, lab_recv):
    me = lax.axis_index('fsdp')
    total = 16
    core = lax.rem(me, 2)
    pos = [lax.rem(me // 2, 2), lax.rem(me // 4, 2), me // 8]
    base = me * vocab_rows
    padded, dim = table_ref.shape
    part_cols = dim // PARTS
    half = 8 * UNIT
    tiles = padded // VOCAB_TILE

    def peer(axis):
        return me + (1 - 2 * pos[axis]) * (2 << axis)

    core_peer = me + 1 - 2 * core

    barrier = pltpu.get_barrier_semaphore()
    for step in range(1, total):
        pl.semaphore_signal(barrier, inc=1, device_id=(lax.rem(me + step, total),), device_id_type=MESH_ID)
    own = pltpu.make_async_copy(z_hbm, zbuf.at[:, pos[2], pos[1], pos[0], core], local_sem)
    own.start()
    dtable_ref[...] = jnp.zeros_like(dtable_ref)
    loss_ref[...] = jnp.zeros_like(loss_ref)
    labs[me] = jnp.zeros((1, half), jnp.float32)
    own.wait()
    pl.semaphore_wait(barrier, total - 1)

    def where(choice):
        return choice.get(2, slice(None)), choice.get(1, slice(None)), choice.get(0, slice(None))

    def axes(part):
        return part % 3, (part + 1) % 3, (part + 2) % 3

    def cols(part):
        return pl.ds(part * part_cols, part_cols)

    def gather_copies(chunk, phase):
        if phase == 4:
            here = zbuf.at[chunk, :, :, :, core]
            return [pltpu.make_async_remote_copy(here, here, ag_send.at[chunk, 9], ag_recv.at[chunk, 9],
                                                 device_id=(core_peer,), device_id_type=MESH_ID)]
        copies = []
        for part in range(PARTS):
            order = axes(part)
            fixed = {axis: pos[axis] for axis in order[phase - 1:]}
            iz, iy, ix = where(fixed)
            here = zbuf.at[chunk, iz, iy, ix, core, :, cols(part)]
            sem = (phase - 1) * PARTS + part
            copies.append(pltpu.make_async_remote_copy(here, here, ag_send.at[chunk, sem], ag_recv.at[chunk, sem],
                                                       device_id=(peer(order[phase - 1]),), device_id_type=MESH_ID))
        return copies

    def reduce_copies(chunk, phase):
        slot, dzs = lax.rem(chunk, 2), lax.rem(chunk, 3)
        if phase == 0:
            return [pltpu.make_async_remote_copy(dzbuf.at[dzs, :, :, :, 1 - core], got_core.at[slot], rs_send.at[chunk, 9], rs_recv.at[chunk, 9],
                                                 device_id=(core_peer,), device_id_type=MESH_ID)]
        copies = []
        for part in range(PARTS):
            order = axes(part)
            fixed = {axis: pos[axis] for axis in order[:phase - 1]}
            fixed[order[phase - 1]] = 1 - pos[order[phase - 1]]
            iz, iy, ix = where(fixed)
            got = (got_one, got_two, got_three)[phase - 1]
            sem = (phase - 1) * PARTS + part
            copies.append(pltpu.make_async_remote_copy(dzbuf.at[dzs, iz, iy, ix, core, :, cols(part)], got.at[slot, part],
                                                       rs_send.at[chunk, sem], rs_recv.at[chunk, sem],
                                                       device_id=(peer(order[phase - 1]),), device_id_type=MESH_ID))
        return copies

    def start(copies):
        for copy in copies:
            copy.start()

    def finish(copies):
        for copy in copies:
            copy.wait()

    def reduce_add(chunk, phase):
        slot, dzs = lax.rem(chunk, 2), lax.rem(chunk, 3)
        if phase == 0:
            dzbuf[dzs, :, :, :, core] += got_core[slot]
            return
        for part in range(PARTS):
            order = axes(part)
            iz, iy, ix = where({axis: pos[axis] for axis in order[:phase]})
            got = (got_one, got_two, got_three)[phase - 1]
            lanes = slice(part * part_cols, (part + 1) * part_cols)
            if phase == 3:
                rows = pl.ds(pl.multiple_of(chunk * UNIT, UNIT), UNIT)
                dz_ref[rows, lanes] = dzbuf[dzs, iz, iy, ix, core, :, lanes] + got[slot, part]
            else:
                dzbuf[dzs, iz, iy, ix, core, :, lanes] += got[slot, part]

    def stat_copies(chunk):
        copies = []
        for step in range(1, total):
            to = lax.rem(me + step, total)
            copies.append(pltpu.make_async_remote_copy(stats.at[chunk, me], stats.at[chunk, me], st_send.at[chunk, step], st_recv.at[chunk, step],
                                                       device_id=(to,), device_id_type=MESH_ID))
        return copies

    def lab_copies():
        return [pltpu.make_async_remote_copy(labs.at[me], labs.at[me], lab_send.at[step], lab_recv.at[step],
                                             device_id=(lax.rem(me + step, total),), device_id_type=MESH_ID) for step in range(1, total)]

    def label_row(chunk, part):
        lab = lab_ref[pl.ds(chunk * 2 + part, 1), :] - base
        return jnp.where(lab < vocab_rows, lab, -1)

    row_ids = lax.broadcasted_iota(jnp.int32, (VOCAB_TILE, half), 0)

    def forward_half(chunk, part):
        slot = lax.rem(chunk, 2)
        zb = zbuf[chunk, part].reshape(half, dim)
        lab = label_row(chunk, part)
        tops, sums, hits = [], [], []
        for tile in range(tiles):
            rows = slice(tile * VOCAB_TILE, (tile + 1) * VOCAB_TILE)
            logits = lax.dot_general(table_ref[rows, :], zb, COLS_DIMS, preferred_element_type=jnp.float32)
            if (tile + 1) * VOCAB_TILE > vocab_rows:
                logits = jnp.where(row_ids < vocab_rows - tile * VOCAB_TILE, logits, PAD_LOGIT)
            lbuf[slot, rows, part * half:(part + 1) * half] = logits
            top = jnp.max(logits, axis=0, keepdims=True)
            tops.append(top)
            sums.append(jnp.sum(jnp.exp(logits - top), axis=0, keepdims=True))
            hits.append(jnp.sum(jnp.where(row_ids == lab - tile * VOCAB_TILE, logits, 0.0), axis=0, keepdims=True))
        top = functools.reduce(jnp.maximum, tops)
        exp_sum = sum(s * jnp.exp(t - top) for s, t in zip(sums, tops))
        stats[chunk, me, part:part + 1, :] = top
        stats[chunk, me, 2 + part:3 + part, :] = exp_sum
        labs[me] += sum(hits)

    def combine(chunk):
        for part in range(2):
            tops = stats[chunk, :, part, :]
            top = jnp.max(tops, axis=0, keepdims=True)
            exp_sum = jnp.sum(stats[chunk, :, 2 + part, :] * jnp.exp(tops - top), axis=0, keepdims=True)
            norm[part:part + 1, :] = top
            norm[2 + part:3 + part, :] = 1.0 / exp_sum
            loss_ref[part:part + 1, :] += top + jnp.log(exp_sum)

    def table_half(chunk, which):
        slot = lax.rem(chunk, 2)
        zc = zbuf[chunk].reshape(2 * half, dim)
        for tile in range(which * tiles // 2, (which + 1) * tiles // 2):
            rows = slice(tile * VOCAB_TILE, (tile + 1) * VOCAB_TILE)
            for part in range(2):
                lanes = slice(part * half, (part + 1) * half)
                probs = jnp.exp(lbuf[slot, rows, lanes] - norm[part:part + 1, :]) * norm[2 + part:3 + part, :]
                hot = row_ids == label_row(chunk, part) - tile * VOCAB_TILE
                gbuf[rows, lanes] = jnp.where(hot, probs - 1.0, probs).astype(jnp.bfloat16)
            dtable_ref[rows, :] += jnp.dot(gbuf[rows, :], zc, preferred_element_type=jnp.float32)

    def token_half(chunk, part):
        dz = lax.dot_general(gbuf[:, part * half:(part + 1) * half], table_ref[...], ROWS_DIMS, preferred_element_type=jnp.float32)
        dzbuf[lax.rem(chunk, 3), part] = dz.reshape(2, 2, 2, UNIT, dim)

    start(gather_copies(0, 1))
    start(gather_copies(1, 1))
    start(gather_copies(2, 1))
    for chunk in range(3):
        finish(gather_copies(chunk, 1))
        start(gather_copies(chunk, 2))
    for chunk in range(2):
        finish(gather_copies(chunk, 2))
        start(gather_copies(chunk, 3))
    finish(gather_copies(0, 3))
    start(gather_copies(0, 4))
    finish(gather_copies(0, 4))

    def body(i, carry):
        def inside(offset, action):
            chunk = i + offset
            pl.when((chunk >= 0) & (chunk < chunks))(lambda: action(jnp.clip(chunk, 0, chunks - 1)))

        def step_reduce(phase, follow):
            def action(chunk):
                finish(reduce_copies(chunk, phase))
                reduce_add(chunk, phase)
                if follow:
                    start(reduce_copies(chunk, phase + 1))
            return action

        def step_gather(phase):
            def action(chunk):
                finish(gather_copies(chunk, phase))
                start(gather_copies(chunk, phase + 1))
            return action

        inside(-4, step_reduce(2, True))
        inside(-2, lambda chunk: start(reduce_copies(chunk, 0)))
        inside(1, step_gather(3))
        inside(3, lambda chunk: start(gather_copies(chunk, 1)))
        inside(2, step_gather(2))

        @pl.when(i < chunks)
        def _():
            forward_half(i, 0)
            forward_half(i, 1)

        inside(-2, step_reduce(0, False))
        inside(-3, step_reduce(1, True))
        inside(-4, step_reduce(3, False))
        inside(3, step_gather(1))
        inside(1, lambda chunk: finish(gather_copies(chunk, 4)))
        inside(-2, lambda chunk: start(reduce_copies(chunk, 1)))
        inside(0, lambda chunk: start(stat_copies(chunk)))

        @pl.when(i == chunks - 1)
        def _():
            start(lab_copies())

        def backward(chunk):
            finish(stat_copies(chunk))
            combine(chunk)
            table_half(chunk, 0)
            table_half(chunk, 1)
            token_half(chunk, 0)
            token_half(chunk, 1)

        inside(-1, backward)
        return carry

    lax.fori_loop(0, chunks + 4, body, 0)
    finish(lab_copies())
    loss_ref[2:3, :] = -jnp.sum(labs[...], axis=0)


def head(z_local, table_padded, lab_rows, vocab_rows):
    tokens, dim = z_local.shape
    chunks = tokens // UNIT
    padded = table_padded.shape[0]
    chunk_tokens = 16 * UNIT
    part_cols = dim // PARTS
    f32, bf16 = jnp.float32, jnp.bfloat16
    sems = pltpu.SemaphoreType.DMA
    vmem = pl.BlockSpec(memory_space=pltpu.VMEM)
    cost = 6 * tokens * 16 * padded * dim
    return pl.pallas_call(
        functools.partial(head_kernel, vocab_rows, chunks),
        in_specs=[pl.BlockSpec(memory_space=pl.ANY), vmem, vmem],
        out_specs=[vmem, vmem, vmem],
        out_shape=[jax.ShapeDtypeStruct((tokens, dim), f32),
                   jax.ShapeDtypeStruct((padded, dim), f32),
                   jax.ShapeDtypeStruct((3, 8 * UNIT), f32)],
        scratch_shapes=[pltpu.VMEM((chunks, 2, 2, 2, 2, UNIT, dim), bf16),
                        pltpu.VMEM((2, padded, chunk_tokens), f32),
                        pltpu.VMEM((padded, chunk_tokens), bf16),
                        pltpu.VMEM((3, 2, 2, 2, 2, UNIT, dim), f32),
                        pltpu.VMEM((2, 2, 2, 2, UNIT, dim), f32),
                        pltpu.VMEM((2, PARTS, 2, 2, UNIT, part_cols), f32),
                        pltpu.VMEM((2, PARTS, 2, UNIT, part_cols), f32),
                        pltpu.VMEM((2, PARTS, UNIT, part_cols), f32),
                        pltpu.VMEM((chunks, 16, STAT_ROWS, 8 * UNIT), f32),
                        pltpu.VMEM((16, 1, 8 * UNIT), f32),
                        pltpu.VMEM((8, 8 * UNIT), f32),
                        sems(()),
                        sems((chunks, 10)), sems((chunks, 10)),
                        sems((chunks, 10)), sems((chunks, 10)),
                        sems((chunks, 16)), sems((chunks, 16)),
                        sems((16,)), sems((16,))],
        compiler_params=pltpu.CompilerParams(vmem_limit_bytes=67043328, collective_id=1, has_side_effects=True),
        cost_estimate=pl.CostEstimate(flops=cost, bytes_accessed=4 * padded * dim, transcendentals=2 * tokens * 16 * padded),
        name="head_all",
    )(z_local.reshape(chunks, UNIT, dim), table_padded, lab_rows)


PIECES = 4


def axes(part):
    return part % 3, (part + 1) % 3, (part + 2) % 3


def cube_index(choice):
    return choice.get(2, slice(None)), choice.get(1, slice(None)), choice.get(0, slice(None))


def tail_kernel(table_rows, gate_hbm, up_hbm, down_hbm, send_hbm, row_ref, dtable_hbm, gate_out, up_out, down_out, dtable_out,
                acc_g, acc_u, acc_d, core_g, core_u, core_d, one_g, one_u, one_d, two_g, two_u, two_d, three_g, three_u, three_d,
                rows_got, split, local_sem, send_sem, recv_sem, row_send, row_recv):
    me = lax.axis_index('fsdp')
    total = 16
    core = lax.rem(me, 2)
    pos = [lax.rem(me // 2, 2), lax.rem(me // 4, 2), me // 8]
    core_peer = me + 1 - 2 * core
    whole = (gate_hbm, up_hbm, down_hbm)
    accs = (acc_g, acc_u, acc_d)
    gots = ((core_g, core_u, core_d), (one_g, one_u, one_d), (two_g, two_u, two_d), (three_g, three_u, three_d))
    outs = (gate_out, up_out, down_out)

    barrier = pltpu.get_barrier_semaphore()
    for step in range(1, total):
        pl.semaphore_signal(barrier, inc=1, device_id=(lax.rem(me + step, total),), device_id_type=MESH_ID)
    loads = [pltpu.make_async_copy(whole[part].at[:, :, :, core], accs[part], local_sem.at[part]) for part in range(3)]
    loads.append(pltpu.make_async_copy(dtable_hbm.at[pl.ds(0, table_rows)], dtable_out, local_sem.at[3]))
    loads.append(pltpu.make_async_copy(send_hbm.at[me], rows_got.at[me], local_sem.at[4]))
    for load in loads:
        load.start()
    pl.semaphore_wait(barrier, total - 1)

    def piece(part, q):
        if part == 2:
            size = acc_d.shape[3] // PIECES
            return pl.ds(q * size, size), slice(None)
        size = acc_g.shape[4] // PIECES
        return slice(None), pl.ds(q * size, size)

    def copies(phase, q):
        made = []
        for part in range(3):
            rows, lanes = piece(part, q)
            order = axes(part)
            if phase == 0:
                src = whole[part].at[:, :, :, 1 - core, rows, lanes]
                dst = gots[0][part].at[:, :, :, rows, lanes]
                to = core_peer
            else:
                fixed = {axis: pos[axis] for axis in order[:phase - 1]}
                fixed[order[phase - 1]] = 1 - pos[order[phase - 1]]
                iz, iy, ix = cube_index(fixed)
                src = accs[part].at[iz, iy, ix, rows, lanes]
                lead = (slice(None),) * (3 - phase)
                dst = gots[phase][part].at[lead + (rows, lanes)]
                axis = order[phase - 1]
                to = me + (1 - 2 * pos[axis]) * (2 << axis)
            made.append(pltpu.make_async_remote_copy(src, dst, send_sem.at[phase, part, q], recv_sem.at[phase, part, q],
                                                     device_id=(to,), device_id_type=MESH_ID))
        return made

    def start(made):
        for copy in made:
            copy.start()

    def finish_add(phase, q):
        for copy in copies(phase, q):
            copy.wait()
        for part in range(3):
            rows, lanes = piece(part, q)
            iz, iy, ix = cube_index({axis: pos[axis] for axis in axes(part)[:phase]})
            got = gots[phase][part][(slice(None),) * (3 - phase) + (rows, lanes)]
            if phase == 3:
                outs[part][rows, lanes] = accs[part][iz, iy, ix, rows, lanes] + got
            else:
                accs[part][iz, iy, ix, rows, lanes] += got

    row_copies = []
    for step in range(1, total):
        to = lax.rem(me + step, total)
        row_copies.append(pltpu.make_async_remote_copy(send_hbm.at[to], rows_got.at[me], row_send.at[step], row_recv.at[step],
                                                       device_id=(to,), device_id_type=MESH_ID))
    for q in range(PIECES):
        start(copies(0, q))
    start(row_copies)
    for load in loads:
        load.wait()
    for q in range(PIECES):
        finish_add(0, q)
        start(copies(1, q))
    for copy in row_copies:
        copy.wait()
    slots, dim = rows_got.shape[0] * rows_got.shape[1], rows_got.shape[2]

    def split_rows(s, carry):
        vals = rows_got[s]
        at = pl.multiple_of(s * SLOTS, SLOTS)
        high = vals.astype(jnp.bfloat16)
        rest = vals - high.astype(jnp.float32)
        mid = rest.astype(jnp.bfloat16)
        split[pl.ds(at, SLOTS), :] = high
        split[pl.ds(slots + at, SLOTS), :] = mid
        split[pl.ds(2 * slots + at, SLOTS), :] = (rest - mid.astype(jnp.float32)).astype(jnp.bfloat16)
        return carry

    lax.fori_loop(0, total, split_rows, 0)

    def add_rows(first, count):
        ids = lax.broadcasted_iota(jnp.int32, (count, slots), 0) + first
        hot = jnp.where(ids == row_ref[...], 1.0, 0.0).astype(jnp.bfloat16)
        dtable_out[pl.ds(first, count), :] += jnp.dot(jnp.concatenate([hot, hot, hot], axis=1), split[...], preferred_element_type=jnp.float32)

    full = table_rows // VOCAB_TILE

    def add_tile(tile, carry):
        add_rows(pl.multiple_of(tile * VOCAB_TILE, VOCAB_TILE), VOCAB_TILE)
        return carry

    lax.fori_loop(0, full, add_tile, 0)
    if table_rows % VOCAB_TILE:
        add_rows(full * VOCAB_TILE, table_rows % VOCAB_TILE)

    for q in range(PIECES + 2):
        if q < PIECES:
            finish_add(1, q)
            start(copies(2, q))
        if 1 <= q <= PIECES:
            finish_add(2, q - 1)
            start(copies(3, q - 1))
        if q >= 2:
            finish_add(3, q - 2)


def tail(grad_gate, grad_up, grad_down, send, row_idx, dtable, table_rows):
    f32 = jnp.float32
    vmem = pl.BlockSpec(memory_space=pltpu.VMEM)
    anywhere = pl.BlockSpec(memory_space=pl.ANY)
    sems = pltpu.SemaphoreType.DMA
    blocks = [tuple(array.shape[4:]) for array in (grad_gate, grad_up, grad_down)]
    scratch = [pltpu.VMEM(lead + block, f32) for lead in ((2, 2, 2), (2, 2, 2), (2, 2), (2,), ()) for block in blocks]
    slots = send.shape[0] * send.shape[1]
    dim = send.shape[2]
    return pl.pallas_call(
        functools.partial(tail_kernel, table_rows),
        in_specs=[anywhere, anywhere, anywhere, anywhere, vmem, anywhere],
        out_specs=[vmem] * 4,
        out_shape=[jax.ShapeDtypeStruct(block, f32) for block in blocks] + [jax.ShapeDtypeStruct((table_rows, dim), f32)],
        scratch_shapes=scratch + [pltpu.VMEM(send.shape, f32), pltpu.VMEM((3 * slots, dim), jnp.bfloat16),
                                  sems((5,)), sems((4, 3, PIECES)), sems((4, 3, PIECES)), sems((16,)), sems((16,))],
        compiler_params=pltpu.CompilerParams(vmem_limit_bytes=60 * 1024 * 1024, collective_id=2, has_side_effects=True),
        cost_estimate=pl.CostEstimate(flops=6 * slots * table_rows * dim, bytes_accessed=40 * 1024 * 1024, transcendentals=0),
        name="tail_all",
    )(grad_gate, grad_up, grad_down, send, row_idx, dtable)


def front_kernel(table_rows, pack_hbm, table_ref, gate_hbm, up_hbm, down_hbm,
                 pack_out, table_out, gate_out, up_out, down_out, x_out, slots_out, rows_out, rank_out,
                 send, got, before_ref, local_sem, id_send, id_recv, w_send, w_recv, c_send, c_recv, row_send, row_recv):
    me = lax.axis_index('fsdp')
    total = 16
    core = lax.rem(me, 2)
    pos = [lax.rem(me // 2, 2), lax.rem(me // 4, 2), me // 8]
    core_peer = me + 1 - 2 * core
    shards = (gate_hbm, up_hbm, down_hbm)
    outs = (gate_out, up_out, down_out)
    tokens = pack_out.shape[2]
    padded, dim = table_out.shape

    barrier = pltpu.get_barrier_semaphore()
    for step in range(1, total):
        pl.semaphore_signal(barrier, inc=1, device_id=(lax.rem(me + step, total),), device_id_type=MESH_ID)
    loads = [pltpu.make_async_copy(shards[part], outs[part].at[pos[2], pos[1], pos[0], core], local_sem.at[part]) for part in range(3)]
    loads.append(pltpu.make_async_copy(pack_hbm, pack_out.at[me], local_sem.at[3]))
    for load in loads:
        load.start()

    def remote(src, dst, send_sem, recv_sem, to):
        return pltpu.make_async_remote_copy(src, dst, send_sem, recv_sem, device_id=(to,), device_id_type=MESH_ID)

    def wide(phase):
        made = []
        for part in range(3):
            order = axes(part)
            iz, iy, ix = cube_index({axis: pos[axis] for axis in order[phase - 1:]})
            here = outs[part].at[iz, iy, ix, core]
            axis = order[phase - 1]
            made.append(remote(shards[part] if phase == 1 else here, here, w_send.at[phase, part], w_recv.at[phase, part],
                               me + (1 - 2 * pos[axis]) * (2 << axis)))
        return made

    def across(stage):
        made = []
        for part in range(3):
            order = axes(part)
            fixed = {axis: pos[axis] for axis in order[stage:]}
            if stage:
                fixed[order[stage - 1]] = 1 - pos[order[stage - 1]]
            iz, iy, ix = cube_index(fixed)
            here = outs[part].at[iz, iy, ix, core]
            made.append(remote(here if stage else shards[part], here, c_send.at[stage, part], c_recv.at[stage, part], core_peer))
        return made

    def id_copies():
        return [remote(pack_hbm, pack_out.at[me], id_send.at[step], id_recv.at[step], lax.rem(me + step, total)) for step in range(1, total)]

    def row_copy(step):
        to = lax.rem(me + step, total)
        return remote(send.at[to], got.at[me], row_send.at[step], row_recv.at[step], to)

    def start(made):
        for copy in made:
            copy.start()

    def finish(made):
        for copy in made:
            copy.wait()

    pl.semaphore_wait(barrier, total - 1)
    start(id_copies())
    start(wide(1))
    start(across(0))
    table_out[0:table_rows, :] = table_ref[...]
    table_out[table_rows:padded, :] = jnp.zeros((padded - table_rows, dim), table_out.dtype)
    earlier = lax.broadcasted_iota(jnp.int32, (tokens, tokens), 0) < lax.broadcasted_iota(jnp.int32, (tokens, tokens), 1)
    before_ref[...] = jnp.where(earlier, 1.0, 0.0).astype(jnp.bfloat16)
    rank_out[...] = jnp.zeros_like(rank_out)
    for load in loads:
        load.wait()
    finish(id_copies())

    lanes_iota = lax.broadcasted_iota(jnp.int32, (SLOTS, padded), 1)
    slot_iota = lax.broadcasted_iota(jnp.int32, (SLOTS, tokens), 0)
    dev_iota = lax.broadcasted_iota(jnp.int32, (total, tokens), 0)

    def build(step):
        to = lax.rem(me + step, total)
        ids = pack_out[to, 0:1, :]
        owner = jnp.zeros_like(ids)
        for k in range(1, total):
            owner = owner + jnp.where(ids >= k * table_rows, 1, 0)
        hot = jnp.where(dev_iota == owner, 1.0, 0.0)
        before = jnp.dot(hot.astype(jnp.bfloat16), before_ref[...], preferred_element_type=jnp.float32)
        rank = jnp.sum(hot * before, axis=0, keepdims=True)
        rank_out[...] = jnp.maximum(rank_out[...], rank)
        rank = rank.astype(jnp.int32)
        owned = jnp.where(owner == me, rank, -1)
        picked = jnp.where(slot_iota == owned, 1.0, 0.0)
        code = ids - me * table_rows + 1
        column = jnp.sum(picked * code.astype(jnp.float32), axis=1, keepdims=True).astype(jnp.int32) - 1
        high = lax.shift_right_arithmetic(code, 6)
        digits = jnp.where(owner == me, jnp.concatenate([high, code - high * 64], axis=0), 0)
        digits = jnp.concatenate([digits, jnp.zeros((6, tokens), jnp.int32)], axis=0).astype(jnp.float32).astype(jnp.bfloat16)
        spread = lax.dot_general(digits, picked.astype(jnp.bfloat16), COLS_DIMS, preferred_element_type=jnp.float32)
        rows_out[pl.ds(to, 1), :] = (spread[0:1] * 64.0 + spread[1:2]).astype(jnp.int32) - 1
        choose = jnp.where(lanes_iota == column, 1.0, 0.0).astype(jnp.bfloat16)
        send[to] = jnp.dot(choose, table_out[...], preferred_element_type=jnp.float32).astype(jnp.bfloat16)
        return owner, rank

    owner, rank = build(0)
    slots_out[...] = jnp.where(rank < SLOTS, owner * SLOTS + rank, -1)
    own_rows = pltpu.make_async_copy(send.at[me], got.at[me], local_sem.at[4])

    def build_step(step, carry):
        build(step)
        pl.when(step > 1)(lambda: row_copy(step - 1).start())
        return carry

    lax.fori_loop(1, 6, build_step, 0)
    own_rows.start()
    finish(wide(1))
    start(wide(2))
    start(across(1))
    lax.fori_loop(6, total, build_step, 0)
    row_copy(total - 1).start()
    finish(wide(2))
    start(wide(3))
    start(across(2))
    own_rows.wait()
    finish([row_copy(step) for step in range(1, total)])
    place = lax.broadcasted_iota(jnp.int32, (total * SLOTS, tokens), 0) == slots_out[...]
    x_out[...] = lax.dot_general(jnp.where(place, 1.0, 0.0).astype(jnp.bfloat16), got[...].reshape(total * SLOTS, dim), ROWS_DIMS,
                                 preferred_element_type=jnp.float32).astype(jnp.bfloat16)
    finish(across(0))
    finish(across(1))
    finish(wide(3))
    start(across(3))
    finish(across(2))
    finish(across(3))


def front(packed, table_shard, gate_shard, up_shard, down_shard):
    bf16 = jnp.bfloat16
    rows, dim = table_shard.shape
    padded = -(-rows // VOCAB_TILE) * VOCAB_TILE
    tokens = packed.shape[1]
    vmem = pl.BlockSpec(memory_space=pltpu.VMEM)
    anywhere = pl.BlockSpec(memory_space=pl.ANY)
    sems = pltpu.SemaphoreType.DMA
    shards = (gate_shard, up_shard, down_shard)
    return pl.pallas_call(
        functools.partial(front_kernel, rows),
        in_specs=[anywhere, vmem, anywhere, anywhere, anywhere],
        out_specs=[vmem] * 9,
        out_shape=[jax.ShapeDtypeStruct((16,) + packed.shape, jnp.int32), jax.ShapeDtypeStruct((padded, dim), bf16)]
        + [jax.ShapeDtypeStruct((2, 2, 2, 2) + shard.shape, bf16) for shard in shards]
        + [jax.ShapeDtypeStruct((tokens, dim), bf16), jax.ShapeDtypeStruct((1, tokens), jnp.int32),
           jax.ShapeDtypeStruct((16, SLOTS), jnp.int32), jax.ShapeDtypeStruct((1, tokens), jnp.float32)],
        scratch_shapes=[pltpu.VMEM((16, SLOTS, dim), bf16), pltpu.VMEM((16, SLOTS, dim), bf16), pltpu.VMEM((tokens, tokens), bf16),
                        sems((5,)), sems((16,)), sems((16,)), sems((4, 3)), sems((4, 3)), sems((4, 3)), sems((4, 3)), sems((16,)), sems((16,))],
        compiler_params=pltpu.CompilerParams(vmem_limit_bytes=60 * 1024 * 1024, collective_id=3, has_side_effects=True),
        cost_estimate=pl.CostEstimate(flops=4 * 16 * SLOTS * padded * dim, bytes_accessed=20 * 1024 * 1024, transcendentals=0),
        name="front_all",
    )(packed, table_shard, gate_shard, up_shard, down_shard)


def split3(values):
    high = lax.reduce_precision(values, 8, 7)
    rest = values - high
    mid = lax.reduce_precision(rest, 8, 7)
    low = rest - mid
    return [part.astype(jnp.bfloat16) for part in (high, mid, low)]


def pick_rows(select, values):
    total = None
    for part in split3(values):
        term = jnp.dot(select, part, preferred_element_type=jnp.float32)
        total = term if total is None else total + term
    return total


def solution(mesh):
    groups = mesh.shape['fsdp']

    def device_step(token_ids, labels, table_shard, gate_shard, up_shard, down_shard, gain_in, gain_out):
        micro_count = token_ids.shape[0]
        tok_micro = token_ids.shape[1] * token_ids.shape[2]
        tok_dev = micro_count * tok_micro
        total_tokens = tok_dev * groups
        rows, dim = table_shard.shape
        me = lax.axis_index('fsdp')

        packed = jnp.stack([token_ids.reshape(tok_dev), labels.reshape(tok_dev)])
        gate_rows, ffn = gate_shard.shape
        down_rows = down_shard.shape[0]
        (packed_all, table_padded, w_gate, w_up, w_down, emb_rows, slots, row_idx, top_rank) = front(
            packed, table_shard, gate_shard, up_shard, down_shard)
        w_gate = w_gate.reshape(groups * gate_rows, ffn)
        w_up = w_up.reshape(groups * gate_rows, ffn)
        w_down = w_down.reshape(groups * down_rows, dim)
        rounds = jnp.max(top_rank).astype(jnp.int32) // SLOTS + 1
        slot_ids = jnp.arange(SLOTS, dtype=jnp.int32)

        def ranks(round_idx):
            ids_all, round_idx = lax.optimization_barrier((packed_all[:, 0], round_idx))
            owner = ids_all // rows
            owner_hot = owner[:, :, None] == jnp.arange(groups, dtype=jnp.int32)
            tri = jnp.tril(jnp.ones((tok_dev, tok_dev), jnp.bfloat16), -1)
            before = jnp.einsum('tu,suo->sto', tri, owner_hot.astype(jnp.bfloat16), preferred_element_type=jnp.float32)
            rank = jnp.sum(jnp.where(owner_hot, before, 0.0), axis=-1).astype(jnp.int32)
            return owner, ids_all - owner * rows, rank - round_idx * SLOTS

        def owned_rows(owner, local, rank):
            hit = (owner == me)[:, None, :] & (rank[:, None, :] == slot_ids[None, :, None])
            return (jnp.sum(jnp.where(hit, local[:, None, :] + 1, 0), axis=-1) - 1).reshape(groups * SLOTS)

        def my_slots(owner, rank):
            mine = lax.dynamic_index_in_dim(owner, me, 0, keepdims=False)
            off = lax.dynamic_index_in_dim(rank, me, 0, keepdims=False)
            return jnp.where((off >= 0) & (off < SLOTS), mine * SLOTS + off, -1)

        def slot_place(slot_row):
            return (jnp.arange(groups * SLOTS, dtype=jnp.int32)[:, None] == slot_row[None, :]).astype(jnp.bfloat16)

        def fetch_round(round_idx):
            owner, local, rank = ranks(round_idx)
            select = (owned_rows(owner, local, rank)[:, None] == jnp.arange(rows, dtype=jnp.int32)[None, :]).astype(jnp.bfloat16)
            send = jnp.dot(select, table_shard, preferred_element_type=jnp.float32).astype(jnp.bfloat16)
            got = lax.all_to_all(send.reshape(groups, SLOTS, dim), 'fsdp', 0, 0).reshape(groups * SLOTS, dim)
            place = slot_place(my_slots(owner, rank))
            return lax.dot_general(place, got, ROWS_DIMS, preferred_element_type=jnp.float32).astype(jnp.bfloat16)

        def return_round(round_idx, grad_rows):
            owner, local, rank = ranks(round_idx)
            send = pick_rows(slot_place(my_slots(owner, rank)), grad_rows)
            got = lax.all_to_all(send.reshape(groups, SLOTS, dim), 'fsdp', 0, 0).reshape(groups * SLOTS, dim)
            select = (jnp.arange(rows, dtype=jnp.int32)[:, None] == owned_rows(owner, local, rank)[None, :]).astype(jnp.bfloat16)
            return pick_rows(select, got)

        emb_rows = lax.fori_loop(1, rounds, lambda r, acc: acc + fetch_round(r), emb_rows)

        normed, saved = [], []
        for m in range(micro_count):
            out, kept = mlp_forward(emb_rows[m * tok_micro:(m + 1) * tok_micro], gain_in, gain_out, w_gate, w_up, w_down)
            normed.append(out)
            saved.append(kept)

        chunks = tok_dev // UNIT
        lab_rows = jnp.transpose(packed_all[:, 1].reshape(groups, chunks, UNIT), (1, 0, 2)).reshape(2 * chunks, groups * UNIT // 2)
        dz, dtable, loss_rows = head(jnp.concatenate(normed, axis=0), table_padded, lab_rows, rows)
        loss_total = jnp.sum(loss_rows)
        grad_normed = [dz[m * tok_micro:(m + 1) * tok_micro] for m in range(micro_count)]

        backs = [mlp_backward(saved[m], grad_normed[m], gain_in, gain_out, w_gate, w_up, w_down) for m in range(micro_count)]
        grad_rows, grad_mid, grad_gate_pre, grad_up_proj = [jnp.concatenate(parts, axis=0) for parts in zip(*backs)]
        normed_in = jnp.concatenate([kept[1] for kept in saved], axis=0)
        acts = jnp.concatenate([kept[5] for kept in saved], axis=0)
        grad_down = lax.dot_general(acts, grad_mid, ROWS_DIMS, preferred_element_type=jnp.float32)
        grad_gate = lax.dot_general(normed_in, grad_gate_pre, ROWS_DIMS, preferred_element_type=jnp.float32)
        grad_up = lax.dot_general(normed_in, grad_up_proj, ROWS_DIMS, preferred_element_type=jnp.float32)
        cube = (2, 2, 2, 2)
        send = pick_rows(slot_place(slots[0]), grad_rows).reshape(groups, SLOTS, dim)
        out_gate, out_up, out_down, dtable = tail(grad_gate.reshape(cube + (gate_rows, ffn)), grad_up.reshape(cube + (gate_rows, ffn)),
                                                  grad_down.reshape(cube + (down_rows, dim)), send, row_idx.reshape(1, groups * SLOTS), dtable, rows)
        dtable = lax.fori_loop(1, rounds, lambda r, acc: acc + return_round(r, grad_rows), dtable)
        return (loss_total / total_tokens, dtable, out_gate, out_up, out_down)

    row_spec = P('fsdp', None)
    tok_spec = P(None, 'fsdp', None)
    return jax.shard_map(device_step, mesh=mesh,
                         in_specs=(tok_spec, tok_spec, row_spec, row_spec, row_spec, row_spec, P(), P()),
                         out_specs=(P(), row_spec, row_spec, row_spec, row_spec), check_vma=False)
```

```python
import functools
import jax
import jax.numpy as jnp
from jax import lax
from jax.experimental import pallas as pl
from jax.experimental.pallas import tpu as pltpu
from jax.sharding import PartitionSpec as P

NORM_EPS = 1e-6
SLOTS = 64


def rms_scale(values, gain_vec):
    vals32 = values.astype(jnp.float32)
    inv_rms = lax.rsqrt(jnp.mean(vals32 * vals32, axis=-1, keepdims=True) + NORM_EPS)
    return (vals32 * inv_rms * gain_vec).astype(jnp.bfloat16), inv_rms


def rms_back(values, inv_rms, gain_vec, grad_out):
    vals32 = values.astype(jnp.float32)
    scaled = grad_out * gain_vec
    proj_mean = jnp.mean(scaled * vals32, axis=-1, keepdims=True)
    return inv_rms * scaled - vals32 * (inv_rms * inv_rms * inv_rms) * proj_mean


def mlp_forward(emb_rows, gain_in, gain_out, w_gate, w_up, w_down):
    normed_in, inv_in = rms_scale(emb_rows, gain_in)
    gate_pre = jnp.dot(normed_in, w_gate, preferred_element_type=jnp.float32).astype(jnp.bfloat16)
    up_proj = jnp.dot(normed_in, w_up, preferred_element_type=jnp.float32).astype(jnp.bfloat16)
    acts = (jax.nn.silu(gate_pre.astype(jnp.float32)) * up_proj.astype(jnp.float32)).astype(jnp.bfloat16)
    mlp_out = jnp.dot(acts, w_down, preferred_element_type=jnp.float32).astype(jnp.bfloat16)
    hidden = (emb_rows.astype(jnp.float32) + mlp_out.astype(jnp.float32)).astype(jnp.bfloat16)
    normed_out, inv_out = rms_scale(hidden, gain_out)
    return normed_out, (emb_rows, normed_in, inv_in, gate_pre, up_proj, acts, hidden, inv_out)


COLS_DIMS = (((1,), (1,)), ((), ()))
ROWS_DIMS = (((0,), (0,)), ((), ()))


def mlp_backward(saved, grad_normed, gain_in, gain_out, w_gate, w_up, w_down):
    emb_rows, normed_in, inv_in, gate_pre, up_proj, acts, hidden, inv_out = saved
    grad_hidden = rms_back(hidden, inv_out, gain_out, grad_normed)
    grad_mid = grad_hidden.astype(jnp.bfloat16)
    grad_acts = lax.dot_general(grad_mid, w_down, COLS_DIMS, preferred_element_type=jnp.float32)
    gate32 = gate_pre.astype(jnp.float32)
    gate_sig = jax.nn.sigmoid(gate32)
    grad_gate_pre = (grad_acts * up_proj.astype(jnp.float32) * gate_sig * (1.0 + gate32 * (1.0 - gate_sig))).astype(jnp.bfloat16)
    grad_up_proj = (grad_acts * gate32 * gate_sig).astype(jnp.bfloat16)
    grad_normed_in = (lax.dot_general(grad_gate_pre, w_gate, COLS_DIMS, preferred_element_type=jnp.float32)
                      + lax.dot_general(grad_up_proj, w_up, COLS_DIMS, preferred_element_type=jnp.float32))
    grad_rows = grad_hidden + rms_back(emb_rows, inv_in, gain_in, grad_normed_in)
    return grad_rows, grad_mid, grad_gate_pre, grad_up_proj


UNIT = 64
CUBE_BITS = 3
PARTS = 3
VOCAB_TILE = 256
STAT_ROWS = 4
MESH_ID = pl.DeviceIdType.MESH
PAD_LOGIT = -1e30


def head_kernel(vocab_rows, chunks, z_hbm, table_ref, lab_ref, dz_ref, dtable_ref, loss_ref,
                zbuf, lbuf, gbuf, dzbuf, got_core, got_one, got_two, got_three, stats, labs, norm,
                local_sem, ag_send, ag_recv, rs_send, rs_recv, st_send, st_recv, lab_send, lab_recv):
    me = lax.axis_index('fsdp')
    total = 16
    core = lax.rem(me, 2)
    pos = [lax.rem(me // 2, 2), lax.rem(me // 4, 2), me // 8]
    base = me * vocab_rows
    padded, dim = table_ref.shape
    part_cols = dim // PARTS
    half = 8 * UNIT
    tiles = padded // VOCAB_TILE

    def peer(axis):
        return me + (1 - 2 * pos[axis]) * (2 << axis)

    core_peer = me + 1 - 2 * core

    barrier = pltpu.get_barrier_semaphore()
    for step in range(1, total):
        pl.semaphore_signal(barrier, inc=1, device_id=(lax.rem(me + step, total),), device_id_type=MESH_ID)
    own = pltpu.make_async_copy(z_hbm, zbuf.at[:, pos[2], pos[1], pos[0], core], local_sem)
    own.start()
    dtable_ref[...] = jnp.zeros_like(dtable_ref)
    loss_ref[...] = jnp.zeros_like(loss_ref)
    labs[me] = jnp.zeros((1, half), jnp.float32)
    own.wait()
    pl.semaphore_wait(barrier, total - 1)

    def where(choice):
        return choice.get(2, slice(None)), choice.get(1, slice(None)), choice.get(0, slice(None))

    def axes(part):
        return part % 3, (part + 1) % 3, (part + 2) % 3

    def cols(part):
        return pl.ds(part * part_cols, part_cols)

    def gather_copies(chunk, phase):
        if phase == 4:
            here = zbuf.at[chunk, :, :, :, core]
            return [pltpu.make_async_remote_copy(here, here, ag_send.at[chunk, 9], ag_recv.at[chunk, 9],
                                                 device_id=(core_peer,), device_id_type=MESH_ID)]
        copies = []
        for part in range(PARTS):
            order = axes(part)
            fixed = {axis: pos[axis] for axis in order[phase - 1:]}
            iz, iy, ix = where(fixed)
            here = zbuf.at[chunk, iz, iy, ix, core, :, cols(part)]
            sem = (phase - 1) * PARTS + part
            copies.append(pltpu.make_async_remote_copy(here, here, ag_send.at[chunk, sem], ag_recv.at[chunk, sem],
                                                       device_id=(peer(order[phase - 1]),), device_id_type=MESH_ID))
        return copies

    def reduce_copies(chunk, phase):
        slot, dzs = lax.rem(chunk, 2), lax.rem(chunk, 3)
        if phase == 0:
            return [pltpu.make_async_remote_copy(dzbuf.at[dzs, :, :, :, 1 - core], got_core.at[slot], rs_send.at[chunk, 9], rs_recv.at[chunk, 9],
                                                 device_id=(core_peer,), device_id_type=MESH_ID)]
        copies = []
        for part in range(PARTS):
            order = axes(part)
            fixed = {axis: pos[axis] for axis in order[:phase - 1]}
            fixed[order[phase - 1]] = 1 - pos[order[phase - 1]]
            iz, iy, ix = where(fixed)
            got = (got_one, got_two, got_three)[phase - 1]
            sem = (phase - 1) * PARTS + part
            copies.append(pltpu.make_async_remote_copy(dzbuf.at[dzs, iz, iy, ix, core, :, cols(part)], got.at[slot, part],
                                                       rs_send.at[chunk, sem], rs_recv.at[chunk, sem],
                                                       device_id=(peer(order[phase - 1]),), device_id_type=MESH_ID))
        return copies

    def start(copies):
        for copy in copies:
            copy.start()

    def finish(copies):
        for copy in copies:
            copy.wait()

    def reduce_add(chunk, phase):
        slot, dzs = lax.rem(chunk, 2), lax.rem(chunk, 3)
        if phase == 0:
            dzbuf[dzs, :, :, :, core] += got_core[slot]
            return
        for part in range(PARTS):
            order = axes(part)
            iz, iy, ix = where({axis: pos[axis] for axis in order[:phase]})
            got = (got_one, got_two, got_three)[phase - 1]
            lanes = slice(part * part_cols, (part + 1) * part_cols)
            if phase == 3:
                rows = pl.ds(pl.multiple_of(chunk * UNIT, UNIT), UNIT)
                dz_ref[rows, lanes] = dzbuf[dzs, iz, iy, ix, core, :, lanes] + got[slot, part]
            else:
                dzbuf[dzs, iz, iy, ix, core, :, lanes] += got[slot, part]

    def stat_copies(chunk):
        copies = []
        for step in range(1, total):
            to = lax.rem(me + step, total)
            copies.append(pltpu.make_async_remote_copy(stats.at[chunk, me], stats.at[chunk, me], st_send.at[chunk, step], st_recv.at[chunk, step],
                                                       device_id=(to,), device_id_type=MESH_ID))
        return copies

    def lab_copies():
        return [pltpu.make_async_remote_copy(labs.at[me], labs.at[me], lab_send.at[step], lab_recv.at[step],
                                             device_id=(lax.rem(me + step, total),), device_id_type=MESH_ID) for step in range(1, total)]

    def label_row(chunk, part):
        lab = lab_ref[pl.ds(chunk * 2 + part, 1), :] - base
        return jnp.where(lab < vocab_rows, lab, -1)

    row_ids = lax.broadcasted_iota(jnp.int32, (VOCAB_TILE, half), 0)

    def forward_half(chunk, part):
        slot = lax.rem(chunk, 2)
        zb = zbuf[chunk, part].reshape(half, dim)
        lab = label_row(chunk, part)
        tops, sums, hits = [], [], []
        for tile in range(tiles):
            rows = slice(tile * VOCAB_TILE, (tile + 1) * VOCAB_TILE)
            logits = lax.dot_general(table_ref[rows, :], zb, COLS_DIMS, preferred_element_type=jnp.float32)
            if (tile + 1) * VOCAB_TILE > vocab_rows:
                logits = jnp.where(row_ids < vocab_rows - tile * VOCAB_TILE, logits, PAD_LOGIT)
            lbuf[slot, rows, part * half:(part + 1) * half] = logits
            top = jnp.max(logits, axis=0, keepdims=True)
            tops.append(top)
            sums.append(jnp.sum(jnp.exp(logits - top), axis=0, keepdims=True))
            hits.append(jnp.sum(jnp.where(row_ids == lab - tile * VOCAB_TILE, logits, 0.0), axis=0, keepdims=True))
        top = functools.reduce(jnp.maximum, tops)
        exp_sum = sum(s * jnp.exp(t - top) for s, t in zip(sums, tops))
        stats[chunk, me, part:part + 1, :] = top
        stats[chunk, me, 2 + part:3 + part, :] = exp_sum
        labs[me] += sum(hits)

    def combine(chunk):
        for part in range(2):
            tops = stats[chunk, :, part, :]
            top = jnp.max(tops, axis=0, keepdims=True)
            exp_sum = jnp.sum(stats[chunk, :, 2 + part, :] * jnp.exp(tops - top), axis=0, keepdims=True)
            norm[part:part + 1, :] = top
            norm[2 + part:3 + part, :] = 1.0 / exp_sum
            loss_ref[part:part + 1, :] += top + jnp.log(exp_sum)

    def table_half(chunk, which):
        slot = lax.rem(chunk, 2)
        zc = zbuf[chunk].reshape(2 * half, dim)
        for tile in range(which * tiles // 2, (which + 1) * tiles // 2):
            rows = slice(tile * VOCAB_TILE, (tile + 1) * VOCAB_TILE)
            for part in range(2):
                lanes = slice(part * half, (part + 1) * half)
                probs = jnp.exp(lbuf[slot, rows, lanes] - norm[part:part + 1, :]) * norm[2 + part:3 + part, :]
                hot = row_ids == label_row(chunk, part) - tile * VOCAB_TILE
                gbuf[rows, lanes] = jnp.where(hot, probs - 1.0, probs).astype(jnp.bfloat16)
            dtable_ref[rows, :] += jnp.dot(gbuf[rows, :], zc, preferred_element_type=jnp.float32)

    def token_half(chunk, part):
        dz = lax.dot_general(gbuf[:, part * half:(part + 1) * half], table_ref[...], ROWS_DIMS, preferred_element_type=jnp.float32)
        dzbuf[lax.rem(chunk, 3), part] = dz.reshape(2, 2, 2, UNIT, dim)

    start(gather_copies(0, 1))
    start(gather_copies(1, 1))
    start(gather_copies(2, 1))
    for chunk in range(3):
        finish(gather_copies(chunk, 1))
        start(gather_copies(chunk, 2))
    for chunk in range(2):
        finish(gather_copies(chunk, 2))
        start(gather_copies(chunk, 3))
    finish(gather_copies(0, 3))
    start(gather_copies(0, 4))
    finish(gather_copies(0, 4))

    def body(i, carry):
        def inside(offset, action):
            chunk = i + offset
            pl.when((chunk >= 0) & (chunk < chunks))(lambda: action(jnp.clip(chunk, 0, chunks - 1)))

        def step_reduce(phase, follow):
            def action(chunk):
                finish(reduce_copies(chunk, phase))
                reduce_add(chunk, phase)
                if follow:
                    start(reduce_copies(chunk, phase + 1))
            return action

        def step_gather(phase):
            def action(chunk):
                finish(gather_copies(chunk, phase))
                start(gather_copies(chunk, phase + 1))
            return action

        inside(-4, step_reduce(2, True))
        inside(-2, lambda chunk: start(reduce_copies(chunk, 0)))
        inside(1, step_gather(3))
        inside(3, lambda chunk: start(gather_copies(chunk, 1)))
        inside(2, step_gather(2))

        @pl.when(i < chunks)
        def _():
            forward_half(i, 0)
            forward_half(i, 1)

        inside(-2, step_reduce(0, False))
        inside(-3, step_reduce(1, True))
        inside(-4, step_reduce(3, False))
        inside(3, step_gather(1))
        inside(1, lambda chunk: finish(gather_copies(chunk, 4)))
        inside(-2, lambda chunk: start(reduce_copies(chunk, 1)))
        inside(0, lambda chunk: start(stat_copies(chunk)))

        @pl.when(i == chunks - 1)
        def _():
            start(lab_copies())

        def backward(chunk):
            finish(stat_copies(chunk))
            combine(chunk)
            table_half(chunk, 0)
            table_half(chunk, 1)
            token_half(chunk, 0)
            token_half(chunk, 1)

        inside(-1, backward)
        return carry

    lax.fori_loop(0, chunks + 4, body, 0)
    finish(lab_copies())
    loss_ref[2:3, :] = -jnp.sum(labs[...], axis=0)


def head(z_local, table_padded, lab_rows, vocab_rows):
    tokens, dim = z_local.shape
    chunks = tokens // UNIT
    padded = table_padded.shape[0]
    chunk_tokens = 16 * UNIT
    part_cols = dim // PARTS
    f32, bf16 = jnp.float32, jnp.bfloat16
    sems = pltpu.SemaphoreType.DMA
    vmem = pl.BlockSpec(memory_space=pltpu.VMEM)
    cost = 6 * tokens * 16 * padded * dim
    return pl.pallas_call(
        functools.partial(head_kernel, vocab_rows, chunks),
        in_specs=[pl.BlockSpec(memory_space=pl.ANY), vmem, vmem],
        out_specs=[vmem, vmem, vmem],
        out_shape=[jax.ShapeDtypeStruct((tokens, dim), f32),
                   jax.ShapeDtypeStruct((padded, dim), f32),
                   jax.ShapeDtypeStruct((3, 8 * UNIT), f32)],
        scratch_shapes=[pltpu.VMEM((chunks, 2, 2, 2, 2, UNIT, dim), bf16),
                        pltpu.VMEM((2, padded, chunk_tokens), f32),
                        pltpu.VMEM((padded, chunk_tokens), bf16),
                        pltpu.VMEM((3, 2, 2, 2, 2, UNIT, dim), f32),
                        pltpu.VMEM((2, 2, 2, 2, UNIT, dim), f32),
                        pltpu.VMEM((2, PARTS, 2, 2, UNIT, part_cols), f32),
                        pltpu.VMEM((2, PARTS, 2, UNIT, part_cols), f32),
                        pltpu.VMEM((2, PARTS, UNIT, part_cols), f32),
                        pltpu.VMEM((chunks, 16, STAT_ROWS, 8 * UNIT), f32),
                        pltpu.VMEM((16, 1, 8 * UNIT), f32),
                        pltpu.VMEM((8, 8 * UNIT), f32),
                        sems(()),
                        sems((chunks, 10)), sems((chunks, 10)),
                        sems((chunks, 10)), sems((chunks, 10)),
                        sems((chunks, 16)), sems((chunks, 16)),
                        sems((16,)), sems((16,))],
        compiler_params=pltpu.CompilerParams(vmem_limit_bytes=67043328, collective_id=1, has_side_effects=True),
        cost_estimate=pl.CostEstimate(flops=cost, bytes_accessed=4 * padded * dim, transcendentals=2 * tokens * 16 * padded),
        name="head_all",
    )(z_local.reshape(chunks, UNIT, dim), table_padded, lab_rows)


PIECES = 4


def axes(part):
    return part % 3, (part + 1) % 3, (part + 2) % 3


def cube_index(choice):
    return choice.get(2, slice(None)), choice.get(1, slice(None)), choice.get(0, slice(None))


def tail_kernel(table_rows, u_ref, acts_ref, mid_ref, gate_ref, up_ref, send_hbm, row_ref, dtable_hbm, gate_out, up_out, down_out, dtable_out,
                all_g, all_u, all_d, core_g, core_u, core_d, one_g, one_u, one_d, two_g, two_u, two_d, three_g, three_u, three_d,
                rows_got, split, local_sem, send_sem, recv_sem, row_send, row_recv):
    me = lax.axis_index('fsdp')
    total = 16
    core = lax.rem(me, 2)
    pos = [lax.rem(me // 2, 2), lax.rem(me // 4, 2), me // 8]
    core_peer = me + 1 - 2 * core
    whole = (all_g, all_u, all_d)
    gots = ((core_g, core_u, core_d), (one_g, one_u, one_d), (two_g, two_u, two_d), (three_g, three_u, three_d))
    outs = (gate_out, up_out, down_out)

    barrier = pltpu.get_barrier_semaphore()
    for step in range(1, total):
        pl.semaphore_signal(barrier, inc=1, device_id=(lax.rem(me + step, total),), device_id_type=MESH_ID)
    loads = []
    loads.append(pltpu.make_async_copy(dtable_hbm.at[pl.ds(0, table_rows)], dtable_out, local_sem.at[3]))
    loads.append(pltpu.make_async_copy(send_hbm.at[me], rows_got.at[me], local_sem.at[4]))
    for load in loads:
        load.start()
    pl.semaphore_wait(barrier, total - 1)

    def piece(part, q):
        if part == 2:
            size = all_d.shape[4] // PIECES
            return pl.ds(q * size, size), slice(None)
        size = all_g.shape[5] // PIECES
        return slice(None), pl.ds(q * size, size)

    def copies(phase, q, parts=(0, 1, 2)):
        made = []
        for part in parts:
            rows, lanes = piece(part, q)
            order = axes(part)
            if phase == 0:
                src = whole[part].at[1 - core, :, :, :, rows, lanes]
                dst = gots[0][part].at[:, :, :, rows, lanes]
                to = core_peer
            else:
                fixed = {axis: pos[axis] for axis in order[:phase - 1]}
                fixed[order[phase - 1]] = 1 - pos[order[phase - 1]]
                iz, iy, ix = cube_index(fixed)
                src = whole[part].at[core, iz, iy, ix, rows, lanes]
                lead = (slice(None),) * (3 - phase)
                dst = gots[phase][part].at[lead + (rows, lanes)]
                axis = order[phase - 1]
                to = me + (1 - 2 * pos[axis]) * (2 << axis)
            made.append(pltpu.make_async_remote_copy(src, dst, send_sem.at[phase, part, q], recv_sem.at[phase, part, q],
                                                     device_id=(to,), device_id_type=MESH_ID))
        return made

    def start(made):
        for copy in made:
            copy.start()

    def finish_add(phase, q):
        for copy in copies(phase, q):
            copy.wait()
        for part in range(3):
            rows, lanes = piece(part, q)
            iz, iy, ix = cube_index({axis: pos[axis] for axis in axes(part)[:phase]})
            got = gots[phase][part][(slice(None),) * (3 - phase) + (rows, lanes)]
            if phase == 3:
                outs[part][rows, lanes] = whole[part][core, iz, iy, ix, rows, lanes] + got
            else:
                whole[part][core, iz, iy, ix, rows, lanes] += got

    row_copies = []
    for step in range(1, total):
        to = lax.rem(me + step, total)
        row_copies.append(pltpu.make_async_remote_copy(send_hbm.at[to], rows_got.at[me], row_send.at[step], row_recv.at[step],
                                                       device_id=(to,), device_id_type=MESH_ID))
    start(row_copies)
    down_rows = all_d.shape[4]
    for chip in range(8):
        block = lax.dot_general(acts_ref[:, 2 * chip * down_rows:2 * (chip + 1) * down_rows], mid_ref[...], ROWS_DIMS,
                                preferred_element_type=jnp.float32)
        for c in range(2):
            all_d[c, chip // 4, chip // 2 % 2, chip % 2] = block[c * down_rows:(c + 1) * down_rows]
    for q in range(PIECES):
        start(copies(0, q, (2,)))
    unit, lanes = all_g.shape[4], all_g.shape[5] // PIECES
    for q in range(PIECES):
        here = slice(q * lanes, (q + 1) * lanes)
        for grads, array in ((gate_ref, all_g), (up_ref, all_u)):
            for h in range(2):
                block = lax.dot_general(u_ref[:, 8 * unit * h:8 * unit * (h + 1)], grads[:, here], ROWS_DIMS, preferred_element_type=jnp.float32)
                for k in range(8):
                    array[k % 2, h, k // 4, k // 2 % 2, :, here] = block[k * unit:(k + 1) * unit]
        start(copies(0, q, (0, 1)))
    for load in loads:
        load.wait()
    for q in range(PIECES):
        finish_add(0, q)
        start(copies(1, q))
    for copy in row_copies:
        copy.wait()
    slots, dim = rows_got.shape[0] * rows_got.shape[1], rows_got.shape[2]

    def split_rows(s, carry):
        vals = rows_got[s]
        at = pl.multiple_of(s * SLOTS, SLOTS)
        high = vals.astype(jnp.bfloat16)
        rest = vals - high.astype(jnp.float32)
        mid = rest.astype(jnp.bfloat16)
        split[pl.ds(at, SLOTS), :] = high
        split[pl.ds(slots + at, SLOTS), :] = mid
        split[pl.ds(2 * slots + at, SLOTS), :] = (rest - mid.astype(jnp.float32)).astype(jnp.bfloat16)
        return carry

    lax.fori_loop(0, total, split_rows, 0)

    def add_rows(first, count):
        ids = lax.broadcasted_iota(jnp.int32, (count, slots), 0) + first
        hot = jnp.where(ids == row_ref[...], 1.0, 0.0).astype(jnp.bfloat16)
        dtable_out[pl.ds(first, count), :] += jnp.dot(jnp.concatenate([hot, hot, hot], axis=1), split[...], preferred_element_type=jnp.float32)

    full = table_rows // VOCAB_TILE

    def add_tile(tile, carry):
        add_rows(pl.multiple_of(tile * VOCAB_TILE, VOCAB_TILE), VOCAB_TILE)
        return carry

    lax.fori_loop(0, full, add_tile, 0)
    if table_rows % VOCAB_TILE:
        add_rows(full * VOCAB_TILE, table_rows % VOCAB_TILE)

    for q in range(PIECES + 2):
        if q < PIECES:
            finish_add(1, q)
            start(copies(2, q))
        if 1 <= q <= PIECES:
            finish_add(2, q - 1)
            start(copies(3, q - 1))
        if q >= 2:
            finish_add(3, q - 2)


def tail(normed_in, acts, grad_mid, grad_gate_pre, grad_up_proj, send, row_idx, dtable, table_rows):
    f32 = jnp.float32
    vmem = pl.BlockSpec(memory_space=pltpu.VMEM)
    anywhere = pl.BlockSpec(memory_space=pl.ANY)
    sems = pltpu.SemaphoreType.DMA
    ffn = acts.shape[1]
    blocks = [(normed_in.shape[1] // 16, ffn), (normed_in.shape[1] // 16, ffn), (ffn // 16, normed_in.shape[1])]
    scratch = [pltpu.VMEM(lead + block, f32) for lead in ((2, 2, 2, 2), (2, 2, 2), (2, 2), (2,), ()) for block in blocks]
    slots = send.shape[0] * send.shape[1]
    dim = send.shape[2]
    return pl.pallas_call(
        functools.partial(tail_kernel, table_rows),
        in_specs=[vmem, vmem, vmem, vmem, vmem, anywhere, vmem, anywhere],
        out_specs=[vmem] * 4,
        out_shape=[jax.ShapeDtypeStruct(block, f32) for block in blocks] + [jax.ShapeDtypeStruct((table_rows, dim), f32)],
        scratch_shapes=scratch + [pltpu.VMEM(send.shape, f32), pltpu.VMEM((3 * slots, dim), jnp.bfloat16),
                                  sems((5,)), sems((4, 3, PIECES)), sems((4, 3, PIECES)), sems((16,)), sems((16,))],
        compiler_params=pltpu.CompilerParams(vmem_limit_bytes=67043328, collective_id=2, has_side_effects=True),
        cost_estimate=pl.CostEstimate(flops=6 * slots * table_rows * dim, bytes_accessed=40 * 1024 * 1024, transcendentals=0),
        name="tail_all",
    )(normed_in, acts, grad_mid, grad_gate_pre, grad_up_proj, send, row_idx, dtable)


def front_kernel(table_rows, pack_hbm, table_ref, gate_hbm, up_hbm, down_hbm,
                 pack_out, table_out, gate_out, up_out, down_out, x_out, slots_out, rows_out, rank_out,
                 send, got, before_ref, local_sem, id_send, id_recv, w_send, w_recv, c_send, c_recv, row_send, row_recv):
    me = lax.axis_index('fsdp')
    total = 16
    core = lax.rem(me, 2)
    pos = [lax.rem(me // 2, 2), lax.rem(me // 4, 2), me // 8]
    core_peer = me + 1 - 2 * core
    shards = (gate_hbm, up_hbm, down_hbm)
    outs = (gate_out, up_out, down_out)
    tokens = pack_out.shape[2]
    padded, dim = table_out.shape

    barrier = pltpu.get_barrier_semaphore()
    for step in range(1, total):
        pl.semaphore_signal(barrier, inc=1, device_id=(lax.rem(me + step, total),), device_id_type=MESH_ID)
    loads = [pltpu.make_async_copy(shards[part], outs[part].at[pos[2], pos[1], pos[0], core], local_sem.at[part]) for part in range(3)]
    loads.append(pltpu.make_async_copy(pack_hbm, pack_out.at[me], local_sem.at[3]))
    for load in loads:
        load.start()

    def remote(src, dst, send_sem, recv_sem, to):
        return pltpu.make_async_remote_copy(src, dst, send_sem, recv_sem, device_id=(to,), device_id_type=MESH_ID)

    def wide(phase):
        made = []
        for part in range(3):
            order = axes(part)
            iz, iy, ix = cube_index({axis: pos[axis] for axis in order[phase - 1:]})
            here = outs[part].at[iz, iy, ix, core]
            axis = order[phase - 1]
            made.append(remote(shards[part] if phase == 1 else here, here, w_send.at[phase, part], w_recv.at[phase, part],
                               me + (1 - 2 * pos[axis]) * (2 << axis)))
        return made

    def across(stage):
        made = []
        for part in range(3):
            order = axes(part)
            fixed = {axis: pos[axis] for axis in order[stage:]}
            if stage:
                fixed[order[stage - 1]] = 1 - pos[order[stage - 1]]
            iz, iy, ix = cube_index(fixed)
            here = outs[part].at[iz, iy, ix, core]
            made.append(remote(here if stage else shards[part], here, c_send.at[stage, part], c_recv.at[stage, part], core_peer))
        return made

    def id_copies():
        return [remote(pack_hbm, pack_out.at[me], id_send.at[step], id_recv.at[step], lax.rem(me + step, total)) for step in range(1, total)]

    def row_copy(step):
        to = lax.rem(me + step, total)
        return remote(send.at[to], got.at[me], row_send.at[step], row_recv.at[step], to)

    def start(made):
        for copy in made:
            copy.start()

    def finish(made):
        for copy in made:
            copy.wait()

    pl.semaphore_wait(barrier, total - 1)
    start(id_copies())
    start(wide(1))
    start(across(0))
    table_out[0:table_rows, :] = table_ref[...]
    table_out[table_rows:padded, :] = jnp.zeros((padded - table_rows, dim), table_out.dtype)
    earlier = lax.broadcasted_iota(jnp.int32, (tokens, tokens), 0) < lax.broadcasted_iota(jnp.int32, (tokens, tokens), 1)
    before_ref[...] = jnp.where(earlier, 1.0, 0.0).astype(jnp.bfloat16)
    rank_out[...] = jnp.zeros_like(rank_out)
    for load in loads:
        load.wait()
    finish(id_copies())

    lanes_iota = lax.broadcasted_iota(jnp.int32, (4 * SLOTS, padded), 1)
    slot_iota = lax.broadcasted_iota(jnp.int32, (SLOTS, tokens), 0)
    dev_iota = lax.broadcasted_iota(jnp.int32, (total, tokens), 0)

    def rank_of(to):
        ids = pack_out[to, 0:1, :]
        owner = jnp.zeros_like(ids)
        for k in range(1, total):
            owner = owner + jnp.where(ids >= k * table_rows, 1, 0)
        hot = jnp.where(dev_iota == owner, 1.0, 0.0)
        before = jnp.dot(hot.astype(jnp.bfloat16), before_ref[...], preferred_element_type=jnp.float32)
        rank = jnp.sum(hot * before, axis=0, keepdims=True)
        rank_out[...] = jnp.maximum(rank_out[...], rank)
        return ids, owner, rank.astype(jnp.int32)

    def build(group):
        columns = []
        for step in range(4 * group, 4 * group + 4):
            to = lax.rem(me + step, total)
            ids, owner, rank = rank_of(to)
            if step == 0:
                slots_out[...] = jnp.where(rank < SLOTS, owner * SLOTS + rank, -1)
            picked = jnp.where(slot_iota == jnp.where(owner == me, rank, -1), 1.0, 0.0)
            code = ids - me * table_rows + 1
            columns.append(jnp.sum(picked * code.astype(jnp.float32), axis=1, keepdims=True).astype(jnp.int32) - 1)
            high = lax.shift_right_arithmetic(code, 6)
            digits = jnp.where(owner == me, jnp.concatenate([high, code - high * 64], axis=0), 0)
            digits = jnp.concatenate([digits, jnp.zeros((6, tokens), jnp.int32)], axis=0).astype(jnp.float32).astype(jnp.bfloat16)
            spread = lax.dot_general(digits, picked.astype(jnp.bfloat16), COLS_DIMS, preferred_element_type=jnp.float32)
            rows_out[pl.ds(to, 1), :] = (spread[0:1] * 64.0 + spread[1:2]).astype(jnp.int32) - 1
        choose = jnp.where(lanes_iota == jnp.concatenate(columns, axis=0), 1.0, 0.0).astype(jnp.bfloat16)
        rows = jnp.dot(choose, table_out[...], preferred_element_type=jnp.float32).astype(jnp.bfloat16)
        for j in range(4):
            send[lax.rem(me + 4 * group + j, total)] = rows[j * SLOTS:(j + 1) * SLOTS]

    own_rows = pltpu.make_async_copy(send.at[me], got.at[me], local_sem.at[4])
    build(0)
    finish(wide(1))
    start(wide(2))
    start(across(1))
    start([row_copy(step) for step in range(1, 4)])
    build(1)
    own_rows.start()
    start([row_copy(step) for step in range(4, 8)])
    build(2)
    start([row_copy(step) for step in range(8, 12)])
    build(3)
    start([row_copy(step) for step in range(12, 16)])
    finish(wide(2))
    start(wide(3))
    start(across(2))
    own_rows.wait()
    finish([row_copy(step) for step in range(1, total)])
    place = lax.broadcasted_iota(jnp.int32, (total * SLOTS, tokens), 0) == slots_out[...]
    x_out[...] = lax.dot_general(jnp.where(place, 1.0, 0.0).astype(jnp.bfloat16), got[...].reshape(total * SLOTS, dim), ROWS_DIMS,
                                 preferred_element_type=jnp.float32).astype(jnp.bfloat16)
    finish(across(0))
    finish(across(1))
    finish(wide(3))
    start(across(3))
    finish(across(2))
    finish(across(3))


def front(packed, table_shard, gate_shard, up_shard, down_shard):
    bf16 = jnp.bfloat16
    rows, dim = table_shard.shape
    padded = -(-rows // VOCAB_TILE) * VOCAB_TILE
    tokens = packed.shape[1]
    vmem = pl.BlockSpec(memory_space=pltpu.VMEM)
    anywhere = pl.BlockSpec(memory_space=pl.ANY)
    sems = pltpu.SemaphoreType.DMA
    shards = (gate_shard, up_shard, down_shard)
    return pl.pallas_call(
        functools.partial(front_kernel, rows),
        in_specs=[anywhere, vmem, anywhere, anywhere, anywhere],
        out_specs=[vmem] * 9,
        out_shape=[jax.ShapeDtypeStruct((16,) + packed.shape, jnp.int32), jax.ShapeDtypeStruct((padded, dim), bf16)]
        + [jax.ShapeDtypeStruct((2, 2, 2, 2) + shard.shape, bf16) for shard in shards]
        + [jax.ShapeDtypeStruct((tokens, dim), bf16), jax.ShapeDtypeStruct((1, tokens), jnp.int32),
           jax.ShapeDtypeStruct((16, SLOTS), jnp.int32), jax.ShapeDtypeStruct((1, tokens), jnp.float32)],
        scratch_shapes=[pltpu.VMEM((16, SLOTS, dim), bf16), pltpu.VMEM((16, SLOTS, dim), bf16), pltpu.VMEM((tokens, tokens), bf16),
                        sems((5,)), sems((16,)), sems((16,)), sems((4, 3)), sems((4, 3)), sems((4, 3)), sems((4, 3)), sems((16,)), sems((16,))],
        compiler_params=pltpu.CompilerParams(vmem_limit_bytes=60 * 1024 * 1024, collective_id=3, has_side_effects=True),
        cost_estimate=pl.CostEstimate(flops=4 * 16 * SLOTS * padded * dim, bytes_accessed=20 * 1024 * 1024, transcendentals=0),
        name="front_all",
    )(packed, table_shard, gate_shard, up_shard, down_shard)


def split3(values):
    high = lax.reduce_precision(values, 8, 7)
    rest = values - high
    mid = lax.reduce_precision(rest, 8, 7)
    low = rest - mid
    return [part.astype(jnp.bfloat16) for part in (high, mid, low)]


def pick_rows(select, values):
    total = None
    for part in split3(values):
        term = jnp.dot(select, part, preferred_element_type=jnp.float32)
        total = term if total is None else total + term
    return total


def solution(mesh):
    groups = mesh.shape['fsdp']

    def device_step(token_ids, labels, table_shard, gate_shard, up_shard, down_shard, gain_in, gain_out):
        micro_count = token_ids.shape[0]
        tok_micro = token_ids.shape[1] * token_ids.shape[2]
        tok_dev = micro_count * tok_micro
        total_tokens = tok_dev * groups
        rows, dim = table_shard.shape
        me = lax.axis_index('fsdp')

        packed = jnp.stack([token_ids.reshape(tok_dev), labels.reshape(tok_dev)])
        gate_rows, ffn = gate_shard.shape
        down_rows = down_shard.shape[0]
        (packed_all, table_padded, w_gate, w_up, w_down, emb_rows, slots, row_idx, top_rank) = front(
            packed, table_shard, gate_shard, up_shard, down_shard)
        w_gate = w_gate.reshape(groups * gate_rows, ffn)
        w_up = w_up.reshape(groups * gate_rows, ffn)
        w_down = w_down.reshape(groups * down_rows, dim)
        rounds = jnp.max(top_rank).astype(jnp.int32) // SLOTS + 1
        slot_ids = jnp.arange(SLOTS, dtype=jnp.int32)

        def ranks(round_idx):
            ids_all, round_idx = lax.optimization_barrier((packed_all[:, 0], round_idx))
            owner = ids_all // rows
            owner_hot = owner[:, :, None] == jnp.arange(groups, dtype=jnp.int32)
            tri = jnp.tril(jnp.ones((tok_dev, tok_dev), jnp.bfloat16), -1)
            before = jnp.einsum('tu,suo->sto', tri, owner_hot.astype(jnp.bfloat16), preferred_element_type=jnp.float32)
            rank = jnp.sum(jnp.where(owner_hot, before, 0.0), axis=-1).astype(jnp.int32)
            return owner, ids_all - owner * rows, rank - round_idx * SLOTS

        def owned_rows(owner, local, rank):
            hit = (owner == me)[:, None, :] & (rank[:, None, :] == slot_ids[None, :, None])
            return (jnp.sum(jnp.where(hit, local[:, None, :] + 1, 0), axis=-1) - 1).reshape(groups * SLOTS)

        def my_slots(owner, rank):
            mine = lax.dynamic_index_in_dim(owner, me, 0, keepdims=False)
            off = lax.dynamic_index_in_dim(rank, me, 0, keepdims=False)
            return jnp.where((off >= 0) & (off < SLOTS), mine * SLOTS + off, -1)

        def slot_place(slot_row):
            return (jnp.arange(groups * SLOTS, dtype=jnp.int32)[:, None] == slot_row[None, :]).astype(jnp.bfloat16)

        def fetch_round(round_idx):
            owner, local, rank = ranks(round_idx)
            select = (owned_rows(owner, local, rank)[:, None] == jnp.arange(rows, dtype=jnp.int32)[None, :]).astype(jnp.bfloat16)
            send = jnp.dot(select, table_shard, preferred_element_type=jnp.float32).astype(jnp.bfloat16)
            got = lax.all_to_all(send.reshape(groups, SLOTS, dim), 'fsdp', 0, 0).reshape(groups * SLOTS, dim)
            place = slot_place(my_slots(owner, rank))
            return lax.dot_general(place, got, ROWS_DIMS, preferred_element_type=jnp.float32).astype(jnp.bfloat16)

        def return_round(round_idx, grad_rows):
            owner, local, rank = ranks(round_idx)
            send = pick_rows(slot_place(my_slots(owner, rank)), grad_rows)
            got = lax.all_to_all(send.reshape(groups, SLOTS, dim), 'fsdp', 0, 0).reshape(groups * SLOTS, dim)
            select = (jnp.arange(rows, dtype=jnp.int32)[:, None] == owned_rows(owner, local, rank)[None, :]).astype(jnp.bfloat16)
            return pick_rows(select, got)

        emb_rows = lax.fori_loop(1, rounds, lambda r, acc: acc + fetch_round(r), emb_rows)

        normed, saved = [], []
        for m in range(micro_count):
            out, kept = mlp_forward(emb_rows[m * tok_micro:(m + 1) * tok_micro], gain_in, gain_out, w_gate, w_up, w_down)
            normed.append(out)
            saved.append(kept)

        chunks = tok_dev // UNIT
        lab_rows = jnp.transpose(packed_all[:, 1].reshape(groups, chunks, UNIT), (1, 0, 2)).reshape(2 * chunks, groups * UNIT // 2)
        dz, dtable, loss_rows = head(jnp.concatenate(normed, axis=0), table_padded, lab_rows, rows)
        loss_total = jnp.sum(loss_rows)
        grad_normed = [dz[m * tok_micro:(m + 1) * tok_micro] for m in range(micro_count)]

        backs = [mlp_backward(saved[m], grad_normed[m], gain_in, gain_out, w_gate, w_up, w_down) for m in range(micro_count)]
        grad_rows, grad_mid, grad_gate_pre, grad_up_proj = [jnp.concatenate(parts, axis=0) for parts in zip(*backs)]
        normed_in = jnp.concatenate([kept[1] for kept in saved], axis=0)
        acts = jnp.concatenate([kept[5] for kept in saved], axis=0)
        send = pick_rows(slot_place(slots[0]), grad_rows).reshape(groups, SLOTS, dim)
        out_gate, out_up, out_down, dtable = tail(normed_in, acts, grad_mid, grad_gate_pre, grad_up_proj, send,
                                                  row_idx.reshape(1, groups * SLOTS), dtable, rows)
        dtable = lax.fori_loop(1, rounds, lambda r, acc: acc + return_round(r, grad_rows), dtable)
        return (loss_total / total_tokens, dtable, out_gate, out_up, out_down)

    row_spec = P('fsdp', None)
    tok_spec = P(None, 'fsdp', None)
    return jax.shard_map(device_step, mesh=mesh,
                         in_specs=(tok_spec, tok_spec, row_spec, row_spec, row_spec, row_spec, P(), P()),
                         out_specs=(P(), row_spec, row_spec, row_spec, row_spec), check_vma=False)
```

```python
import functools
import jax
import jax.numpy as jnp
from jax import lax
from jax.experimental import pallas as pl
from jax.experimental.pallas import tpu as pltpu
from jax.sharding import PartitionSpec as P

NORM_EPS = 1e-6
SLOTS = 64


def rms_scale(values, gain_vec):
    vals32 = values.astype(jnp.float32)
    inv_rms = lax.rsqrt(jnp.mean(vals32 * vals32, axis=-1, keepdims=True) + NORM_EPS)
    return (vals32 * inv_rms * gain_vec).astype(jnp.bfloat16), inv_rms


def rms_back(values, inv_rms, gain_vec, grad_out):
    vals32 = values.astype(jnp.float32)
    scaled = grad_out * gain_vec
    proj_mean = jnp.mean(scaled * vals32, axis=-1, keepdims=True)
    return inv_rms * scaled - vals32 * (inv_rms * inv_rms * inv_rms) * proj_mean


def mlp_forward(emb_rows, gain_in, gain_out, w_gate, w_up, w_down):
    normed_in, inv_in = rms_scale(emb_rows, gain_in)
    gate_pre = jnp.dot(normed_in, w_gate, preferred_element_type=jnp.float32).astype(jnp.bfloat16)
    up_proj = jnp.dot(normed_in, w_up, preferred_element_type=jnp.float32).astype(jnp.bfloat16)
    acts = (jax.nn.silu(gate_pre.astype(jnp.float32)) * up_proj.astype(jnp.float32)).astype(jnp.bfloat16)
    mlp_out = jnp.dot(acts, w_down, preferred_element_type=jnp.float32).astype(jnp.bfloat16)
    hidden = (emb_rows.astype(jnp.float32) + mlp_out.astype(jnp.float32)).astype(jnp.bfloat16)
    normed_out, inv_out = rms_scale(hidden, gain_out)
    return normed_out, (emb_rows, normed_in, inv_in, gate_pre, up_proj, acts, hidden, inv_out)


COLS_DIMS = (((1,), (1,)), ((), ()))
ROWS_DIMS = (((0,), (0,)), ((), ()))


def mlp_backward(saved, grad_normed, gain_in, gain_out, w_gate, w_up, w_down):
    emb_rows, normed_in, inv_in, gate_pre, up_proj, acts, hidden, inv_out = saved
    grad_hidden = rms_back(hidden, inv_out, gain_out, grad_normed)
    grad_mid = grad_hidden.astype(jnp.bfloat16)
    grad_acts = lax.dot_general(grad_mid, w_down, COLS_DIMS, preferred_element_type=jnp.float32)
    gate32 = gate_pre.astype(jnp.float32)
    gate_sig = jax.nn.sigmoid(gate32)
    grad_gate_pre = (grad_acts * up_proj.astype(jnp.float32) * gate_sig * (1.0 + gate32 * (1.0 - gate_sig))).astype(jnp.bfloat16)
    grad_up_proj = (grad_acts * gate32 * gate_sig).astype(jnp.bfloat16)
    grad_normed_in = (lax.dot_general(grad_gate_pre, w_gate, COLS_DIMS, preferred_element_type=jnp.float32)
                      + lax.dot_general(grad_up_proj, w_up, COLS_DIMS, preferred_element_type=jnp.float32))
    grad_rows = grad_hidden + rms_back(emb_rows, inv_in, gain_in, grad_normed_in)
    return grad_rows, grad_mid, grad_gate_pre, grad_up_proj


UNIT = 64
CUBE_BITS = 3
PARTS = 3
VOCAB_TILE = 256
STAT_ROWS = 2
MESH_ID = pl.DeviceIdType.MESH
PAD_LOGIT = -1e30


def head_kernel(vocab_rows, chunks, z_hbm, table_ref, lab_ref, dz_ref, dtable_ref, loss_ref,
                zbuf, lbuf, gbuf, dzbuf, got_core, got_one, got_two, got_three, stats, labs, norm, loss_acc,
                local_sem, ag_send, ag_recv, rs_send, rs_recv, st_send, st_recv, lab_send, lab_recv):
    me = lax.axis_index('fsdp')
    total = 16
    core = lax.rem(me, 2)
    pos = [lax.rem(me // 2, 2), lax.rem(me // 4, 2), me // 8]
    base = me * vocab_rows
    padded, dim = table_ref.shape
    part_cols = dim // PARTS
    half = 8 * UNIT
    tiles = padded // VOCAB_TILE

    def peer(axis):
        return me + (1 - 2 * pos[axis]) * (2 << axis)

    core_peer = me + 1 - 2 * core

    barrier = pltpu.get_barrier_semaphore()
    for step in range(1, total):
        pl.semaphore_signal(barrier, inc=1, device_id=(lax.rem(me + step, total),), device_id_type=MESH_ID)
    own = pltpu.make_async_copy(z_hbm, zbuf.at[:, pos[2], pos[1], pos[0], core], local_sem)
    own.start()
    dtable_ref[...] = jnp.zeros_like(dtable_ref)
    loss_acc[...] = jnp.zeros_like(loss_acc)
    labs[me] = jnp.zeros((1, half), jnp.float32)
    own.wait()
    pl.semaphore_wait(barrier, total - 1)

    def where(choice):
        return choice.get(2, slice(None)), choice.get(1, slice(None)), choice.get(0, slice(None))

    def axes(part):
        return part % 3, (part + 1) % 3, (part + 2) % 3

    def cols(part):
        return pl.ds(part * part_cols, part_cols)

    def gather_copies(chunk, phase):
        if phase == 4:
            here = zbuf.at[chunk, :, :, :, core]
            return [pltpu.make_async_remote_copy(here, here, ag_send.at[chunk, 9], ag_recv.at[chunk, 9],
                                                 device_id=(core_peer,), device_id_type=MESH_ID)]
        copies = []
        for part in range(PARTS):
            order = axes(part)
            fixed = {axis: pos[axis] for axis in order[phase - 1:]}
            iz, iy, ix = where(fixed)
            here = zbuf.at[chunk, iz, iy, ix, core, :, cols(part)]
            sem = (phase - 1) * PARTS + part
            copies.append(pltpu.make_async_remote_copy(here, here, ag_send.at[chunk, sem], ag_recv.at[chunk, sem],
                                                       device_id=(peer(order[phase - 1]),), device_id_type=MESH_ID))
        return copies

    def reduce_copies(chunk, phase):
        slot, dzs = lax.rem(chunk, 2), lax.rem(chunk, 3)
        if phase == 0:
            return [pltpu.make_async_remote_copy(dzbuf.at[dzs, :, :, :, 1 - core], got_core.at[slot], rs_send.at[chunk, 9], rs_recv.at[chunk, 9],
                                                 device_id=(core_peer,), device_id_type=MESH_ID)]
        copies = []
        for part in range(PARTS):
            order = axes(part)
            fixed = {axis: pos[axis] for axis in order[:phase - 1]}
            fixed[order[phase - 1]] = 1 - pos[order[phase - 1]]
            iz, iy, ix = where(fixed)
            got = (got_one, got_two, got_three)[phase - 1]
            sem = (phase - 1) * PARTS + part
            copies.append(pltpu.make_async_remote_copy(dzbuf.at[dzs, iz, iy, ix, core, :, cols(part)], got.at[slot, part],
                                                       rs_send.at[chunk, sem], rs_recv.at[chunk, sem],
                                                       device_id=(peer(order[phase - 1]),), device_id_type=MESH_ID))
        return copies

    def start(copies):
        for copy in copies:
            copy.start()

    def finish(copies):
        for copy in copies:
            copy.wait()

    def reduce_add(chunk, phase):
        slot, dzs = lax.rem(chunk, 2), lax.rem(chunk, 3)
        if phase == 0:
            dzbuf[dzs, :, :, :, core] += got_core[slot]
            return
        for part in range(PARTS):
            order = axes(part)
            iz, iy, ix = where({axis: pos[axis] for axis in order[:phase]})
            got = (got_one, got_two, got_three)[phase - 1]
            lanes = slice(part * part_cols, (part + 1) * part_cols)
            if phase == 3:
                rows = pl.ds(pl.multiple_of(chunk * UNIT, UNIT), UNIT)
                dz_ref[rows, lanes] = dzbuf[dzs, iz, iy, ix, core, :, lanes] + got[slot, part]
            else:
                dzbuf[dzs, iz, iy, ix, core, :, lanes] += got[slot, part]

    def stat_copies(chunk):
        copies = []
        for step in range(1, total):
            to = lax.rem(me + step, total)
            copies.append(pltpu.make_async_remote_copy(stats.at[chunk, me], stats.at[chunk, me], st_send.at[chunk, step], st_recv.at[chunk, step],
                                                       device_id=(to,), device_id_type=MESH_ID))
        return copies

    def lab_copies():
        return [pltpu.make_async_remote_copy(labs.at[me], labs.at[me], lab_send.at[step], lab_recv.at[step],
                                             device_id=(lax.rem(me + step, total),), device_id_type=MESH_ID) for step in range(1, total)]

    def label_row(chunk, part):
        lab = lab_ref[pl.ds(chunk * 2 + part, 1), :] - base
        return jnp.where(lab < vocab_rows, lab, -1)

    row_ids = lax.broadcasted_iota(jnp.int32, (VOCAB_TILE, half), 0)

    def forward_half(chunk, part):
        slot = lax.rem(chunk, 2)
        zb = zbuf[chunk, part].reshape(half, dim)
        lab = label_row(chunk, part)
        tops, sums, hits = [], [], []
        for tile in range(tiles):
            rows = slice(tile * VOCAB_TILE, (tile + 1) * VOCAB_TILE)
            logits = lax.dot_general(table_ref[rows, :], zb, COLS_DIMS, preferred_element_type=jnp.float32)
            if (tile + 1) * VOCAB_TILE > vocab_rows:
                logits = jnp.where(row_ids < vocab_rows - tile * VOCAB_TILE, logits, PAD_LOGIT)
            lbuf[slot, rows, part * half:(part + 1) * half] = logits
            top = jnp.max(logits, axis=0, keepdims=True)
            tops.append(top)
            sums.append(jnp.sum(jnp.exp(logits - top), axis=0, keepdims=True))
            hits.append(jnp.sum(jnp.where(row_ids == lab - tile * VOCAB_TILE, logits, 0.0), axis=0, keepdims=True))
        top = functools.reduce(jnp.maximum, tops)
        exp_sum = sum(s * jnp.exp(t - top) for s, t in zip(sums, tops))
        stats[chunk, me, part:part + 1, :] = top + jnp.log(exp_sum)
        labs[me] += sum(hits)

    def combine(chunk):
        for part in range(2):
            tops = stats[chunk, :, part, :]
            top = jnp.max(tops, axis=0, keepdims=True)
            exp_sum = jnp.sum(jnp.exp(tops - top), axis=0, keepdims=True)
            norm[part:part + 1, :] = top
            norm[2 + part:3 + part, :] = 1.0 / exp_sum
            loss_acc[...] += top + jnp.log(exp_sum)

    def table_half(chunk, which):
        slot = lax.rem(chunk, 2)
        zc = zbuf[chunk].reshape(2 * half, dim)
        for tile in range(which * tiles // 2, (which + 1) * tiles // 2):
            rows = slice(tile * VOCAB_TILE, (tile + 1) * VOCAB_TILE)
            for part in range(2):
                lanes = slice(part * half, (part + 1) * half)
                probs = jnp.exp(lbuf[slot, rows, lanes] - norm[part:part + 1, :]) * norm[2 + part:3 + part, :]
                hot = row_ids == label_row(chunk, part) - tile * VOCAB_TILE
                gbuf[rows, lanes] = jnp.where(hot, probs - 1.0, probs).astype(jnp.bfloat16)
            dtable_ref[rows, :] += jnp.dot(gbuf[rows, :], zc, preferred_element_type=jnp.float32)

    def token_half(chunk, part):
        dz = lax.dot_general(gbuf[:, part * half:(part + 1) * half], table_ref[...], ROWS_DIMS, preferred_element_type=jnp.float32)
        dzbuf[lax.rem(chunk, 3), part] = dz.reshape(2, 2, 2, UNIT, dim)

    start(gather_copies(0, 1))
    start(gather_copies(1, 1))
    start(gather_copies(2, 1))
    for chunk in range(3):
        finish(gather_copies(chunk, 1))
        start(gather_copies(chunk, 2))
    for chunk in range(2):
        finish(gather_copies(chunk, 2))
        start(gather_copies(chunk, 3))
    finish(gather_copies(0, 3))
    start(gather_copies(0, 4))
    finish(gather_copies(0, 4))

    def body(i, carry):
        def inside(offset, action):
            chunk = i + offset
            pl.when((chunk >= 0) & (chunk < chunks))(lambda: action(jnp.clip(chunk, 0, chunks - 1)))

        def step_reduce(phase, follow):
            def action(chunk):
                finish(reduce_copies(chunk, phase))
                reduce_add(chunk, phase)
                if follow:
                    start(reduce_copies(chunk, phase + 1))
            return action

        def step_gather(phase):
            def action(chunk):
                finish(gather_copies(chunk, phase))
                start(gather_copies(chunk, phase + 1))
            return action

        inside(-4, step_reduce(2, True))
        inside(-2, lambda chunk: start(reduce_copies(chunk, 0)))
        inside(1, step_gather(3))
        inside(3, lambda chunk: start(gather_copies(chunk, 1)))
        inside(2, step_gather(2))

        @pl.when(i < chunks)
        def _():
            forward_half(i, 0)
            forward_half(i, 1)

        inside(-2, step_reduce(0, False))
        inside(-3, step_reduce(1, True))
        inside(-4, step_reduce(3, False))
        inside(3, step_gather(1))
        inside(1, lambda chunk: finish(gather_copies(chunk, 4)))
        inside(-2, lambda chunk: start(reduce_copies(chunk, 1)))
        inside(0, lambda chunk: start(stat_copies(chunk)))

        @pl.when(i == chunks - 1)
        def _():
            start(lab_copies())

        def backward(chunk):
            finish(stat_copies(chunk))
            combine(chunk)
            table_half(chunk, 0)
            table_half(chunk, 1)
            token_half(chunk, 0)
            token_half(chunk, 1)

        inside(-1, backward)
        return carry

    lax.fori_loop(0, chunks + 4, body, 0)
    finish(lab_copies())
    loss_ref[...] = jnp.broadcast_to(jnp.sum(loss_acc[...] - jnp.sum(labs[...], axis=0), axis=1, keepdims=True), loss_ref.shape)


def head(z_local, table_padded, lab_rows, vocab_rows):
    tokens, dim = z_local.shape
    chunks = tokens // UNIT
    padded = table_padded.shape[0]
    chunk_tokens = 16 * UNIT
    part_cols = dim // PARTS
    f32, bf16 = jnp.float32, jnp.bfloat16
    sems = pltpu.SemaphoreType.DMA
    vmem = pl.BlockSpec(memory_space=pltpu.VMEM)
    cost = 6 * tokens * 16 * padded * dim
    return pl.pallas_call(
        functools.partial(head_kernel, vocab_rows, chunks),
        in_specs=[pl.BlockSpec(memory_space=pl.ANY), vmem, vmem],
        out_specs=[vmem, vmem, vmem],
        out_shape=[jax.ShapeDtypeStruct((tokens, dim), f32),
                   jax.ShapeDtypeStruct((padded, dim), f32),
                   jax.ShapeDtypeStruct((1, 128), f32)],
        scratch_shapes=[pltpu.VMEM((chunks, 2, 2, 2, 2, UNIT, dim), bf16),
                        pltpu.VMEM((2, padded, chunk_tokens), f32),
                        pltpu.VMEM((padded, chunk_tokens), bf16),
                        pltpu.VMEM((3, 2, 2, 2, 2, UNIT, dim), f32),
                        pltpu.VMEM((2, 2, 2, 2, UNIT, dim), f32),
                        pltpu.VMEM((2, PARTS, 2, 2, UNIT, part_cols), f32),
                        pltpu.VMEM((2, PARTS, 2, UNIT, part_cols), f32),
                        pltpu.VMEM((2, PARTS, UNIT, part_cols), f32),
                        pltpu.VMEM((chunks, 16, STAT_ROWS, 8 * UNIT), f32),
                        pltpu.VMEM((16, 1, 8 * UNIT), f32),
                        pltpu.VMEM((8, 8 * UNIT), f32),
                        pltpu.VMEM((1, 8 * UNIT), f32),
                        sems(()),
                        sems((chunks, 10)), sems((chunks, 10)),
                        sems((chunks, 10)), sems((chunks, 10)),
                        sems((chunks, 16)), sems((chunks, 16)),
                        sems((16,)), sems((16,))],
        compiler_params=pltpu.CompilerParams(vmem_limit_bytes=67043328, collective_id=1, has_side_effects=True),
        cost_estimate=pl.CostEstimate(flops=cost, bytes_accessed=4 * padded * dim, transcendentals=2 * tokens * 16 * padded),
        name="head_all",
    )(z_local.reshape(chunks, UNIT, dim), table_padded, lab_rows)


PIECES = 4


def axes(part):
    return part % 3, (part + 1) % 3, (part + 2) % 3


def cube_index(choice):
    return choice.get(2, slice(None)), choice.get(1, slice(None)), choice.get(0, slice(None))


def tail_kernel(table_rows, u_ref, acts_ref, mid_ref, gate_ref, up_ref, send_hbm, row_ref, dtable_hbm, gate_out, up_out, down_out, dtable_out,
                all_g, all_u, all_d, core_g, core_u, core_d, one_g, one_u, one_d, two_g, two_u, two_d, three_g, three_u, three_d,
                rows_got, split, local_sem, send_sem, recv_sem, row_send, row_recv):
    me = lax.axis_index('fsdp')
    total = 16
    core = lax.rem(me, 2)
    pos = [lax.rem(me // 2, 2), lax.rem(me // 4, 2), me // 8]
    core_peer = me + 1 - 2 * core
    whole = (all_g, all_u, all_d)
    gots = ((core_g, core_u, core_d), (one_g, one_u, one_d), (two_g, two_u, two_d), (three_g, three_u, three_d))
    outs = (gate_out, up_out, down_out)

    barrier = pltpu.get_barrier_semaphore()
    for step in range(1, total):
        pl.semaphore_signal(barrier, inc=1, device_id=(lax.rem(me + step, total),), device_id_type=MESH_ID)
    loads = []
    loads.append(pltpu.make_async_copy(dtable_hbm.at[pl.ds(0, table_rows)], dtable_out, local_sem.at[3]))
    loads.append(pltpu.make_async_copy(send_hbm.at[me], rows_got.at[me], local_sem.at[4]))
    for load in loads:
        load.start()
    pl.semaphore_wait(barrier, total - 1)

    def piece(part, q):
        if part == 2:
            size = all_d.shape[4] // PIECES
            return pl.ds(q * size, size), slice(None)
        size = all_g.shape[5] // PIECES
        return slice(None), pl.ds(q * size, size)

    def copies(phase, q, parts=(0, 1, 2)):
        made = []
        for part in parts:
            rows, lanes = piece(part, q)
            order = axes(part)
            if phase == 0:
                src = whole[part].at[1 - core, :, :, :, rows, lanes]
                dst = gots[0][part].at[:, :, :, rows, lanes]
                to = core_peer
            else:
                fixed = {axis: pos[axis] for axis in order[:phase - 1]}
                fixed[order[phase - 1]] = 1 - pos[order[phase - 1]]
                iz, iy, ix = cube_index(fixed)
                src = whole[part].at[core, iz, iy, ix, rows, lanes]
                lead = (slice(None),) * (3 - phase)
                dst = gots[phase][part].at[lead + (rows, lanes)]
                axis = order[phase - 1]
                to = me + (1 - 2 * pos[axis]) * (2 << axis)
            made.append(pltpu.make_async_remote_copy(src, dst, send_sem.at[phase, part, q], recv_sem.at[phase, part, q],
                                                     device_id=(to,), device_id_type=MESH_ID))
        return made

    def start(made):
        for copy in made:
            copy.start()

    def finish_add(phase, q):
        for copy in copies(phase, q):
            copy.wait()
        for part in range(3):
            rows, lanes = piece(part, q)
            iz, iy, ix = cube_index({axis: pos[axis] for axis in axes(part)[:phase]})
            got = gots[phase][part][(slice(None),) * (3 - phase) + (rows, lanes)]
            if phase == 3:
                outs[part][rows, lanes] = whole[part][core, iz, iy, ix, rows, lanes] + got
            else:
                whole[part][core, iz, iy, ix, rows, lanes] += got

    row_copies = []
    for step in range(1, total):
        to = lax.rem(me + step, total)
        row_copies.append(pltpu.make_async_remote_copy(send_hbm.at[to], rows_got.at[me], row_send.at[step], row_recv.at[step],
                                                       device_id=(to,), device_id_type=MESH_ID))
    start(row_copies)
    down_rows = all_d.shape[4]
    for chip in range(8):
        block = lax.dot_general(acts_ref[:, 2 * chip * down_rows:2 * (chip + 1) * down_rows], mid_ref[...], ROWS_DIMS,
                                preferred_element_type=jnp.float32)
        for c in range(2):
            all_d[c, chip // 4, chip // 2 % 2, chip % 2] = block[c * down_rows:(c + 1) * down_rows]
    for q in range(PIECES):
        start(copies(0, q, (2,)))
    unit, lanes = all_g.shape[4], all_g.shape[5] // PIECES
    for q in range(PIECES):
        here = slice(q * lanes, (q + 1) * lanes)
        for grads, array in ((gate_ref, all_g), (up_ref, all_u)):
            for h in range(2):
                block = lax.dot_general(u_ref[:, 8 * unit * h:8 * unit * (h + 1)], grads[:, here], ROWS_DIMS, preferred_element_type=jnp.float32)
                for k in range(8):
                    array[k % 2, h, k // 4, k // 2 % 2, :, here] = block[k * unit:(k + 1) * unit]
        start(copies(0, q, (0, 1)))
    for load in loads:
        load.wait()
    for q in range(PIECES):
        finish_add(0, q)
        start(copies(1, q))
    for copy in row_copies:
        copy.wait()
    slots, dim = rows_got.shape[0] * rows_got.shape[1], rows_got.shape[2]

    def split_rows(s, carry):
        vals = rows_got[s]
        at = pl.multiple_of(s * SLOTS, SLOTS)
        high = vals.astype(jnp.bfloat16)
        rest = vals - high.astype(jnp.float32)
        mid = rest.astype(jnp.bfloat16)
        split[pl.ds(at, SLOTS), :] = high
        split[pl.ds(slots + at, SLOTS), :] = mid
        split[pl.ds(2 * slots + at, SLOTS), :] = (rest - mid.astype(jnp.float32)).astype(jnp.bfloat16)
        return carry

    lax.fori_loop(0, total, split_rows, 0)

    def add_rows(first, count):
        ids = lax.broadcasted_iota(jnp.int32, (count, slots), 0) + first
        hot = jnp.where(ids == row_ref[...], 1.0, 0.0).astype(jnp.bfloat16)
        dtable_out[pl.ds(first, count), :] += jnp.dot(jnp.concatenate([hot, hot, hot], axis=1), split[...], preferred_element_type=jnp.float32)

    full = table_rows // VOCAB_TILE

    def add_tile(tile, carry):
        add_rows(pl.multiple_of(tile * VOCAB_TILE, VOCAB_TILE), VOCAB_TILE)
        return carry

    lax.fori_loop(0, full, add_tile, 0)
    if table_rows % VOCAB_TILE:
        add_rows(full * VOCAB_TILE, table_rows % VOCAB_TILE)

    for q in range(PIECES + 2):
        if q < PIECES:
            finish_add(1, q)
            start(copies(2, q))
        if 1 <= q <= PIECES:
            finish_add(2, q - 1)
            start(copies(3, q - 1))
        if q >= 2:
            finish_add(3, q - 2)


def tail(normed_in, acts, grad_mid, grad_gate_pre, grad_up_proj, send, row_idx, dtable, table_rows):
    f32 = jnp.float32
    vmem = pl.BlockSpec(memory_space=pltpu.VMEM)
    anywhere = pl.BlockSpec(memory_space=pl.ANY)
    sems = pltpu.SemaphoreType.DMA
    ffn = acts.shape[1]
    blocks = [(normed_in.shape[1] // 16, ffn), (normed_in.shape[1] // 16, ffn), (ffn // 16, normed_in.shape[1])]
    scratch = [pltpu.VMEM(lead + block, f32) for lead in ((2, 2, 2, 2), (2, 2, 2), (2, 2), (2,), ()) for block in blocks]
    slots = send.shape[0] * send.shape[1]
    dim = send.shape[2]
    return pl.pallas_call(
        functools.partial(tail_kernel, table_rows),
        in_specs=[vmem, vmem, vmem, vmem, vmem, anywhere, vmem, anywhere],
        out_specs=[vmem] * 4,
        out_shape=[jax.ShapeDtypeStruct(block, f32) for block in blocks] + [jax.ShapeDtypeStruct((table_rows, dim), f32)],
        scratch_shapes=scratch + [pltpu.VMEM(send.shape, f32), pltpu.VMEM((3 * slots, dim), jnp.bfloat16),
                                  sems((5,)), sems((4, 3, PIECES)), sems((4, 3, PIECES)), sems((16,)), sems((16,))],
        compiler_params=pltpu.CompilerParams(vmem_limit_bytes=67043328, collective_id=2, has_side_effects=True),
        cost_estimate=pl.CostEstimate(flops=6 * slots * table_rows * dim, bytes_accessed=40 * 1024 * 1024, transcendentals=0),
        name="tail_all",
    )(normed_in, acts, grad_mid, grad_gate_pre, grad_up_proj, send, row_idx, dtable)


def front_kernel(table_rows, pack_hbm, table_ref, gate_hbm, up_hbm, down_hbm,
                 pack_out, table_out, gate_out, up_out, down_out, x_out, slots_out, rows_out, rank_out,
                 send, got, before_ref, rank_top, local_sem, id_send, id_recv, w_send, w_recv, c_send, c_recv, row_send, row_recv):
    me = lax.axis_index('fsdp')
    total = 16
    core = lax.rem(me, 2)
    pos = [lax.rem(me // 2, 2), lax.rem(me // 4, 2), me // 8]
    core_peer = me + 1 - 2 * core
    shards = (gate_hbm, up_hbm, down_hbm)
    outs = (gate_out, up_out, down_out)
    tokens = pack_out.shape[2]
    padded, dim = table_out.shape

    barrier = pltpu.get_barrier_semaphore()
    for step in range(1, total):
        pl.semaphore_signal(barrier, inc=1, device_id=(lax.rem(me + step, total),), device_id_type=MESH_ID)
    loads = [pltpu.make_async_copy(shards[part], outs[part].at[pos[2], pos[1], pos[0], core], local_sem.at[part]) for part in range(3)]
    loads.append(pltpu.make_async_copy(pack_hbm, pack_out.at[me], local_sem.at[3]))
    for load in loads:
        load.start()

    def remote(src, dst, send_sem, recv_sem, to):
        return pltpu.make_async_remote_copy(src, dst, send_sem, recv_sem, device_id=(to,), device_id_type=MESH_ID)

    def wide(phase):
        made = []
        for part in range(3):
            order = axes(part)
            iz, iy, ix = cube_index({axis: pos[axis] for axis in order[phase - 1:]})
            here = outs[part].at[iz, iy, ix, core]
            axis = order[phase - 1]
            made.append(remote(shards[part] if phase == 1 else here, here, w_send.at[phase, part], w_recv.at[phase, part],
                               me + (1 - 2 * pos[axis]) * (2 << axis)))
        return made

    def across(stage):
        made = []
        for part in range(3):
            order = axes(part)
            fixed = {axis: pos[axis] for axis in order[stage:]}
            if stage:
                fixed[order[stage - 1]] = 1 - pos[order[stage - 1]]
            iz, iy, ix = cube_index(fixed)
            here = outs[part].at[iz, iy, ix, core]
            made.append(remote(here if stage else shards[part], here, c_send.at[stage, part], c_recv.at[stage, part], core_peer))
        return made

    def id_copies():
        return [remote(pack_hbm, pack_out.at[me], id_send.at[step], id_recv.at[step], lax.rem(me + step, total)) for step in range(1, total)]

    def row_copy(step):
        to = lax.rem(me + step, total)
        return remote(send.at[to], got.at[me], row_send.at[step], row_recv.at[step], to)

    def start(made):
        for copy in made:
            copy.start()

    def finish(made):
        for copy in made:
            copy.wait()

    pl.semaphore_wait(barrier, total - 1)
    start(id_copies())
    start(wide(1))
    start(across(0))
    table_out[0:table_rows, :] = table_ref[...]
    table_out[table_rows:padded, :] = jnp.zeros((padded - table_rows, dim), table_out.dtype)
    earlier = lax.broadcasted_iota(jnp.int32, (tokens, tokens), 0) < lax.broadcasted_iota(jnp.int32, (tokens, tokens), 1)
    before_ref[...] = jnp.where(earlier, 1.0, 0.0).astype(jnp.bfloat16)
    rank_top[...] = jnp.zeros_like(rank_top)
    for load in loads:
        load.wait()
    finish(id_copies())

    lanes_iota = lax.broadcasted_iota(jnp.int32, (4 * SLOTS, padded), 1)
    slot_iota = lax.broadcasted_iota(jnp.int32, (SLOTS, tokens), 0)
    dev_iota = lax.broadcasted_iota(jnp.int32, (total, tokens), 0)

    def rank_of(to):
        ids = pack_out[to, 0:1, :]
        owner = jnp.zeros_like(ids)
        for k in range(1, total):
            owner = owner + jnp.where(ids >= k * table_rows, 1, 0)
        hot = jnp.where(dev_iota == owner, 1.0, 0.0)
        before = jnp.dot(hot.astype(jnp.bfloat16), before_ref[...], preferred_element_type=jnp.float32)
        rank = jnp.sum(hot * before, axis=0, keepdims=True)
        rank_top[...] = jnp.maximum(rank_top[...], rank)
        return ids, owner, rank.astype(jnp.int32)

    def build(group):
        columns = []
        for step in range(4 * group, 4 * group + 4):
            to = lax.rem(me + step, total)
            ids, owner, rank = rank_of(to)
            if step == 0:
                slots_out[...] = jnp.where(rank < SLOTS, owner * SLOTS + rank, -1)
            picked = jnp.where(slot_iota == jnp.where(owner == me, rank, -1), 1.0, 0.0)
            code = ids - me * table_rows + 1
            columns.append(jnp.sum(picked * code.astype(jnp.float32), axis=1, keepdims=True).astype(jnp.int32) - 1)
            high = lax.shift_right_arithmetic(code, 6)
            digits = jnp.where(owner == me, jnp.concatenate([high, code - high * 64], axis=0), 0)
            digits = jnp.concatenate([digits, jnp.zeros((6, tokens), jnp.int32)], axis=0).astype(jnp.float32).astype(jnp.bfloat16)
            spread = lax.dot_general(digits, picked.astype(jnp.bfloat16), COLS_DIMS, preferred_element_type=jnp.float32)
            rows_out[pl.ds(to, 1), :] = (spread[0:1] * 64.0 + spread[1:2]).astype(jnp.int32) - 1
        choose = jnp.where(lanes_iota == jnp.concatenate(columns, axis=0), 1.0, 0.0).astype(jnp.bfloat16)
        rows = jnp.dot(choose, table_out[...], preferred_element_type=jnp.float32).astype(jnp.bfloat16)
        for j in range(4):
            send[lax.rem(me + 4 * group + j, total)] = rows[j * SLOTS:(j + 1) * SLOTS]

    own_rows = pltpu.make_async_copy(send.at[me], got.at[me], local_sem.at[4])
    build(0)
    finish(wide(1))
    start(wide(2))
    start(across(1))
    start([row_copy(step) for step in range(1, 4)])
    build(1)
    own_rows.start()
    start([row_copy(step) for step in range(4, 8)])
    build(2)
    start([row_copy(step) for step in range(8, 12)])
    build(3)
    rank_out[...] = jnp.broadcast_to(jnp.max(rank_top[...], axis=1, keepdims=True), rank_out.shape).astype(jnp.int32)
    start([row_copy(step) for step in range(12, 16)])
    finish(wide(2))
    start(wide(3))
    start(across(2))
    own_rows.wait()
    finish([row_copy(step) for step in range(1, total)])
    place = lax.broadcasted_iota(jnp.int32, (total * SLOTS, tokens), 0) == slots_out[...]
    x_out[...] = lax.dot_general(jnp.where(place, 1.0, 0.0).astype(jnp.bfloat16), got[...].reshape(total * SLOTS, dim), ROWS_DIMS,
                                 preferred_element_type=jnp.float32).astype(jnp.bfloat16)
    finish(across(0))
    finish(across(1))
    finish(wide(3))
    start(across(3))
    finish(across(2))
    finish(across(3))


def front(packed, table_shard, gate_shard, up_shard, down_shard):
    bf16 = jnp.bfloat16
    rows, dim = table_shard.shape
    padded = -(-rows // VOCAB_TILE) * VOCAB_TILE
    tokens = packed.shape[1]
    vmem = pl.BlockSpec(memory_space=pltpu.VMEM)
    anywhere = pl.BlockSpec(memory_space=pl.ANY)
    sems = pltpu.SemaphoreType.DMA
    shards = (gate_shard, up_shard, down_shard)
    return pl.pallas_call(
        functools.partial(front_kernel, rows),
        in_specs=[anywhere, vmem, anywhere, anywhere, anywhere],
        out_specs=[vmem] * 9,
        out_shape=[jax.ShapeDtypeStruct((16,) + packed.shape, jnp.int32), jax.ShapeDtypeStruct((padded, dim), bf16)]
        + [jax.ShapeDtypeStruct((2, 2, 2, 2) + shard.shape, bf16) for shard in shards]
        + [jax.ShapeDtypeStruct((tokens, dim), bf16), jax.ShapeDtypeStruct((1, tokens), jnp.int32),
           jax.ShapeDtypeStruct((16, SLOTS), jnp.int32), jax.ShapeDtypeStruct((1, 128), jnp.int32)],
        scratch_shapes=[pltpu.VMEM((16, SLOTS, dim), bf16), pltpu.VMEM((16, SLOTS, dim), bf16), pltpu.VMEM((tokens, tokens), bf16), pltpu.VMEM((1, tokens), jnp.float32),
                        sems((5,)), sems((16,)), sems((16,)), sems((4, 3)), sems((4, 3)), sems((4, 3)), sems((4, 3)), sems((16,)), sems((16,))],
        compiler_params=pltpu.CompilerParams(vmem_limit_bytes=60 * 1024 * 1024, collective_id=3, has_side_effects=True),
        cost_estimate=pl.CostEstimate(flops=4 * 16 * SLOTS * padded * dim, bytes_accessed=20 * 1024 * 1024, transcendentals=0),
        name="front_all",
    )(packed, table_shard, gate_shard, up_shard, down_shard)


def split3(values):
    high = lax.reduce_precision(values, 8, 7)
    rest = values - high
    mid = lax.reduce_precision(rest, 8, 7)
    low = rest - mid
    return [part.astype(jnp.bfloat16) for part in (high, mid, low)]


def pick_rows(select, values):
    total = None
    for part in split3(values):
        term = jnp.dot(select, part, preferred_element_type=jnp.float32)
        total = term if total is None else total + term
    return total


def solution(mesh):
    groups = mesh.shape['fsdp']

    def device_step(token_ids, labels, table_shard, gate_shard, up_shard, down_shard, gain_in, gain_out):
        micro_count = token_ids.shape[0]
        tok_micro = token_ids.shape[1] * token_ids.shape[2]
        tok_dev = micro_count * tok_micro
        total_tokens = tok_dev * groups
        rows, dim = table_shard.shape
        me = lax.axis_index('fsdp')

        packed = jnp.stack([token_ids.reshape(tok_dev), labels.reshape(tok_dev)])
        gate_rows, ffn = gate_shard.shape
        down_rows = down_shard.shape[0]
        (packed_all, table_padded, w_gate, w_up, w_down, emb_rows, slots, row_idx, top_rank) = front(
            packed, table_shard, gate_shard, up_shard, down_shard)
        w_gate = w_gate.reshape(groups * gate_rows, ffn)
        w_up = w_up.reshape(groups * gate_rows, ffn)
        w_down = w_down.reshape(groups * down_rows, dim)
        rounds = top_rank[0, 0] // SLOTS + 1
        slot_ids = jnp.arange(SLOTS, dtype=jnp.int32)

        def ranks(round_idx):
            ids_all, round_idx = lax.optimization_barrier((packed_all[:, 0], round_idx))
            owner = ids_all // rows
            owner_hot = owner[:, :, None] == jnp.arange(groups, dtype=jnp.int32)
            tri = jnp.tril(jnp.ones((tok_dev, tok_dev), jnp.bfloat16), -1)
            before = jnp.einsum('tu,suo->sto', tri, owner_hot.astype(jnp.bfloat16), preferred_element_type=jnp.float32)
            rank = jnp.sum(jnp.where(owner_hot, before, 0.0), axis=-1).astype(jnp.int32)
            return owner, ids_all - owner * rows, rank - round_idx * SLOTS

        def owned_rows(owner, local, rank):
            hit = (owner == me)[:, None, :] & (rank[:, None, :] == slot_ids[None, :, None])
            return (jnp.sum(jnp.where(hit, local[:, None, :] + 1, 0), axis=-1) - 1).reshape(groups * SLOTS)

        def my_slots(owner, rank):
            mine = lax.dynamic_index_in_dim(owner, me, 0, keepdims=False)
            off = lax.dynamic_index_in_dim(rank, me, 0, keepdims=False)
            return jnp.where((off >= 0) & (off < SLOTS), mine * SLOTS + off, -1)

        def slot_place(slot_row):
            return (jnp.arange(groups * SLOTS, dtype=jnp.int32)[:, None] == slot_row[None, :]).astype(jnp.bfloat16)

        def fetch_round(round_idx):
            owner, local, rank = ranks(round_idx)
            select = (owned_rows(owner, local, rank)[:, None] == jnp.arange(rows, dtype=jnp.int32)[None, :]).astype(jnp.bfloat16)
            send = jnp.dot(select, table_shard, preferred_element_type=jnp.float32).astype(jnp.bfloat16)
            got = lax.all_to_all(send.reshape(groups, SLOTS, dim), 'fsdp', 0, 0).reshape(groups * SLOTS, dim)
            place = slot_place(my_slots(owner, rank))
            return lax.dot_general(place, got, ROWS_DIMS, preferred_element_type=jnp.float32).astype(jnp.bfloat16)

        def return_round(round_idx, grad_rows):
            owner, local, rank = ranks(round_idx)
            send = pick_rows(slot_place(my_slots(owner, rank)), grad_rows)
            got = lax.all_to_all(send.reshape(groups, SLOTS, dim), 'fsdp', 0, 0).reshape(groups * SLOTS, dim)
            select = (jnp.arange(rows, dtype=jnp.int32)[:, None] == owned_rows(owner, local, rank)[None, :]).astype(jnp.bfloat16)
            return pick_rows(select, got)

        emb_rows = lax.fori_loop(1, rounds, lambda r, acc: acc + fetch_round(r), emb_rows)

        normed_out, saved = mlp_forward(emb_rows, gain_in, gain_out, w_gate, w_up, w_down)
        chunks = tok_dev // UNIT
        lab_rows = jnp.transpose(packed_all[:, 1].reshape(groups, chunks, UNIT), (1, 0, 2)).reshape(2 * chunks, groups * UNIT // 2)
        dz, dtable, loss_rows = head(normed_out, table_padded, lab_rows, rows)
        loss_total = loss_rows[0, 0]
        grad_rows, grad_mid, grad_gate_pre, grad_up_proj = mlp_backward(saved, dz, gain_in, gain_out, w_gate, w_up, w_down)
        normed_in, acts = saved[1], saved[5]
        send = pick_rows(slot_place(slots[0]), grad_rows).reshape(groups, SLOTS, dim)
        out_gate, out_up, out_down, dtable = tail(normed_in, acts, grad_mid, grad_gate_pre, grad_up_proj, send,
                                                  row_idx.reshape(1, groups * SLOTS), dtable, rows)
        dtable = lax.fori_loop(1, rounds, lambda r, acc: acc + return_round(r, grad_rows), dtable)
        return (loss_total / total_tokens, dtable, out_gate, out_up, out_down)

    row_spec = P('fsdp', None)
    tok_spec = P(None, 'fsdp', None)
    return jax.shard_map(device_step, mesh=mesh,
                         in_specs=(tok_spec, tok_spec, row_spec, row_spec, row_spec, row_spec, P(), P()),
                         out_specs=(P(), row_spec, row_spec, row_spec, row_spec), check_vma=False)
```

```python
import functools
import jax
import jax.numpy as jnp
from jax import lax
from jax.experimental import pallas as pl
from jax.experimental.pallas import tpu as pltpu
from jax.sharding import PartitionSpec as P

NORM_EPS = 1e-6
SLOTS = 64
BACK_SLOTS = 56


def rms_scale(values, gain_vec):
    vals32 = values.astype(jnp.float32)
    inv_rms = lax.rsqrt(jnp.mean(vals32 * vals32, axis=-1, keepdims=True) + NORM_EPS)
    return (vals32 * inv_rms * gain_vec).astype(jnp.bfloat16), inv_rms


def rms_back(values, inv_rms, gain_vec, grad_out):
    vals32 = values.astype(jnp.float32)
    scaled = grad_out * gain_vec
    proj_mean = jnp.mean(scaled * vals32, axis=-1, keepdims=True)
    return inv_rms * scaled - vals32 * (inv_rms * inv_rms * inv_rms) * proj_mean


def mlp_forward(emb_rows, gain_in, gain_out, w_gate, w_up, w_down):
    normed_in, inv_in = rms_scale(emb_rows, gain_in)
    gate_pre = jnp.dot(normed_in, w_gate, preferred_element_type=jnp.float32).astype(jnp.bfloat16)
    up_proj = jnp.dot(normed_in, w_up, preferred_element_type=jnp.float32).astype(jnp.bfloat16)
    acts = (jax.nn.silu(gate_pre.astype(jnp.float32)) * up_proj.astype(jnp.float32)).astype(jnp.bfloat16)
    mlp_out = jnp.dot(acts, w_down, preferred_element_type=jnp.float32).astype(jnp.bfloat16)
    hidden = (emb_rows.astype(jnp.float32) + mlp_out.astype(jnp.float32)).astype(jnp.bfloat16)
    normed_out, inv_out = rms_scale(hidden, gain_out)
    return normed_out, (emb_rows, normed_in, inv_in, gate_pre, up_proj, acts, hidden, inv_out)


COLS_DIMS = (((1,), (1,)), ((), ()))
ROWS_DIMS = (((0,), (0,)), ((), ()))


def mlp_backward(saved, grad_normed, gain_in, gain_out, w_gate, w_up, w_down):
    emb_rows, normed_in, inv_in, gate_pre, up_proj, acts, hidden, inv_out = saved
    grad_hidden = rms_back(hidden, inv_out, gain_out, grad_normed)
    grad_mid = grad_hidden.astype(jnp.bfloat16)
    grad_acts = lax.dot_general(grad_mid, w_down, COLS_DIMS, preferred_element_type=jnp.float32)
    gate32 = gate_pre.astype(jnp.float32)
    gate_sig = jax.nn.sigmoid(gate32)
    grad_gate_pre = (grad_acts * up_proj.astype(jnp.float32) * gate_sig * (1.0 + gate32 * (1.0 - gate_sig))).astype(jnp.bfloat16)
    grad_up_proj = (grad_acts * gate32 * gate_sig).astype(jnp.bfloat16)
    grad_normed_in = (lax.dot_general(grad_gate_pre, w_gate, COLS_DIMS, preferred_element_type=jnp.float32)
                      + lax.dot_general(grad_up_proj, w_up, COLS_DIMS, preferred_element_type=jnp.float32))
    grad_rows = grad_hidden + rms_back(emb_rows, inv_in, gain_in, grad_normed_in)
    return grad_rows, grad_mid, grad_gate_pre, grad_up_proj


UNIT = 64
CUBE_BITS = 3
PARTS = 3
VOCAB_TILE = 256
STAT_ROWS = 2
MESH_ID = pl.DeviceIdType.MESH
PAD_LOGIT = -1e30


def head_kernel(vocab_rows, chunks, z_hbm, table_ref, lab_ref, dz_ref, dtable_ref, loss_ref,
                zbuf, lbuf, gbuf, dzbuf, got_core, got_one, got_two, got_three, stats, labs, norm, loss_acc,
                local_sem, ag_send, ag_recv, rs_send, rs_recv, st_send, st_recv, lab_send, lab_recv):
    me = lax.axis_index('fsdp')
    total = 16
    core = lax.rem(me, 2)
    pos = [lax.rem(me // 2, 2), lax.rem(me // 4, 2), me // 8]
    base = me * vocab_rows
    padded, dim = table_ref.shape
    part_cols = dim // PARTS
    half = 8 * UNIT
    tiles = padded // VOCAB_TILE

    def peer(axis):
        return me + (1 - 2 * pos[axis]) * (2 << axis)

    core_peer = me + 1 - 2 * core

    barrier = pltpu.get_barrier_semaphore()
    for step in range(1, total):
        pl.semaphore_signal(barrier, inc=1, device_id=(lax.rem(me + step, total),), device_id_type=MESH_ID)
    own = pltpu.make_async_copy(z_hbm, zbuf.at[:, pos[2], pos[1], pos[0], core], local_sem)
    own.start()
    dtable_ref[...] = jnp.zeros_like(dtable_ref)
    loss_acc[...] = jnp.zeros_like(loss_acc)
    labs[me] = jnp.zeros((1, half), jnp.float32)
    own.wait()
    pl.semaphore_wait(barrier, total - 1)

    def where(choice):
        return choice.get(2, slice(None)), choice.get(1, slice(None)), choice.get(0, slice(None))

    def axes(part):
        return part % 3, (part + 1) % 3, (part + 2) % 3

    def cols(part):
        return pl.ds(part * part_cols, part_cols)

    def gather_copies(chunk, phase):
        if phase == 4:
            here = zbuf.at[chunk, :, :, :, core]
            return [pltpu.make_async_remote_copy(here, here, ag_send.at[chunk, 9], ag_recv.at[chunk, 9],
                                                 device_id=(core_peer,), device_id_type=MESH_ID)]
        copies = []
        for part in range(PARTS):
            order = axes(part)
            fixed = {axis: pos[axis] for axis in order[phase - 1:]}
            iz, iy, ix = where(fixed)
            here = zbuf.at[chunk, iz, iy, ix, core, :, cols(part)]
            sem = (phase - 1) * PARTS + part
            copies.append(pltpu.make_async_remote_copy(here, here, ag_send.at[chunk, sem], ag_recv.at[chunk, sem],
                                                       device_id=(peer(order[phase - 1]),), device_id_type=MESH_ID))
        return copies

    def reduce_copies(chunk, phase):
        slot, dzs = lax.rem(chunk, 2), lax.rem(chunk, 3)
        if phase == 0:
            return [pltpu.make_async_remote_copy(dzbuf.at[dzs, :, :, :, 1 - core], got_core.at[slot], rs_send.at[chunk, 9], rs_recv.at[chunk, 9],
                                                 device_id=(core_peer,), device_id_type=MESH_ID)]
        copies = []
        for part in range(PARTS):
            order = axes(part)
            fixed = {axis: pos[axis] for axis in order[:phase - 1]}
            fixed[order[phase - 1]] = 1 - pos[order[phase - 1]]
            iz, iy, ix = where(fixed)
            got = (got_one, got_two, got_three)[phase - 1]
            sem = (phase - 1) * PARTS + part
            copies.append(pltpu.make_async_remote_copy(dzbuf.at[dzs, iz, iy, ix, core, :, cols(part)], got.at[slot, part],
                                                       rs_send.at[chunk, sem], rs_recv.at[chunk, sem],
                                                       device_id=(peer(order[phase - 1]),), device_id_type=MESH_ID))
        return copies

    def start(copies):
        for copy in copies:
            copy.start()

    def finish(copies):
        for copy in copies:
            copy.wait()

    def reduce_add(chunk, phase):
        slot, dzs = lax.rem(chunk, 2), lax.rem(chunk, 3)
        if phase == 0:
            dzbuf[dzs, :, :, :, core] += got_core[slot]
            return
        for part in range(PARTS):
            order = axes(part)
            iz, iy, ix = where({axis: pos[axis] for axis in order[:phase]})
            got = (got_one, got_two, got_three)[phase - 1]
            lanes = slice(part * part_cols, (part + 1) * part_cols)
            if phase == 3:
                rows = pl.ds(pl.multiple_of(chunk * UNIT, UNIT), UNIT)
                dz_ref[rows, lanes] = dzbuf[dzs, iz, iy, ix, core, :, lanes] + got[slot, part]
            else:
                dzbuf[dzs, iz, iy, ix, core, :, lanes] += got[slot, part]

    def stat_copies(chunk):
        copies = []
        for step in range(1, total):
            to = lax.rem(me + step, total)
            copies.append(pltpu.make_async_remote_copy(stats.at[chunk, me], stats.at[chunk, me], st_send.at[chunk, step], st_recv.at[chunk, step],
                                                       device_id=(to,), device_id_type=MESH_ID))
        return copies

    def lab_copies():
        return [pltpu.make_async_remote_copy(labs.at[me], labs.at[me], lab_send.at[step], lab_recv.at[step],
                                             device_id=(lax.rem(me + step, total),), device_id_type=MESH_ID) for step in range(1, total)]

    def label_row(chunk, part):
        lab = lab_ref[pl.ds(chunk * 2 + part, 1), :] - base
        return jnp.where(lab < vocab_rows, lab, -1)

    row_ids = lax.broadcasted_iota(jnp.int32, (VOCAB_TILE, half), 0)

    def forward_half(chunk, part):
        slot = lax.rem(chunk, 2)
        zb = zbuf[chunk, part].reshape(half, dim)
        lab = label_row(chunk, part)
        tops, sums, hits = [], [], []
        for tile in range(tiles):
            rows = slice(tile * VOCAB_TILE, (tile + 1) * VOCAB_TILE)
            logits = lax.dot_general(table_ref[rows, :], zb, COLS_DIMS, preferred_element_type=jnp.float32)
            if (tile + 1) * VOCAB_TILE > vocab_rows:
                logits = jnp.where(row_ids < vocab_rows - tile * VOCAB_TILE, logits, PAD_LOGIT)
            lbuf[slot, rows, part * half:(part + 1) * half] = logits
            top = jnp.max(logits, axis=0, keepdims=True)
            tops.append(top)
            sums.append(jnp.sum(jnp.exp(logits - top), axis=0, keepdims=True))
            hits.append(jnp.sum(jnp.where(row_ids == lab - tile * VOCAB_TILE, logits, 0.0), axis=0, keepdims=True))
        top = functools.reduce(jnp.maximum, tops)
        exp_sum = sum(s * jnp.exp(t - top) for s, t in zip(sums, tops))
        stats[chunk, me, part:part + 1, :] = top + jnp.log(exp_sum)
        labs[me] += sum(hits)

    def combine(chunk):
        for part in range(2):
            tops = stats[chunk, :, part, :]
            top = jnp.max(tops, axis=0, keepdims=True)
            exp_sum = jnp.sum(jnp.exp(tops - top), axis=0, keepdims=True)
            norm[part:part + 1, :] = top
            norm[2 + part:3 + part, :] = 1.0 / exp_sum
            loss_acc[...] += top + jnp.log(exp_sum)

    def table_half(chunk, which):
        slot = lax.rem(chunk, 2)
        zc = zbuf[chunk].reshape(2 * half, dim)
        for tile in range(which * tiles // 2, (which + 1) * tiles // 2):
            rows = slice(tile * VOCAB_TILE, (tile + 1) * VOCAB_TILE)
            for part in range(2):
                lanes = slice(part * half, (part + 1) * half)
                probs = jnp.exp(lbuf[slot, rows, lanes] - norm[part:part + 1, :]) * norm[2 + part:3 + part, :]
                hot = row_ids == label_row(chunk, part) - tile * VOCAB_TILE
                gbuf[rows, lanes] = jnp.where(hot, probs - 1.0, probs).astype(jnp.bfloat16)
            dtable_ref[rows, :] += jnp.dot(gbuf[rows, :], zc, preferred_element_type=jnp.float32)

    def token_half(chunk, part):
        dz = lax.dot_general(gbuf[:, part * half:(part + 1) * half], table_ref[...], ROWS_DIMS, preferred_element_type=jnp.float32)
        dzbuf[lax.rem(chunk, 3), part] = dz.reshape(2, 2, 2, UNIT, dim)

    start(gather_copies(0, 1))
    start(gather_copies(1, 1))
    start(gather_copies(2, 1))
    for chunk in range(3):
        finish(gather_copies(chunk, 1))
        start(gather_copies(chunk, 2))
    for chunk in range(2):
        finish(gather_copies(chunk, 2))
        start(gather_copies(chunk, 3))
    finish(gather_copies(0, 3))
    start(gather_copies(0, 4))
    finish(gather_copies(0, 4))

    def body(i, carry):
        def inside(offset, action):
            chunk = i + offset
            pl.when((chunk >= 0) & (chunk < chunks))(lambda: action(jnp.clip(chunk, 0, chunks - 1)))

        def step_reduce(phase, follow):
            def action(chunk):
                finish(reduce_copies(chunk, phase))
                reduce_add(chunk, phase)
                if follow:
                    start(reduce_copies(chunk, phase + 1))
            return action

        def step_gather(phase):
            def action(chunk):
                finish(gather_copies(chunk, phase))
                start(gather_copies(chunk, phase + 1))
            return action

        inside(-4, step_reduce(2, True))
        inside(-2, lambda chunk: start(reduce_copies(chunk, 0)))
        inside(1, step_gather(3))
        inside(3, lambda chunk: start(gather_copies(chunk, 1)))
        inside(2, step_gather(2))

        @pl.when(i < chunks)
        def _():
            forward_half(i, 0)
            forward_half(i, 1)

        inside(-2, step_reduce(0, False))
        inside(-3, step_reduce(1, True))
        inside(-4, step_reduce(3, False))
        inside(3, step_gather(1))
        inside(1, lambda chunk: finish(gather_copies(chunk, 4)))
        inside(-2, lambda chunk: start(reduce_copies(chunk, 1)))
        inside(0, lambda chunk: start(stat_copies(chunk)))

        @pl.when(i == chunks - 1)
        def _():
            start(lab_copies())

        def backward(chunk):
            finish(stat_copies(chunk))
            combine(chunk)
            table_half(chunk, 0)
            table_half(chunk, 1)
            token_half(chunk, 0)
            token_half(chunk, 1)

        inside(-1, backward)
        return carry

    lax.fori_loop(0, chunks + 4, body, 0)
    finish(lab_copies())
    loss_ref[...] = jnp.broadcast_to(jnp.sum(loss_acc[...] - jnp.sum(labs[...], axis=0), axis=1, keepdims=True), loss_ref.shape)


def head(z_local, table_padded, lab_rows, vocab_rows):
    tokens, dim = z_local.shape
    chunks = tokens // UNIT
    padded = table_padded.shape[0]
    chunk_tokens = 16 * UNIT
    part_cols = dim // PARTS
    f32, bf16 = jnp.float32, jnp.bfloat16
    sems = pltpu.SemaphoreType.DMA
    vmem = pl.BlockSpec(memory_space=pltpu.VMEM)
    cost = 6 * tokens * 16 * padded * dim
    return pl.pallas_call(
        functools.partial(head_kernel, vocab_rows, chunks),
        in_specs=[pl.BlockSpec(memory_space=pl.ANY), vmem, vmem],
        out_specs=[vmem, vmem, vmem],
        out_shape=[jax.ShapeDtypeStruct((tokens, dim), f32),
                   jax.ShapeDtypeStruct((padded, dim), f32),
                   jax.ShapeDtypeStruct((1, 128), f32)],
        scratch_shapes=[pltpu.VMEM((chunks, 2, 2, 2, 2, UNIT, dim), bf16),
                        pltpu.VMEM((2, padded, chunk_tokens), f32),
                        pltpu.VMEM((padded, chunk_tokens), bf16),
                        pltpu.VMEM((3, 2, 2, 2, 2, UNIT, dim), f32),
                        pltpu.VMEM((2, 2, 2, 2, UNIT, dim), f32),
                        pltpu.VMEM((2, PARTS, 2, 2, UNIT, part_cols), f32),
                        pltpu.VMEM((2, PARTS, 2, UNIT, part_cols), f32),
                        pltpu.VMEM((2, PARTS, UNIT, part_cols), f32),
                        pltpu.VMEM((chunks, 16, STAT_ROWS, 8 * UNIT), f32),
                        pltpu.VMEM((16, 1, 8 * UNIT), f32),
                        pltpu.VMEM((8, 8 * UNIT), f32),
                        pltpu.VMEM((1, 8 * UNIT), f32),
                        sems(()),
                        sems((chunks, 10)), sems((chunks, 10)),
                        sems((chunks, 10)), sems((chunks, 10)),
                        sems((chunks, 16)), sems((chunks, 16)),
                        sems((16,)), sems((16,))],
        compiler_params=pltpu.CompilerParams(vmem_limit_bytes=67043328, collective_id=1, has_side_effects=True),
        cost_estimate=pl.CostEstimate(flops=cost, bytes_accessed=4 * padded * dim, transcendentals=2 * tokens * 16 * padded),
        name="head_all",
    )(z_local.reshape(chunks, UNIT, dim), table_padded, lab_rows)


PIECES = 4


def axes(part):
    return part % 3, (part + 1) % 3, (part + 2) % 3


def cube_index(choice):
    return choice.get(2, slice(None)), choice.get(1, slice(None)), choice.get(0, slice(None))


def tail_kernel(table_rows, u_ref, acts_ref, mid_ref, gate_ref, up_ref, send_hbm, row_ref, dtable_hbm, gate_out, up_out, down_out, dtable_out,
                all_g, all_u, all_d, core_g, core_u, core_d, one_g, one_u, one_d, two_g, two_u, two_d, three_g, three_u, three_d,
                rows_got, split, local_sem, send_sem, recv_sem, row_send, row_recv):
    me = lax.axis_index('fsdp')
    total = 16
    core = lax.rem(me, 2)
    pos = [lax.rem(me // 2, 2), lax.rem(me // 4, 2), me // 8]
    core_peer = me + 1 - 2 * core
    whole = (all_g, all_u, all_d)
    gots = ((core_g, core_u, core_d), (one_g, one_u, one_d), (two_g, two_u, two_d), (three_g, three_u, three_d))
    outs = (gate_out, up_out, down_out)

    barrier = pltpu.get_barrier_semaphore()
    for step in range(1, total):
        pl.semaphore_signal(barrier, inc=1, device_id=(lax.rem(me + step, total),), device_id_type=MESH_ID)
    loads = []
    loads.append(pltpu.make_async_copy(dtable_hbm.at[pl.ds(0, table_rows)], dtable_out, local_sem.at[3]))
    loads.append(pltpu.make_async_copy(send_hbm.at[me], rows_got.at[me], local_sem.at[4]))
    for load in loads:
        load.start()
    pl.semaphore_wait(barrier, total - 1)

    def piece(part, q):
        if part == 2:
            size = all_d.shape[4] // PIECES
            return pl.ds(q * size, size), slice(None)
        size = all_g.shape[5] // PIECES
        return slice(None), pl.ds(q * size, size)

    def copies(phase, q, parts=(0, 1, 2)):
        made = []
        for part in parts:
            rows, lanes = piece(part, q)
            order = axes(part)
            if phase == 0:
                src = whole[part].at[1 - core, :, :, :, rows, lanes]
                dst = gots[0][part].at[:, :, :, rows, lanes]
                to = core_peer
            else:
                fixed = {axis: pos[axis] for axis in order[:phase - 1]}
                fixed[order[phase - 1]] = 1 - pos[order[phase - 1]]
                iz, iy, ix = cube_index(fixed)
                src = whole[part].at[core, iz, iy, ix, rows, lanes]
                lead = (slice(None),) * (3 - phase)
                dst = gots[phase][part].at[lead + (rows, lanes)]
                axis = order[phase - 1]
                to = me + (1 - 2 * pos[axis]) * (2 << axis)
            made.append(pltpu.make_async_remote_copy(src, dst, send_sem.at[phase, part, q], recv_sem.at[phase, part, q],
                                                     device_id=(to,), device_id_type=MESH_ID))
        return made

    def start(made):
        for copy in made:
            copy.start()

    def finish_add(phase, q):
        for copy in copies(phase, q):
            copy.wait()
        for part in range(3):
            rows, lanes = piece(part, q)
            iz, iy, ix = cube_index({axis: pos[axis] for axis in axes(part)[:phase]})
            got = gots[phase][part][(slice(None),) * (3 - phase) + (rows, lanes)]
            if phase == 3:
                outs[part][rows, lanes] = whole[part][core, iz, iy, ix, rows, lanes] + got
            else:
                whole[part][core, iz, iy, ix, rows, lanes] += got

    row_copies = []
    for step in range(1, total):
        to = lax.rem(me + step, total)
        row_copies.append(pltpu.make_async_remote_copy(send_hbm.at[to], rows_got.at[me], row_send.at[step], row_recv.at[step],
                                                       device_id=(to,), device_id_type=MESH_ID))
    start(row_copies)
    down_rows = all_d.shape[4]
    for chip in range(8):
        block = lax.dot_general(acts_ref[:, 2 * chip * down_rows:2 * (chip + 1) * down_rows], mid_ref[...], ROWS_DIMS,
                                preferred_element_type=jnp.float32)
        for c in range(2):
            all_d[c, chip // 4, chip // 2 % 2, chip % 2] = block[c * down_rows:(c + 1) * down_rows]
    for q in range(PIECES):
        start(copies(0, q, (2,)))
    unit, lanes = all_g.shape[4], all_g.shape[5] // PIECES
    for q in range(PIECES):
        here = slice(q * lanes, (q + 1) * lanes)
        for grads, array in ((gate_ref, all_g), (up_ref, all_u)):
            for h in range(2):
                block = lax.dot_general(u_ref[:, 8 * unit * h:8 * unit * (h + 1)], grads[:, here], ROWS_DIMS, preferred_element_type=jnp.float32)
                for k in range(8):
                    array[k % 2, h, k // 4, k // 2 % 2, :, here] = block[k * unit:(k + 1) * unit]
        start(copies(0, q, (0, 1)))
    for load in loads:
        load.wait()
    for q in range(PIECES):
        finish_add(0, q)
        start(copies(1, q))
    for copy in row_copies:
        copy.wait()
    slots, dim = rows_got.shape[0] * rows_got.shape[1], rows_got.shape[2]

    pair = 2 * rows_got.shape[1]

    def split_rows(s, carry):
        vals = rows_got[pl.ds(2 * s, 2)].reshape(pair, dim)
        at = pl.multiple_of(s * pair, pair)
        high = vals.astype(jnp.bfloat16)
        rest = vals - high.astype(jnp.float32)
        mid = rest.astype(jnp.bfloat16)
        split[pl.ds(at, pair), :] = high
        split[pl.ds(slots + at, pair), :] = mid
        split[pl.ds(2 * slots + at, pair), :] = (rest - mid.astype(jnp.float32)).astype(jnp.bfloat16)
        return carry

    lax.fori_loop(0, total // 2, split_rows, 0)

    def add_rows(first, count):
        ids = lax.broadcasted_iota(jnp.int32, (count, slots), 0) + first
        hot = jnp.where(ids == row_ref[...], 1.0, 0.0).astype(jnp.bfloat16)
        dtable_out[pl.ds(first, count), :] += jnp.dot(jnp.concatenate([hot, hot, hot], axis=1), split[...], preferred_element_type=jnp.float32)

    full = table_rows // VOCAB_TILE

    def add_tile(tile, carry):
        add_rows(pl.multiple_of(tile * VOCAB_TILE, VOCAB_TILE), VOCAB_TILE)
        return carry

    lax.fori_loop(0, full, add_tile, 0)
    if table_rows % VOCAB_TILE:
        add_rows(full * VOCAB_TILE, table_rows % VOCAB_TILE)

    for q in range(PIECES + 2):
        if q < PIECES:
            finish_add(1, q)
            start(copies(2, q))
        if 1 <= q <= PIECES:
            finish_add(2, q - 1)
            start(copies(3, q - 1))
        if q >= 2:
            finish_add(3, q - 2)


def tail(normed_in, acts, grad_mid, grad_gate_pre, grad_up_proj, send, row_idx, dtable, table_rows):
    f32 = jnp.float32
    vmem = pl.BlockSpec(memory_space=pltpu.VMEM)
    anywhere = pl.BlockSpec(memory_space=pl.ANY)
    sems = pltpu.SemaphoreType.DMA
    ffn = acts.shape[1]
    blocks = [(normed_in.shape[1] // 16, ffn), (normed_in.shape[1] // 16, ffn), (ffn // 16, normed_in.shape[1])]
    scratch = [pltpu.VMEM(lead + block, f32) for lead in ((2, 2, 2, 2), (2, 2, 2), (2, 2), (2,), ()) for block in blocks]
    slots = send.shape[0] * send.shape[1]
    dim = send.shape[2]
    return pl.pallas_call(
        functools.partial(tail_kernel, table_rows),
        in_specs=[vmem, vmem, vmem, vmem, vmem, anywhere, vmem, anywhere],
        out_specs=[vmem] * 4,
        out_shape=[jax.ShapeDtypeStruct(block, f32) for block in blocks] + [jax.ShapeDtypeStruct((table_rows, dim), f32)],
        scratch_shapes=scratch + [pltpu.VMEM(send.shape, f32), pltpu.VMEM((3 * slots, dim), jnp.bfloat16),
                                  sems((5,)), sems((4, 3, PIECES)), sems((4, 3, PIECES)), sems((16,)), sems((16,))],
        compiler_params=pltpu.CompilerParams(vmem_limit_bytes=67043328, collective_id=2, has_side_effects=True),
        cost_estimate=pl.CostEstimate(flops=6 * slots * table_rows * dim, bytes_accessed=40 * 1024 * 1024, transcendentals=0),
        name="tail_all",
    )(normed_in, acts, grad_mid, grad_gate_pre, grad_up_proj, send, row_idx, dtable)


def front_kernel(table_rows, pack_hbm, table_ref, gate_hbm, up_hbm, down_hbm,
                 pack_out, table_out, gate_out, up_out, down_out, x_out, slots_out, rows_out, rank_out,
                 send, got, before_ref, rank_top, local_sem, id_send, id_recv, w_send, w_recv, c_send, c_recv, row_send, row_recv):
    me = lax.axis_index('fsdp')
    total = 16
    core = lax.rem(me, 2)
    pos = [lax.rem(me // 2, 2), lax.rem(me // 4, 2), me // 8]
    core_peer = me + 1 - 2 * core
    shards = (gate_hbm, up_hbm, down_hbm)
    outs = (gate_out, up_out, down_out)
    tokens = pack_out.shape[2]
    padded, dim = table_out.shape

    barrier = pltpu.get_barrier_semaphore()
    for step in range(1, total):
        pl.semaphore_signal(barrier, inc=1, device_id=(lax.rem(me + step, total),), device_id_type=MESH_ID)
    loads = [pltpu.make_async_copy(shards[part], outs[part].at[pos[2], pos[1], pos[0], core], local_sem.at[part]) for part in range(3)]
    loads.append(pltpu.make_async_copy(pack_hbm, pack_out.at[me], local_sem.at[3]))
    for load in loads:
        load.start()

    def remote(src, dst, send_sem, recv_sem, to):
        return pltpu.make_async_remote_copy(src, dst, send_sem, recv_sem, device_id=(to,), device_id_type=MESH_ID)

    def wide(phase):
        made = []
        for part in range(3):
            order = axes(part)
            iz, iy, ix = cube_index({axis: pos[axis] for axis in order[phase - 1:]})
            here = outs[part].at[iz, iy, ix, core]
            axis = order[phase - 1]
            made.append(remote(shards[part] if phase == 1 else here, here, w_send.at[phase, part], w_recv.at[phase, part],
                               me + (1 - 2 * pos[axis]) * (2 << axis)))
        return made

    def across(stage):
        made = []
        for part in range(3):
            order = axes(part)
            fixed = {axis: pos[axis] for axis in order[stage:]}
            if stage:
                fixed[order[stage - 1]] = 1 - pos[order[stage - 1]]
            iz, iy, ix = cube_index(fixed)
            here = outs[part].at[iz, iy, ix, core]
            made.append(remote(here if stage else shards[part], here, c_send.at[stage, part], c_recv.at[stage, part], core_peer))
        return made

    def id_copies():
        return [remote(pack_hbm, pack_out.at[me], id_send.at[step], id_recv.at[step], lax.rem(me + step, total)) for step in range(1, total)]

    def row_copy(step):
        to = lax.rem(me + step, total)
        return remote(send.at[to], got.at[me], row_send.at[step], row_recv.at[step], to)

    def start(made):
        for copy in made:
            copy.start()

    def finish(made):
        for copy in made:
            copy.wait()

    pl.semaphore_wait(barrier, total - 1)
    start(id_copies())
    start(wide(1))
    start(across(0))
    table_out[0:table_rows, :] = table_ref[...]
    table_out[table_rows:padded, :] = jnp.zeros((padded - table_rows, dim), table_out.dtype)
    earlier = lax.broadcasted_iota(jnp.int32, (tokens, tokens), 0) < lax.broadcasted_iota(jnp.int32, (tokens, tokens), 1)
    before_ref[...] = jnp.where(earlier, 1.0, 0.0).astype(jnp.bfloat16)
    rank_top[...] = jnp.zeros_like(rank_top)
    for load in loads:
        load.wait()
    finish(id_copies())

    lanes_iota = lax.broadcasted_iota(jnp.int32, (4 * SLOTS, padded), 1)
    slot_iota = lax.broadcasted_iota(jnp.int32, (SLOTS, tokens), 0)
    dev_iota = lax.broadcasted_iota(jnp.int32, (total, tokens), 0)

    def rank_of(to):
        ids = pack_out[to, 0:1, :]
        owner = jnp.zeros_like(ids)
        for k in range(1, total):
            owner = owner + jnp.where(ids >= k * table_rows, 1, 0)
        hot = jnp.where(dev_iota == owner, 1.0, 0.0)
        before = jnp.dot(hot.astype(jnp.bfloat16), before_ref[...], preferred_element_type=jnp.float32)
        rank = jnp.sum(hot * before, axis=0, keepdims=True)
        rank_top[...] = jnp.maximum(rank_top[...], rank)
        return ids, owner, rank.astype(jnp.int32)

    def build(group):
        columns = []
        for step in range(4 * group, 4 * group + 4):
            to = lax.rem(me + step, total)
            ids, owner, rank = rank_of(to)
            if step == 0:
                slots_out[...] = jnp.where(rank < SLOTS, owner * SLOTS + rank, -1)
            picked = jnp.where(slot_iota == jnp.where(owner == me, rank, -1), 1.0, 0.0)
            code = ids - me * table_rows + 1
            columns.append(jnp.sum(picked * code.astype(jnp.float32), axis=1, keepdims=True).astype(jnp.int32) - 1)
            high = lax.shift_right_arithmetic(code, 6)
            digits = jnp.where(owner == me, jnp.concatenate([high, code - high * 64], axis=0), 0)
            digits = jnp.concatenate([digits, jnp.zeros((6, tokens), jnp.int32)], axis=0).astype(jnp.float32).astype(jnp.bfloat16)
            spread = lax.dot_general(digits, picked.astype(jnp.bfloat16), COLS_DIMS, preferred_element_type=jnp.float32)
            rows_out[pl.ds(to, 1), :] = (spread[0:1] * 64.0 + spread[1:2]).astype(jnp.int32) - 1
        choose = jnp.where(lanes_iota == jnp.concatenate(columns, axis=0), 1.0, 0.0).astype(jnp.bfloat16)
        rows = jnp.dot(choose, table_out[...], preferred_element_type=jnp.float32).astype(jnp.bfloat16)
        for j in range(4):
            send[lax.rem(me + 4 * group + j, total)] = rows[j * SLOTS:(j + 1) * SLOTS]

    own_rows = pltpu.make_async_copy(send.at[me], got.at[me], local_sem.at[4])
    build(0)
    finish(wide(1))
    start(wide(2))
    start(across(1))
    start([row_copy(step) for step in range(1, 4)])
    build(1)
    own_rows.start()
    start([row_copy(step) for step in range(4, 8)])
    build(2)
    start([row_copy(step) for step in range(8, 12)])
    build(3)
    rank_out[...] = jnp.broadcast_to(jnp.max(rank_top[...], axis=1, keepdims=True), rank_out.shape).astype(jnp.int32)
    start([row_copy(step) for step in range(12, 16)])
    finish(wide(2))
    start(wide(3))
    start(across(2))
    own_rows.wait()
    finish([row_copy(step) for step in range(1, total)])
    place = lax.broadcasted_iota(jnp.int32, (total * SLOTS, tokens), 0) == slots_out[...]
    x_out[...] = lax.dot_general(jnp.where(place, 1.0, 0.0).astype(jnp.bfloat16), got[...].reshape(total * SLOTS, dim), ROWS_DIMS,
                                 preferred_element_type=jnp.float32).astype(jnp.bfloat16)
    finish(across(0))
    finish(across(1))
    finish(wide(3))
    start(across(3))
    finish(across(2))
    finish(across(3))


def front(packed, table_shard, gate_shard, up_shard, down_shard):
    bf16 = jnp.bfloat16
    rows, dim = table_shard.shape
    padded = -(-rows // VOCAB_TILE) * VOCAB_TILE
    tokens = packed.shape[1]
    vmem = pl.BlockSpec(memory_space=pltpu.VMEM)
    anywhere = pl.BlockSpec(memory_space=pl.ANY)
    sems = pltpu.SemaphoreType.DMA
    shards = (gate_shard, up_shard, down_shard)
    return pl.pallas_call(
        functools.partial(front_kernel, rows),
        in_specs=[anywhere, vmem, anywhere, anywhere, anywhere],
        out_specs=[vmem] * 9,
        out_shape=[jax.ShapeDtypeStruct((16,) + packed.shape, jnp.int32), jax.ShapeDtypeStruct((padded, dim), bf16)]
        + [jax.ShapeDtypeStruct((2, 2, 2, 2) + shard.shape, bf16) for shard in shards]
        + [jax.ShapeDtypeStruct((tokens, dim), bf16), jax.ShapeDtypeStruct((1, tokens), jnp.int32),
           jax.ShapeDtypeStruct((16, SLOTS), jnp.int32), jax.ShapeDtypeStruct((1, 128), jnp.int32)],
        scratch_shapes=[pltpu.VMEM((16, SLOTS, dim), bf16), pltpu.VMEM((16, SLOTS, dim), bf16), pltpu.VMEM((tokens, tokens), bf16), pltpu.VMEM((1, tokens), jnp.float32),
                        sems((5,)), sems((16,)), sems((16,)), sems((4, 3)), sems((4, 3)), sems((4, 3)), sems((4, 3)), sems((16,)), sems((16,))],
        compiler_params=pltpu.CompilerParams(vmem_limit_bytes=60 * 1024 * 1024, collective_id=3, has_side_effects=True),
        cost_estimate=pl.CostEstimate(flops=4 * 16 * SLOTS * padded * dim, bytes_accessed=20 * 1024 * 1024, transcendentals=0),
        name="front_all",
    )(packed, table_shard, gate_shard, up_shard, down_shard)


def split3(values):
    high = lax.reduce_precision(values, 8, 7)
    rest = values - high
    mid = lax.reduce_precision(rest, 8, 7)
    low = rest - mid
    return [part.astype(jnp.bfloat16) for part in (high, mid, low)]


def pick_rows(select, values):
    return jnp.dot(select, jnp.concatenate(split3(values), axis=0), preferred_element_type=jnp.float32)


def solution(mesh):
    groups = mesh.shape['fsdp']

    def device_step(token_ids, labels, table_shard, gate_shard, up_shard, down_shard, gain_in, gain_out):
        micro_count = token_ids.shape[0]
        tok_micro = token_ids.shape[1] * token_ids.shape[2]
        tok_dev = micro_count * tok_micro
        total_tokens = tok_dev * groups
        rows, dim = table_shard.shape
        me = lax.axis_index('fsdp')

        packed = jnp.stack([token_ids.reshape(tok_dev), labels.reshape(tok_dev)])
        gate_rows, ffn = gate_shard.shape
        down_rows = down_shard.shape[0]
        (packed_all, table_padded, w_gate, w_up, w_down, emb_rows, slots, row_idx, top_rank) = front(
            packed, table_shard, gate_shard, up_shard, down_shard)
        w_gate = w_gate.reshape(groups * gate_rows, ffn)
        w_up = w_up.reshape(groups * gate_rows, ffn)
        w_down = w_down.reshape(groups * down_rows, dim)
        rounds = top_rank[0, 0] // SLOTS + 1
        back_rounds = top_rank[0, 0] // BACK_SLOTS + 1

        def ranks(round_idx, count):
            ids_all, round_idx = lax.optimization_barrier((packed_all[:, 0], round_idx))
            owner = ids_all // rows
            owner_hot = owner[:, :, None] == jnp.arange(groups, dtype=jnp.int32)
            tri = jnp.tril(jnp.ones((tok_dev, tok_dev), jnp.bfloat16), -1)
            before = jnp.einsum('tu,suo->sto', tri, owner_hot.astype(jnp.bfloat16), preferred_element_type=jnp.float32)
            rank = jnp.sum(jnp.where(owner_hot, before, 0.0), axis=-1).astype(jnp.int32)
            return owner, ids_all - owner * rows, rank - round_idx * count

        def owned_rows(owner, local, rank, count):
            hit = (owner == me)[:, None, :] & (rank[:, None, :] == jnp.arange(count, dtype=jnp.int32)[None, :, None])
            return (jnp.sum(jnp.where(hit, local[:, None, :] + 1, 0), axis=-1) - 1).reshape(groups * count)

        def my_slots(owner, rank, count):
            mine = lax.dynamic_index_in_dim(owner, me, 0, keepdims=False)
            off = lax.dynamic_index_in_dim(rank, me, 0, keepdims=False)
            return jnp.where((off >= 0) & (off < count), mine * count + off, -1)

        def slot_place(slot_row, count):
            return (jnp.arange(groups * count, dtype=jnp.int32)[:, None] == slot_row[None, :]).astype(jnp.bfloat16)

        def fetch_round(round_idx):
            owner, local, rank = ranks(round_idx, SLOTS)
            select = (owned_rows(owner, local, rank, SLOTS)[:, None] == jnp.arange(rows, dtype=jnp.int32)[None, :]).astype(jnp.bfloat16)
            send = jnp.dot(select, table_shard, preferred_element_type=jnp.float32).astype(jnp.bfloat16)
            got = lax.all_to_all(send.reshape(groups, SLOTS, dim), 'fsdp', 0, 0).reshape(groups * SLOTS, dim)
            place = slot_place(my_slots(owner, rank, SLOTS), SLOTS)
            return lax.dot_general(place, got, ROWS_DIMS, preferred_element_type=jnp.float32).astype(jnp.bfloat16)

        def return_round(round_idx, grad_rows):
            owner, local, rank = ranks(round_idx, BACK_SLOTS)
            send = pick_rows(slot_place(jnp.tile(my_slots(owner, rank, BACK_SLOTS), 3), BACK_SLOTS), grad_rows)
            got = lax.all_to_all(send.reshape(groups, BACK_SLOTS, dim), 'fsdp', 0, 0).reshape(groups * BACK_SLOTS, dim)
            row_of = jnp.tile(owned_rows(owner, local, rank, BACK_SLOTS), 3)
            return pick_rows((jnp.arange(rows, dtype=jnp.int32)[:, None] == row_of[None, :]).astype(jnp.bfloat16), got)

        emb_rows = lax.fori_loop(1, rounds, lambda r, acc: acc + fetch_round(r), emb_rows)

        normed_out, saved = mlp_forward(emb_rows, gain_in, gain_out, w_gate, w_up, w_down)
        chunks = tok_dev // UNIT
        lab_rows = jnp.transpose(packed_all[:, 1].reshape(groups, chunks, UNIT), (1, 0, 2)).reshape(2 * chunks, groups * UNIT // 2)
        dz, dtable, loss_rows = head(normed_out, table_padded, lab_rows, rows)
        loss_total = loss_rows[0, 0]
        grad_rows, grad_mid, grad_gate_pre, grad_up_proj = mlp_backward(saved, dz, gain_in, gain_out, w_gate, w_up, w_down)
        normed_in, acts = saved[1], saved[5]
        first_rank = slots[0] % SLOTS
        back_slots = jnp.where((slots[0] >= 0) & (first_rank < BACK_SLOTS), slots[0] // SLOTS * BACK_SLOTS + first_rank, -1)
        send = pick_rows(slot_place(jnp.tile(back_slots, 3), BACK_SLOTS), grad_rows).reshape(groups, BACK_SLOTS, dim)
        out_gate, out_up, out_down, dtable = tail(normed_in, acts, grad_mid, grad_gate_pre, grad_up_proj, send,
                                                  row_idx[:, :BACK_SLOTS].reshape(1, groups * BACK_SLOTS), dtable, rows)
        dtable = lax.fori_loop(1, back_rounds, lambda r, acc: acc + return_round(r, grad_rows), dtable)
        return (loss_total / total_tokens, dtable, out_gate, out_up, out_down)

    row_spec = P('fsdp', None)
    tok_spec = P(None, 'fsdp', None)
    return jax.shard_map(device_step, mesh=mesh,
                         in_specs=(tok_spec, tok_spec, row_spec, row_spec, row_spec, row_spec, P(), P()),
                         out_specs=(P(), row_spec, row_spec, row_spec, row_spec), check_vma=False)
```

```python
import functools
import jax
import jax.numpy as jnp
from jax import lax
from jax.experimental import pallas as pl
from jax.experimental.pallas import tpu as pltpu
from jax.sharding import PartitionSpec as P

NORM_EPS = 1e-6
SLOTS = 64
BACK_SLOTS = 56


def rms_scale(values, gain_vec):
    vals32 = values.astype(jnp.float32)
    inv_rms = lax.rsqrt(jnp.mean(vals32 * vals32, axis=-1, keepdims=True) + NORM_EPS)
    return (vals32 * inv_rms * gain_vec).astype(jnp.bfloat16), inv_rms


def rms_back(values, inv_rms, gain_vec, grad_out):
    vals32 = values.astype(jnp.float32)
    scaled = grad_out * gain_vec
    proj_mean = jnp.mean(scaled * vals32, axis=-1, keepdims=True)
    return inv_rms * scaled - vals32 * (inv_rms * inv_rms * inv_rms) * proj_mean


def mlp_forward(emb_rows, gain_in, gain_out, w_gate, w_up, w_down):
    normed_in, inv_in = rms_scale(emb_rows, gain_in)
    gate_pre = jnp.dot(normed_in, w_gate, preferred_element_type=jnp.float32).astype(jnp.bfloat16)
    up_proj = jnp.dot(normed_in, w_up, preferred_element_type=jnp.float32).astype(jnp.bfloat16)
    acts = (jax.nn.silu(gate_pre.astype(jnp.float32)) * up_proj.astype(jnp.float32)).astype(jnp.bfloat16)
    mlp_out = jnp.dot(acts, w_down, preferred_element_type=jnp.float32).astype(jnp.bfloat16)
    hidden = (emb_rows.astype(jnp.float32) + mlp_out.astype(jnp.float32)).astype(jnp.bfloat16)
    normed_out, inv_out = rms_scale(hidden, gain_out)
    return normed_out, (emb_rows, normed_in, inv_in, gate_pre, up_proj, acts, hidden, inv_out)


COLS_DIMS = (((1,), (1,)), ((), ()))
ROWS_DIMS = (((0,), (0,)), ((), ()))


def mlp_backward(saved, grad_normed, gain_in, gain_out, w_gate, w_up, w_down):
    emb_rows, normed_in, inv_in, gate_pre, up_proj, acts, hidden, inv_out = saved
    grad_hidden = rms_back(hidden, inv_out, gain_out, grad_normed)
    grad_mid = grad_hidden.astype(jnp.bfloat16)
    grad_acts = lax.dot_general(grad_mid, w_down, COLS_DIMS, preferred_element_type=jnp.float32)
    gate32 = gate_pre.astype(jnp.float32)
    gate_sig = jax.nn.sigmoid(gate32)
    grad_gate_pre = (grad_acts * up_proj.astype(jnp.float32) * gate_sig * (1.0 + gate32 * (1.0 - gate_sig))).astype(jnp.bfloat16)
    grad_up_proj = (grad_acts * gate32 * gate_sig).astype(jnp.bfloat16)
    grad_normed_in = (lax.dot_general(grad_gate_pre, w_gate, COLS_DIMS, preferred_element_type=jnp.float32)
                      + lax.dot_general(grad_up_proj, w_up, COLS_DIMS, preferred_element_type=jnp.float32))
    grad_rows = grad_hidden + rms_back(emb_rows, inv_in, gain_in, grad_normed_in)
    return grad_rows, grad_mid, grad_gate_pre, grad_up_proj


UNIT = 64
CUBE_BITS = 3
PARTS = 3
VOCAB_TILE = 256
STAT_ROWS = 2
MESH_ID = pl.DeviceIdType.MESH
PAD_LOGIT = -1e30


def head_kernel(vocab_rows, chunks, z_hbm, table_ref, lab_ref, dz_ref, dtable_ref, loss_ref,
                zbuf, lbuf, gbuf, dzbuf, got_core, got_one, got_two, got_three, stats, labs, norm, loss_acc,
                local_sem, ag_send, ag_recv, rs_send, rs_recv, st_send, st_recv, lab_send, lab_recv):
    me = lax.axis_index('fsdp')
    total = 16
    core = lax.rem(me, 2)
    pos = [lax.rem(me // 2, 2), lax.rem(me // 4, 2), me // 8]
    base = me * vocab_rows
    padded, dim = table_ref.shape
    part_cols = dim // PARTS
    half = 8 * UNIT
    tiles = padded // VOCAB_TILE

    def peer(axis):
        return me + (1 - 2 * pos[axis]) * (2 << axis)

    core_peer = me + 1 - 2 * core

    barrier = pltpu.get_barrier_semaphore()
    for step in range(1, total):
        pl.semaphore_signal(barrier, inc=1, device_id=(lax.rem(me + step, total),), device_id_type=MESH_ID)
    own = pltpu.make_async_copy(z_hbm, zbuf.at[:, pos[2], pos[1], pos[0], core], local_sem)
    own.start()
    dtable_ref[...] = jnp.zeros_like(dtable_ref)
    loss_acc[...] = jnp.zeros_like(loss_acc)
    labs[me] = jnp.zeros((1, half), jnp.float32)
    own.wait()
    pl.semaphore_wait(barrier, total - 1)

    def where(choice):
        return choice.get(2, slice(None)), choice.get(1, slice(None)), choice.get(0, slice(None))

    def axes(part):
        return part % 3, (part + 1) % 3, (part + 2) % 3

    def cols(part):
        return pl.ds(part * part_cols, part_cols)

    def gather_copies(chunk, phase):
        if phase == 4:
            here = zbuf.at[chunk, :, :, :, core]
            return [pltpu.make_async_remote_copy(here, here, ag_send.at[chunk, 9], ag_recv.at[chunk, 9],
                                                 device_id=(core_peer,), device_id_type=MESH_ID)]
        copies = []
        for part in range(PARTS):
            order = axes(part)
            fixed = {axis: pos[axis] for axis in order[phase - 1:]}
            iz, iy, ix = where(fixed)
            here = zbuf.at[chunk, iz, iy, ix, core, :, cols(part)]
            sem = (phase - 1) * PARTS + part
            copies.append(pltpu.make_async_remote_copy(here, here, ag_send.at[chunk, sem], ag_recv.at[chunk, sem],
                                                       device_id=(peer(order[phase - 1]),), device_id_type=MESH_ID))
        return copies

    def reduce_copies(chunk, phase):
        slot, dzs = lax.rem(chunk, 2), lax.rem(chunk, 3)
        if phase == 0:
            return [pltpu.make_async_remote_copy(dzbuf.at[dzs, :, :, :, 1 - core], got_core.at[slot], rs_send.at[chunk, 9], rs_recv.at[chunk, 9],
                                                 device_id=(core_peer,), device_id_type=MESH_ID)]
        copies = []
        for part in range(PARTS):
            order = axes(part)
            fixed = {axis: pos[axis] for axis in order[:phase - 1]}
            fixed[order[phase - 1]] = 1 - pos[order[phase - 1]]
            iz, iy, ix = where(fixed)
            got = (got_one, got_two, got_three)[phase - 1]
            sem = (phase - 1) * PARTS + part
            copies.append(pltpu.make_async_remote_copy(dzbuf.at[dzs, iz, iy, ix, core, :, cols(part)], got.at[slot, part],
                                                       rs_send.at[chunk, sem], rs_recv.at[chunk, sem],
                                                       device_id=(peer(order[phase - 1]),), device_id_type=MESH_ID))
        return copies

    def start(copies):
        for copy in copies:
            copy.start()

    def finish(copies):
        for copy in copies:
            copy.wait()

    def reduce_add(chunk, phase):
        slot, dzs = lax.rem(chunk, 2), lax.rem(chunk, 3)
        if phase == 0:
            dzbuf[dzs, :, :, :, core] += got_core[slot]
            return
        for part in range(PARTS):
            order = axes(part)
            iz, iy, ix = where({axis: pos[axis] for axis in order[:phase]})
            got = (got_one, got_two, got_three)[phase - 1]
            lanes = slice(part * part_cols, (part + 1) * part_cols)
            if phase == 3:
                rows = pl.ds(pl.multiple_of(chunk * UNIT, UNIT), UNIT)
                dz_ref[rows, lanes] = dzbuf[dzs, iz, iy, ix, core, :, lanes] + got[slot, part]
            else:
                dzbuf[dzs, iz, iy, ix, core, :, lanes] += got[slot, part]

    def stat_copies(chunk):
        copies = []
        for step in range(1, total):
            to = lax.rem(me + step, total)
            copies.append(pltpu.make_async_remote_copy(stats.at[chunk, me], stats.at[chunk, me], st_send.at[chunk, step], st_recv.at[chunk, step],
                                                       device_id=(to,), device_id_type=MESH_ID))
        return copies

    def lab_copies():
        return [pltpu.make_async_remote_copy(labs.at[me], labs.at[me], lab_send.at[step], lab_recv.at[step],
                                             device_id=(lax.rem(me + step, total),), device_id_type=MESH_ID) for step in range(1, total)]

    def label_row(chunk, part):
        lab = lab_ref[pl.ds(chunk * 2 + part, 1), :] - base
        return jnp.where(lab < vocab_rows, lab, -1)

    row_ids = lax.broadcasted_iota(jnp.int32, (VOCAB_TILE, half), 0)

    def forward_half(chunk, part):
        slot = lax.rem(chunk, 2)
        zb = zbuf[chunk, part].reshape(half, dim)
        lab = label_row(chunk, part)
        tops, sums, hits = [], [], []
        for tile in range(tiles):
            rows = slice(tile * VOCAB_TILE, (tile + 1) * VOCAB_TILE)
            logits = lax.dot_general(table_ref[rows, :], zb, COLS_DIMS, preferred_element_type=jnp.float32)
            if (tile + 1) * VOCAB_TILE > vocab_rows:
                logits = jnp.where(row_ids < vocab_rows - tile * VOCAB_TILE, logits, PAD_LOGIT)
            lbuf[slot, rows, part * half:(part + 1) * half] = logits
            top = jnp.max(logits, axis=0, keepdims=True)
            tops.append(top)
            sums.append(jnp.sum(jnp.exp(logits - top), axis=0, keepdims=True))
            hits.append(jnp.sum(jnp.where(row_ids == lab - tile * VOCAB_TILE, logits, 0.0), axis=0, keepdims=True))
        top = functools.reduce(jnp.maximum, tops)
        exp_sum = sum(s * jnp.exp(t - top) for s, t in zip(sums, tops))
        stats[chunk, me, part:part + 1, :] = top + jnp.log(exp_sum)
        labs[me] += sum(hits)

    def combine(chunk):
        for part in range(2):
            tops = stats[chunk, :, part, :]
            top = jnp.max(tops, axis=0, keepdims=True)
            exp_sum = jnp.sum(jnp.exp(tops - top), axis=0, keepdims=True)
            norm[part:part + 1, :] = top
            norm[2 + part:3 + part, :] = 1.0 / exp_sum
            loss_acc[...] += top + jnp.log(exp_sum)

    def table_half(chunk, which):
        slot = lax.rem(chunk, 2)
        zc = zbuf[chunk].reshape(2 * half, dim)
        for tile in range(which * tiles // 2, (which + 1) * tiles // 2):
            rows = slice(tile * VOCAB_TILE, (tile + 1) * VOCAB_TILE)
            for part in range(2):
                lanes = slice(part * half, (part + 1) * half)
                probs = jnp.exp(lbuf[slot, rows, lanes] - norm[part:part + 1, :]) * norm[2 + part:3 + part, :]
                hot = row_ids == label_row(chunk, part) - tile * VOCAB_TILE
                gbuf[rows, lanes] = jnp.where(hot, probs - 1.0, probs).astype(jnp.bfloat16)
            dtable_ref[rows, :] += jnp.dot(gbuf[rows, :], zc, preferred_element_type=jnp.float32)

    def token_half(chunk, part):
        dz = lax.dot_general(gbuf[:, part * half:(part + 1) * half], table_ref[...], ROWS_DIMS, preferred_element_type=jnp.float32)
        dzbuf[lax.rem(chunk, 3), part] = dz.reshape(2, 2, 2, UNIT, dim)

    start(gather_copies(0, 1))
    start(gather_copies(1, 1))
    start(gather_copies(2, 1))
    for chunk in range(3):
        finish(gather_copies(chunk, 1))
        start(gather_copies(chunk, 2))
    for chunk in range(2):
        finish(gather_copies(chunk, 2))
        start(gather_copies(chunk, 3))
    finish(gather_copies(0, 3))
    start(gather_copies(0, 4))
    finish(gather_copies(0, 4))

    def body(i, carry):
        def inside(offset, action):
            chunk = i + offset
            pl.when((chunk >= 0) & (chunk < chunks))(lambda: action(jnp.clip(chunk, 0, chunks - 1)))

        def step_reduce(phase, follow):
            def action(chunk):
                finish(reduce_copies(chunk, phase))
                reduce_add(chunk, phase)
                if follow:
                    start(reduce_copies(chunk, phase + 1))
            return action

        def step_gather(phase):
            def action(chunk):
                finish(gather_copies(chunk, phase))
                start(gather_copies(chunk, phase + 1))
            return action

        inside(-4, step_reduce(2, True))
        inside(-2, lambda chunk: start(reduce_copies(chunk, 0)))
        inside(1, step_gather(3))
        inside(3, lambda chunk: start(gather_copies(chunk, 1)))
        inside(2, step_gather(2))

        @pl.when(i < chunks)
        def _():
            forward_half(i, 0)
            forward_half(i, 1)

        inside(-2, step_reduce(0, False))
        inside(-3, step_reduce(1, True))
        inside(-4, step_reduce(3, False))
        inside(3, step_gather(1))
        inside(1, lambda chunk: finish(gather_copies(chunk, 4)))
        inside(-2, lambda chunk: start(reduce_copies(chunk, 1)))
        inside(0, lambda chunk: start(stat_copies(chunk)))

        @pl.when(i == chunks - 1)
        def _():
            start(lab_copies())

        def backward(chunk):
            finish(stat_copies(chunk))
            combine(chunk)
            table_half(chunk, 0)
            table_half(chunk, 1)
            token_half(chunk, 0)
            token_half(chunk, 1)

        inside(-1, backward)
        return carry

    lax.fori_loop(0, chunks + 4, body, 0)
    finish(lab_copies())
    loss_ref[...] = jnp.broadcast_to(jnp.sum(loss_acc[...] - jnp.sum(labs[...], axis=0), axis=1, keepdims=True), loss_ref.shape)


def head(z_local, table_padded, lab_rows, vocab_rows):
    tokens, dim = z_local.shape
    chunks = tokens // UNIT
    padded = table_padded.shape[0]
    chunk_tokens = 16 * UNIT
    part_cols = dim // PARTS
    f32, bf16 = jnp.float32, jnp.bfloat16
    sems = pltpu.SemaphoreType.DMA
    vmem = pl.BlockSpec(memory_space=pltpu.VMEM)
    cost = 6 * tokens * 16 * padded * dim
    return pl.pallas_call(
        functools.partial(head_kernel, vocab_rows, chunks),
        in_specs=[pl.BlockSpec(memory_space=pl.ANY), vmem, vmem],
        out_specs=[vmem, vmem, vmem],
        out_shape=[jax.ShapeDtypeStruct((tokens, dim), f32),
                   jax.ShapeDtypeStruct((padded, dim), f32),
                   jax.ShapeDtypeStruct((1, 128), f32)],
        scratch_shapes=[pltpu.VMEM((chunks, 2, 2, 2, 2, UNIT, dim), bf16),
                        pltpu.VMEM((2, padded, chunk_tokens), f32),
                        pltpu.VMEM((padded, chunk_tokens), bf16),
                        pltpu.VMEM((3, 2, 2, 2, 2, UNIT, dim), f32),
                        pltpu.VMEM((2, 2, 2, 2, UNIT, dim), f32),
                        pltpu.VMEM((2, PARTS, 2, 2, UNIT, part_cols), f32),
                        pltpu.VMEM((2, PARTS, 2, UNIT, part_cols), f32),
                        pltpu.VMEM((2, PARTS, UNIT, part_cols), f32),
                        pltpu.VMEM((chunks, 16, STAT_ROWS, 8 * UNIT), f32),
                        pltpu.VMEM((16, 1, 8 * UNIT), f32),
                        pltpu.VMEM((8, 8 * UNIT), f32),
                        pltpu.VMEM((1, 8 * UNIT), f32),
                        sems(()),
                        sems((chunks, 10)), sems((chunks, 10)),
                        sems((chunks, 10)), sems((chunks, 10)),
                        sems((chunks, 16)), sems((chunks, 16)),
                        sems((16,)), sems((16,))],
        compiler_params=pltpu.CompilerParams(vmem_limit_bytes=67043328, collective_id=1, has_side_effects=True),
        cost_estimate=pl.CostEstimate(flops=cost, bytes_accessed=4 * padded * dim, transcendentals=2 * tokens * 16 * padded),
        name="head_all",
    )(z_local.reshape(chunks, UNIT, dim), table_padded, lab_rows)


PIECES = 8


def axes(part):
    return part % 3, (part + 1) % 3, (part + 2) % 3


def cube_index(choice):
    return choice.get(2, slice(None)), choice.get(1, slice(None)), choice.get(0, slice(None))


def tail_kernel(table_rows, u_ref, acts_ref, mid_ref, gate_ref, up_ref, send_hbm, row_ref, dtable_hbm, gate_out, up_out, down_out, dtable_hbm_out,
                all_g, all_u, all_d, core_g, core_u, core_d, one_g, one_u, one_d, two_g, two_u, two_d, three_g, three_u, three_d,
                rows_got, split, dtable_out, local_sem, send_sem, recv_sem, row_send, row_recv):
    me = lax.axis_index('fsdp')
    total = 16
    core = lax.rem(me, 2)
    pos = [lax.rem(me // 2, 2), lax.rem(me // 4, 2), me // 8]
    core_peer = me + 1 - 2 * core
    whole = (all_g, all_u, all_d)
    gots = ((core_g, core_u, core_d), (one_g, one_u, one_d), (two_g, two_u, two_d), (three_g, three_u, three_d))
    outs = (gate_out, up_out, down_out)

    barrier = pltpu.get_barrier_semaphore()
    for step in range(1, total):
        pl.semaphore_signal(barrier, inc=1, device_id=(lax.rem(me + step, total),), device_id_type=MESH_ID)
    loads = []
    loads.append(pltpu.make_async_copy(dtable_hbm.at[pl.ds(0, table_rows)], dtable_out, local_sem.at[3]))
    loads.append(pltpu.make_async_copy(send_hbm.at[me], rows_got.at[me], local_sem.at[4]))
    for load in loads:
        load.start()
    pl.semaphore_wait(barrier, total - 1)

    def piece(part, q):
        if part == 2:
            size = all_d.shape[4] // PIECES
            return pl.ds(q * size, size), slice(None)
        size = all_g.shape[5] // PIECES
        return slice(None), pl.ds(q * size, size)

    def copies(phase, q, parts=(0, 1, 2)):
        made = []
        for part in parts:
            rows, lanes = piece(part, q)
            order = axes(part)
            if phase == 0:
                src = whole[part].at[1 - core, :, :, :, rows, lanes]
                dst = gots[0][part].at[:, :, :, rows, lanes]
                to = core_peer
            else:
                fixed = {axis: pos[axis] for axis in order[:phase - 1]}
                fixed[order[phase - 1]] = 1 - pos[order[phase - 1]]
                iz, iy, ix = cube_index(fixed)
                src = whole[part].at[core, iz, iy, ix, rows, lanes]
                lead = (slice(None),) * (3 - phase)
                dst = gots[phase][part].at[lead + (rows, lanes)]
                axis = order[phase - 1]
                to = me + (1 - 2 * pos[axis]) * (2 << axis)
            made.append(pltpu.make_async_remote_copy(src, dst, send_sem.at[phase, part, q], recv_sem.at[phase, part, q],
                                                     device_id=(to,), device_id_type=MESH_ID))
        return made

    def start(made):
        for copy in made:
            copy.start()

    def finish_add(phase, q):
        for copy in copies(phase, q):
            copy.wait()
        for part in range(3):
            rows, lanes = piece(part, q)
            iz, iy, ix = cube_index({axis: pos[axis] for axis in axes(part)[:phase]})
            got = gots[phase][part][(slice(None),) * (3 - phase) + (rows, lanes)]
            if phase == 3:
                outs[part][rows, lanes] = whole[part][core, iz, iy, ix, rows, lanes] + got
            else:
                whole[part][core, iz, iy, ix, rows, lanes] += got

    row_copies = []
    for step in range(1, total):
        to = lax.rem(me + step, total)
        row_copies.append(pltpu.make_async_remote_copy(send_hbm.at[to], rows_got.at[me], row_send.at[step], row_recv.at[step],
                                                       device_id=(to,), device_id_type=MESH_ID))
    start(row_copies)
    down_rows = all_d.shape[4]
    for chip in range(8):
        block = lax.dot_general(acts_ref[:, 2 * chip * down_rows:2 * (chip + 1) * down_rows], mid_ref[...], ROWS_DIMS,
                                preferred_element_type=jnp.float32)
        for c in range(2):
            all_d[c, chip // 4, chip // 2 % 2, chip % 2] = block[c * down_rows:(c + 1) * down_rows]
    for q in range(PIECES):
        start(copies(0, q, (2,)))
    unit, lanes = all_g.shape[4], all_g.shape[5] // PIECES
    for q in range(PIECES):
        here = slice(q * lanes, (q + 1) * lanes)
        for grads, array in ((gate_ref, all_g), (up_ref, all_u)):
            for h in range(2):
                block = lax.dot_general(u_ref[:, 8 * unit * h:8 * unit * (h + 1)], grads[:, here], ROWS_DIMS, preferred_element_type=jnp.float32)
                for k in range(8):
                    array[k % 2, h, k // 4, k // 2 % 2, :, here] = block[k * unit:(k + 1) * unit]
        start(copies(0, q, (0, 1)))
    for load in loads:
        load.wait()
    for q in range(PIECES):
        finish_add(0, q)
        start(copies(1, q))
    for copy in row_copies:
        copy.wait()
    slots, dim = rows_got.shape[0] * rows_got.shape[1], rows_got.shape[2]

    pair = 2 * rows_got.shape[1]

    def split_rows(s, carry):
        vals = rows_got[pl.ds(2 * s, 2)].reshape(pair, dim)
        at = pl.multiple_of(s * pair, pair)
        high = vals.astype(jnp.bfloat16)
        rest = vals - high.astype(jnp.float32)
        mid = rest.astype(jnp.bfloat16)
        split[pl.ds(at, pair), :] = high
        split[pl.ds(slots + at, pair), :] = mid
        split[pl.ds(2 * slots + at, pair), :] = (rest - mid.astype(jnp.float32)).astype(jnp.bfloat16)
        return carry

    lax.fori_loop(0, total // 2, split_rows, 0)

    def add_rows(first, count):
        ids = lax.broadcasted_iota(jnp.int32, (count, slots), 0) + first
        hot = jnp.where(ids == row_ref[...], 1.0, 0.0).astype(jnp.bfloat16)
        dtable_out[pl.ds(first, count), :] += jnp.dot(jnp.concatenate([hot, hot, hot], axis=1), split[...], preferred_element_type=jnp.float32)

    full = table_rows // VOCAB_TILE

    def add_tile(tile, carry):
        add_rows(pl.multiple_of(tile * VOCAB_TILE, VOCAB_TILE), VOCAB_TILE)
        return carry

    lax.fori_loop(0, full, add_tile, 0)
    if table_rows % VOCAB_TILE:
        add_rows(full * VOCAB_TILE, table_rows % VOCAB_TILE)

    save = pltpu.make_async_copy(dtable_out, dtable_hbm_out, local_sem.at[0])
    for q in range(PIECES + 2):
        if q == 1:
            save.start()
        if q < PIECES:
            finish_add(1, q)
            start(copies(2, q))
        if 1 <= q <= PIECES:
            finish_add(2, q - 1)
            start(copies(3, q - 1))
        if q >= 2:
            finish_add(3, q - 2)
    save.wait()


def tail(normed_in, acts, grad_mid, grad_gate_pre, grad_up_proj, send, row_idx, dtable, table_rows):
    f32 = jnp.float32
    vmem = pl.BlockSpec(memory_space=pltpu.VMEM)
    anywhere = pl.BlockSpec(memory_space=pl.ANY)
    sems = pltpu.SemaphoreType.DMA
    ffn = acts.shape[1]
    blocks = [(normed_in.shape[1] // 16, ffn), (normed_in.shape[1] // 16, ffn), (ffn // 16, normed_in.shape[1])]
    scratch = [pltpu.VMEM(lead + block, f32) for lead in ((2, 2, 2, 2), (2, 2, 2), (2, 2), (2,), ()) for block in blocks]
    slots = send.shape[0] * send.shape[1]
    dim = send.shape[2]
    return pl.pallas_call(
        functools.partial(tail_kernel, table_rows),
        in_specs=[vmem, vmem, vmem, vmem, vmem, anywhere, vmem, anywhere],
        out_specs=[vmem, vmem, vmem, anywhere],
        out_shape=[jax.ShapeDtypeStruct(block, f32) for block in blocks] + [jax.ShapeDtypeStruct((table_rows, dim), f32)],
        scratch_shapes=scratch + [pltpu.VMEM(send.shape, f32), pltpu.VMEM((3 * slots, dim), jnp.bfloat16), pltpu.VMEM((table_rows, dim), f32),
                                  sems((5,)), sems((4, 3, PIECES)), sems((4, 3, PIECES)), sems((16,)), sems((16,))],
        compiler_params=pltpu.CompilerParams(vmem_limit_bytes=67043328, collective_id=2, has_side_effects=True),
        cost_estimate=pl.CostEstimate(flops=6 * slots * table_rows * dim, bytes_accessed=40 * 1024 * 1024, transcendentals=0),
        name="tail_all",
    )(normed_in, acts, grad_mid, grad_gate_pre, grad_up_proj, send, row_idx, dtable)


def front_kernel(table_rows, pack_hbm, table_ref, gate_hbm, up_hbm, down_hbm,
                 pack_out, table_hbm_out, gate_hbm_out, up_hbm_out, down_hbm_out, x_out, slots_out, rows_out, rank_out,
                 table_out, gate_out, up_out, down_out, send, got, before_ref, rank_top, local_sem, save_sem, id_send, id_recv, w_send, w_recv, c_send, c_recv, row_send, row_recv):
    me = lax.axis_index('fsdp')
    total = 16
    core = lax.rem(me, 2)
    pos = [lax.rem(me // 2, 2), lax.rem(me // 4, 2), me // 8]
    core_peer = me + 1 - 2 * core
    shards = (gate_hbm, up_hbm, down_hbm)
    outs = (gate_out, up_out, down_out)
    tokens = pack_out.shape[2]
    padded, dim = table_out.shape

    barrier = pltpu.get_barrier_semaphore()
    for step in range(1, total):
        pl.semaphore_signal(barrier, inc=1, device_id=(lax.rem(me + step, total),), device_id_type=MESH_ID)
    loads = [pltpu.make_async_copy(shards[part], outs[part].at[pos[2], pos[1], pos[0], core], local_sem.at[part]) for part in range(3)]
    loads.append(pltpu.make_async_copy(pack_hbm, pack_out.at[me], local_sem.at[3]))
    for load in loads:
        load.start()

    def remote(src, dst, send_sem, recv_sem, to):
        return pltpu.make_async_remote_copy(src, dst, send_sem, recv_sem, device_id=(to,), device_id_type=MESH_ID)

    def wide(phase):
        made = []
        for part in range(3):
            order = axes(part)
            iz, iy, ix = cube_index({axis: pos[axis] for axis in order[phase - 1:]})
            here = outs[part].at[iz, iy, ix, core]
            axis = order[phase - 1]
            made.append(remote(shards[part] if phase == 1 else here, here, w_send.at[phase, part], w_recv.at[phase, part],
                               me + (1 - 2 * pos[axis]) * (2 << axis)))
        return made

    def across(stage):
        made = []
        for part in range(3):
            order = axes(part)
            fixed = {axis: pos[axis] for axis in order[stage:]}
            if stage:
                fixed[order[stage - 1]] = 1 - pos[order[stage - 1]]
            iz, iy, ix = cube_index(fixed)
            here = outs[part].at[iz, iy, ix, core]
            made.append(remote(here if stage else shards[part], here, c_send.at[stage, part], c_recv.at[stage, part], core_peer))
        return made

    def id_copies():
        return [remote(pack_hbm, pack_out.at[me], id_send.at[step], id_recv.at[step], lax.rem(me + step, total)) for step in range(1, total)]

    def row_copy(step):
        to = lax.rem(me + step, total)
        return remote(send.at[to], got.at[me], row_send.at[step], row_recv.at[step], to)

    def start(made):
        for copy in made:
            copy.start()

    def finish(made):
        for copy in made:
            copy.wait()

    pl.semaphore_wait(barrier, total - 1)
    start(id_copies())
    start(wide(1))
    start(across(0))
    table_out[0:table_rows, :] = table_ref[...]
    table_out[table_rows:padded, :] = jnp.zeros((padded - table_rows, dim), table_out.dtype)
    earlier = lax.broadcasted_iota(jnp.int32, (tokens, tokens), 0) < lax.broadcasted_iota(jnp.int32, (tokens, tokens), 1)
    before_ref[...] = jnp.where(earlier, 1.0, 0.0).astype(jnp.bfloat16)
    rank_top[...] = jnp.zeros_like(rank_top)
    for load in loads:
        load.wait()
    finish(id_copies())

    lanes_iota = lax.broadcasted_iota(jnp.int32, (4 * SLOTS, padded), 1)
    slot_iota = lax.broadcasted_iota(jnp.int32, (SLOTS, tokens), 0)
    dev_iota = lax.broadcasted_iota(jnp.int32, (total, tokens), 0)

    def rank_of(to):
        ids = pack_out[to, 0:1, :]
        owner = jnp.zeros_like(ids)
        for k in range(1, total):
            owner = owner + jnp.where(ids >= k * table_rows, 1, 0)
        hot = jnp.where(dev_iota == owner, 1.0, 0.0)
        before = jnp.dot(hot.astype(jnp.bfloat16), before_ref[...], preferred_element_type=jnp.float32)
        rank = jnp.sum(hot * before, axis=0, keepdims=True)
        rank_top[...] = jnp.maximum(rank_top[...], rank)
        return ids, owner, rank.astype(jnp.int32)

    def build(group):
        columns = []
        for step in range(4 * group, 4 * group + 4):
            to = lax.rem(me + step, total)
            ids, owner, rank = rank_of(to)
            if step == 0:
                slots_out[...] = jnp.where(rank < SLOTS, owner * SLOTS + rank, -1)
            picked = jnp.where(slot_iota == jnp.where(owner == me, rank, -1), 1.0, 0.0)
            code = ids - me * table_rows + 1
            columns.append(jnp.sum(picked * code.astype(jnp.float32), axis=1, keepdims=True).astype(jnp.int32) - 1)
            high = lax.shift_right_arithmetic(code, 6)
            digits = jnp.where(owner == me, jnp.concatenate([high, code - high * 64], axis=0), 0)
            digits = jnp.concatenate([digits, jnp.zeros((6, tokens), jnp.int32)], axis=0).astype(jnp.float32).astype(jnp.bfloat16)
            spread = lax.dot_general(digits, picked.astype(jnp.bfloat16), COLS_DIMS, preferred_element_type=jnp.float32)
            rows_out[pl.ds(to, 1), :] = (spread[0:1] * 64.0 + spread[1:2]).astype(jnp.int32) - 1
        choose = jnp.where(lanes_iota == jnp.concatenate(columns, axis=0), 1.0, 0.0).astype(jnp.bfloat16)
        rows = jnp.dot(choose, table_out[...], preferred_element_type=jnp.float32).astype(jnp.bfloat16)
        for j in range(4):
            send[lax.rem(me + 4 * group + j, total)] = rows[j * SLOTS:(j + 1) * SLOTS]

    own_rows = pltpu.make_async_copy(send.at[me], got.at[me], local_sem.at[4])
    build(0)
    finish(wide(1))
    start(wide(2))
    start(across(1))
    start([row_copy(step) for step in range(1, 4)])
    build(1)
    own_rows.start()
    start([row_copy(step) for step in range(4, 8)])
    build(2)
    start([row_copy(step) for step in range(8, 12)])
    build(3)
    rank_out[...] = jnp.broadcast_to(jnp.max(rank_top[...], axis=1, keepdims=True), rank_out.shape).astype(jnp.int32)
    start([row_copy(step) for step in range(12, 16)])
    finish(wide(2))
    start(wide(3))
    start(across(2))
    saves = [pltpu.make_async_copy(table_out, table_hbm_out, save_sem.at[9])]
    saves[0].start()
    results = (gate_hbm_out, up_hbm_out, down_hbm_out)

    def save(mine, which, sem):
        for part in range(3):
            axis = axes(part)[2]
            index = cube_index({axis: pos[axis] if mine else 1 - pos[axis]}) + (which,)
            saves.append(pltpu.make_async_copy(outs[part].at[index], results[part].at[index], save_sem.at[sem * 3 + part]))
            saves[-1].start()

    for stage in range(3):
        finish(across(stage))
    save(True, slice(None), 0)
    own_rows.wait()
    finish([row_copy(step) for step in range(1, total)])
    place = lax.broadcasted_iota(jnp.int32, (total * SLOTS, tokens), 0) == slots_out[...]
    x_out[...] = lax.dot_general(jnp.where(place, 1.0, 0.0).astype(jnp.bfloat16), got[...].reshape(total * SLOTS, dim), ROWS_DIMS,
                                 preferred_element_type=jnp.float32).astype(jnp.bfloat16)
    finish(wide(3))
    start(across(3))
    save(False, core, 1)
    finish(across(3))
    save(False, 1 - core, 2)
    for copy in saves:
        copy.wait()


def front(packed, table_shard, gate_shard, up_shard, down_shard):
    bf16 = jnp.bfloat16
    rows, dim = table_shard.shape
    padded = -(-rows // VOCAB_TILE) * VOCAB_TILE
    tokens = packed.shape[1]
    vmem = pl.BlockSpec(memory_space=pltpu.VMEM)
    anywhere = pl.BlockSpec(memory_space=pl.ANY)
    sems = pltpu.SemaphoreType.DMA
    shards = (gate_shard, up_shard, down_shard)
    return pl.pallas_call(
        functools.partial(front_kernel, rows),
        in_specs=[anywhere, vmem, anywhere, anywhere, anywhere],
        out_specs=[vmem] + [anywhere] * 4 + [vmem] * 4,
        out_shape=[jax.ShapeDtypeStruct((16,) + packed.shape, jnp.int32), jax.ShapeDtypeStruct((padded, dim), bf16)]
        + [jax.ShapeDtypeStruct((2, 2, 2, 2) + shard.shape, bf16) for shard in shards]
        + [jax.ShapeDtypeStruct((tokens, dim), bf16), jax.ShapeDtypeStruct((1, tokens), jnp.int32),
           jax.ShapeDtypeStruct((16, SLOTS), jnp.int32), jax.ShapeDtypeStruct((1, 128), jnp.int32)],
        scratch_shapes=[pltpu.VMEM((padded, dim), bf16)] + [pltpu.VMEM((2, 2, 2, 2) + shard.shape, bf16) for shard in shards]
        + [pltpu.VMEM((16, SLOTS, dim), bf16), pltpu.VMEM((16, SLOTS, dim), bf16), pltpu.VMEM((tokens, tokens), bf16), pltpu.VMEM((1, tokens), jnp.float32),
           sems((5,)), sems((10,)), sems((16,)), sems((16,)), sems((4, 3)), sems((4, 3)), sems((4, 3)), sems((4, 3)), sems((16,)), sems((16,))],
        compiler_params=pltpu.CompilerParams(vmem_limit_bytes=60 * 1024 * 1024, collective_id=3, has_side_effects=True),
        cost_estimate=pl.CostEstimate(flops=4 * 16 * SLOTS * padded * dim, bytes_accessed=20 * 1024 * 1024, transcendentals=0),
        name="front_all",
    )(packed, table_shard, gate_shard, up_shard, down_shard)


def split3(values):
    high = lax.reduce_precision(values, 8, 7)
    rest = values - high
    mid = lax.reduce_precision(rest, 8, 7)
    low = rest - mid
    return [part.astype(jnp.bfloat16) for part in (high, mid, low)]


def pick_rows(select, values):
    return jnp.dot(select, jnp.concatenate(split3(values), axis=0), preferred_element_type=jnp.float32)


def solution(mesh):
    groups = mesh.shape['fsdp']

    def device_step(token_ids, labels, table_shard, gate_shard, up_shard, down_shard, gain_in, gain_out):
        micro_count = token_ids.shape[0]
        tok_micro = token_ids.shape[1] * token_ids.shape[2]
        tok_dev = micro_count * tok_micro
        total_tokens = tok_dev * groups
        rows, dim = table_shard.shape
        me = lax.axis_index('fsdp')

        packed = jnp.stack([token_ids.reshape(tok_dev), labels.reshape(tok_dev)])
        gate_rows, ffn = gate_shard.shape
        down_rows = down_shard.shape[0]
        (packed_all, table_padded, w_gate, w_up, w_down, emb_rows, slots, row_idx, top_rank) = front(
            packed, table_shard, gate_shard, up_shard, down_shard)
        w_gate = w_gate.reshape(groups * gate_rows, ffn)
        w_up = w_up.reshape(groups * gate_rows, ffn)
        w_down = w_down.reshape(groups * down_rows, dim)
        rounds = top_rank[0, 0] // SLOTS + 1
        back_rounds = top_rank[0, 0] // BACK_SLOTS + 1

        def ranks(round_idx, count):
            ids_all, round_idx = lax.optimization_barrier((packed_all[:, 0], round_idx))
            owner = ids_all // rows
            owner_hot = owner[:, :, None] == jnp.arange(groups, dtype=jnp.int32)
            tri = jnp.tril(jnp.ones((tok_dev, tok_dev), jnp.bfloat16), -1)
            before = jnp.einsum('tu,suo->sto', tri, owner_hot.astype(jnp.bfloat16), preferred_element_type=jnp.float32)
            rank = jnp.sum(jnp.where(owner_hot, before, 0.0), axis=-1).astype(jnp.int32)
            return owner, ids_all - owner * rows, rank - round_idx * count

        def owned_rows(owner, local, rank, count):
            hit = (owner == me)[:, None, :] & (rank[:, None, :] == jnp.arange(count, dtype=jnp.int32)[None, :, None])
            return (jnp.sum(jnp.where(hit, local[:, None, :] + 1, 0), axis=-1) - 1).reshape(groups * count)

        def my_slots(owner, rank, count):
            mine = lax.dynamic_index_in_dim(owner, me, 0, keepdims=False)
            off = lax.dynamic_index_in_dim(rank, me, 0, keepdims=False)
            return jnp.where((off >= 0) & (off < count), mine * count + off, -1)

        def slot_place(slot_row, count):
            return (jnp.arange(groups * count, dtype=jnp.int32)[:, None] == slot_row[None, :]).astype(jnp.bfloat16)

        def fetch_round(round_idx):
            owner, local, rank = ranks(round_idx, SLOTS)
            select = (owned_rows(owner, local, rank, SLOTS)[:, None] == jnp.arange(rows, dtype=jnp.int32)[None, :]).astype(jnp.bfloat16)
            send = jnp.dot(select, table_shard, preferred_element_type=jnp.float32).astype(jnp.bfloat16)
            got = lax.all_to_all(send.reshape(groups, SLOTS, dim), 'fsdp', 0, 0).reshape(groups * SLOTS, dim)
            place = slot_place(my_slots(owner, rank, SLOTS), SLOTS)
            return lax.dot_general(place, got, ROWS_DIMS, preferred_element_type=jnp.float32).astype(jnp.bfloat16)

        def return_round(round_idx, grad_rows):
            owner, local, rank = ranks(round_idx, BACK_SLOTS)
            send = pick_rows(slot_place(jnp.tile(my_slots(owner, rank, BACK_SLOTS), 3), BACK_SLOTS), grad_rows)
            got = lax.all_to_all(send.reshape(groups, BACK_SLOTS, dim), 'fsdp', 0, 0).reshape(groups * BACK_SLOTS, dim)
            row_of = jnp.tile(owned_rows(owner, local, rank, BACK_SLOTS), 3)
            return pick_rows((jnp.arange(rows, dtype=jnp.int32)[:, None] == row_of[None, :]).astype(jnp.bfloat16), got)

        emb_rows = lax.fori_loop(1, rounds, lambda r, acc: acc + fetch_round(r), emb_rows)

        normed_out, saved = mlp_forward(emb_rows, gain_in, gain_out, w_gate, w_up, w_down)
        chunks = tok_dev // UNIT
        lab_rows = jnp.transpose(packed_all[:, 1].reshape(groups, chunks, UNIT), (1, 0, 2)).reshape(2 * chunks, groups * UNIT // 2)
        dz, dtable, loss_rows = head(normed_out, table_padded, lab_rows, rows)
        loss_total = loss_rows[0, 0]
        grad_rows, grad_mid, grad_gate_pre, grad_up_proj = mlp_backward(saved, dz, gain_in, gain_out, w_gate, w_up, w_down)
        normed_in, acts = saved[1], saved[5]
        first_rank = slots[0] % SLOTS
        back_slots = jnp.where((slots[0] >= 0) & (first_rank < BACK_SLOTS), slots[0] // SLOTS * BACK_SLOTS + first_rank, -1)
        send = pick_rows(slot_place(jnp.tile(back_slots, 3), BACK_SLOTS), grad_rows).reshape(groups, BACK_SLOTS, dim)
        out_gate, out_up, out_down, dtable = tail(normed_in, acts, grad_mid, grad_gate_pre, grad_up_proj, send,
                                                  row_idx[:, :BACK_SLOTS].reshape(1, groups * BACK_SLOTS), dtable, rows)
        dtable = lax.fori_loop(1, back_rounds, lambda r, acc: acc + return_round(r, grad_rows), dtable)
        return (loss_total / total_tokens, dtable, out_gate, out_up, out_down)

    row_spec = P('fsdp', None)
    tok_spec = P(None, 'fsdp', None)
    return jax.shard_map(device_step, mesh=mesh,
                         in_specs=(tok_spec, tok_spec, row_spec, row_spec, row_spec, row_spec, P(), P()),
                         out_specs=(P(), row_spec, row_spec, row_spec, row_spec), check_vma=False)
```

```python
import functools
import jax
import jax.numpy as jnp
from jax import lax
from jax.experimental import pallas as pl
from jax.experimental.pallas import tpu as pltpu
from jax.sharding import PartitionSpec as P

NORM_EPS = 1e-6
SLOTS = 64
BACK_SLOTS = 56


def rms_scale(values, gain_vec):
    vals32 = values.astype(jnp.float32)
    inv_rms = lax.rsqrt(jnp.mean(vals32 * vals32, axis=-1, keepdims=True) + NORM_EPS)
    return (vals32 * inv_rms * gain_vec).astype(jnp.bfloat16), inv_rms


def rms_back(values, inv_rms, gain_vec, grad_out):
    vals32 = values.astype(jnp.float32)
    scaled = grad_out * gain_vec
    proj_mean = jnp.mean(scaled * vals32, axis=-1, keepdims=True)
    return inv_rms * scaled - vals32 * (inv_rms * inv_rms * inv_rms) * proj_mean


def mlp_forward(emb_rows, gain_in, gain_out, w_gate, w_up, w_down):
    normed_in, inv_in = rms_scale(emb_rows, gain_in)
    gate_pre = jnp.dot(normed_in, w_gate, preferred_element_type=jnp.float32).astype(jnp.bfloat16)
    up_proj = jnp.dot(normed_in, w_up, preferred_element_type=jnp.float32).astype(jnp.bfloat16)
    acts = (jax.nn.silu(gate_pre.astype(jnp.float32)) * up_proj.astype(jnp.float32)).astype(jnp.bfloat16)
    mlp_out = jnp.dot(acts, w_down, preferred_element_type=jnp.float32).astype(jnp.bfloat16)
    hidden = (emb_rows.astype(jnp.float32) + mlp_out.astype(jnp.float32)).astype(jnp.bfloat16)
    normed_out, inv_out = rms_scale(hidden, gain_out)
    return normed_out, (emb_rows, normed_in, inv_in, gate_pre, up_proj, acts, hidden, inv_out)


COLS_DIMS = (((1,), (1,)), ((), ()))
ROWS_DIMS = (((0,), (0,)), ((), ()))


def mlp_backward(saved, grad_normed, gain_in, gain_out, w_gate, w_up, w_down):
    emb_rows, normed_in, inv_in, gate_pre, up_proj, acts, hidden, inv_out = saved
    grad_hidden = rms_back(hidden, inv_out, gain_out, grad_normed)
    grad_mid = grad_hidden.astype(jnp.bfloat16)
    grad_acts = lax.dot_general(grad_mid, w_down, COLS_DIMS, preferred_element_type=jnp.float32)
    gate32 = gate_pre.astype(jnp.float32)
    gate_sig = jax.nn.sigmoid(gate32)
    grad_gate_pre = (grad_acts * up_proj.astype(jnp.float32) * gate_sig * (1.0 + gate32 * (1.0 - gate_sig))).astype(jnp.bfloat16)
    grad_up_proj = (grad_acts * gate32 * gate_sig).astype(jnp.bfloat16)
    grad_normed_in = (lax.dot_general(grad_gate_pre, w_gate, COLS_DIMS, preferred_element_type=jnp.float32)
                      + lax.dot_general(grad_up_proj, w_up, COLS_DIMS, preferred_element_type=jnp.float32))
    grad_rows = grad_hidden + rms_back(emb_rows, inv_in, gain_in, grad_normed_in)
    return grad_rows, grad_mid, grad_gate_pre, grad_up_proj


UNIT = 64
CUBE_BITS = 3
PARTS = 3
VOCAB_TILE = 256
STAT_ROWS = 2
MESH_ID = pl.DeviceIdType.MESH
PAD_LOGIT = -1e30


def head_kernel(vocab_rows, chunks, z_hbm, table_ref, lab_ref, dz_ref, dtable_ref, loss_ref,
                zbuf, lbuf, gbuf, dzbuf, got_core, got_one, got_two, got_three, stats, labs, norm, loss_acc,
                local_sem, ag_send, ag_recv, rs_send, rs_recv, st_send, st_recv, lab_send, lab_recv):
    me = lax.axis_index('fsdp')
    total = 16
    core = lax.rem(me, 2)
    pos = [lax.rem(me // 2, 2), lax.rem(me // 4, 2), me // 8]
    base = me * vocab_rows
    padded, dim = table_ref.shape
    part_cols = dim // PARTS
    half = 8 * UNIT
    tiles = padded // VOCAB_TILE

    def peer(axis):
        return me + (1 - 2 * pos[axis]) * (2 << axis)

    core_peer = me + 1 - 2 * core

    barrier = pltpu.get_barrier_semaphore()
    for step in range(1, total):
        pl.semaphore_signal(barrier, inc=1, device_id=(lax.rem(me + step, total),), device_id_type=MESH_ID)
    own = pltpu.make_async_copy(z_hbm, zbuf.at[:, pos[2], pos[1], pos[0], core], local_sem)
    own.start()
    dtable_ref[...] = jnp.zeros_like(dtable_ref)
    loss_acc[...] = jnp.zeros_like(loss_acc)
    labs[me] = jnp.zeros((1, half), jnp.float32)
    own.wait()
    pl.semaphore_wait(barrier, total - 1)

    def where(choice):
        return choice.get(2, slice(None)), choice.get(1, slice(None)), choice.get(0, slice(None))

    def axes(part):
        return part % 3, (part + 1) % 3, (part + 2) % 3

    def cols(part):
        return pl.ds(part * part_cols, part_cols)

    def gather_copies(chunk, phase):
        if phase == 4:
            here = zbuf.at[chunk, :, :, :, core]
            return [pltpu.make_async_remote_copy(here, here, ag_send.at[chunk, 9], ag_recv.at[chunk, 9],
                                                 device_id=(core_peer,), device_id_type=MESH_ID)]
        copies = []
        for part in range(PARTS):
            order = axes(part)
            fixed = {axis: pos[axis] for axis in order[phase - 1:]}
            iz, iy, ix = where(fixed)
            here = zbuf.at[chunk, iz, iy, ix, core, :, cols(part)]
            sem = (phase - 1) * PARTS + part
            copies.append(pltpu.make_async_remote_copy(here, here, ag_send.at[chunk, sem], ag_recv.at[chunk, sem],
                                                       device_id=(peer(order[phase - 1]),), device_id_type=MESH_ID))
        return copies

    def reduce_copies(chunk, phase):
        slot, dzs = lax.rem(chunk, 2), lax.rem(chunk, 3)
        if phase == 0:
            return [pltpu.make_async_remote_copy(dzbuf.at[dzs, :, :, :, 1 - core], got_core.at[slot], rs_send.at[chunk, 9], rs_recv.at[chunk, 9],
                                                 device_id=(core_peer,), device_id_type=MESH_ID)]
        copies = []
        for part in range(PARTS):
            order = axes(part)
            fixed = {axis: pos[axis] for axis in order[:phase - 1]}
            fixed[order[phase - 1]] = 1 - pos[order[phase - 1]]
            iz, iy, ix = where(fixed)
            got = (got_one, got_two, got_three)[phase - 1]
            sem = (phase - 1) * PARTS + part
            copies.append(pltpu.make_async_remote_copy(dzbuf.at[dzs, iz, iy, ix, core, :, cols(part)], got.at[slot, part],
                                                       rs_send.at[chunk, sem], rs_recv.at[chunk, sem],
                                                       device_id=(peer(order[phase - 1]),), device_id_type=MESH_ID))
        return copies

    def start(copies):
        for copy in copies:
            copy.start()

    def finish(copies):
        for copy in copies:
            copy.wait()

    def reduce_add(chunk, phase):
        slot, dzs = lax.rem(chunk, 2), lax.rem(chunk, 3)
        if phase == 0:
            dzbuf[dzs, :, :, :, core] += got_core[slot]
            return
        for part in range(PARTS):
            order = axes(part)
            iz, iy, ix = where({axis: pos[axis] for axis in order[:phase]})
            got = (got_one, got_two, got_three)[phase - 1]
            lanes = slice(part * part_cols, (part + 1) * part_cols)
            if phase == 3:
                rows = pl.ds(pl.multiple_of(chunk * UNIT, UNIT), UNIT)
                dz_ref[rows, lanes] = dzbuf[dzs, iz, iy, ix, core, :, lanes] + got[slot, part]
            else:
                dzbuf[dzs, iz, iy, ix, core, :, lanes] += got[slot, part]

    def stat_copies(chunk):
        copies = []
        for step in range(1, total):
            to = lax.rem(me + step, total)
            copies.append(pltpu.make_async_remote_copy(stats.at[chunk, me], stats.at[chunk, me], st_send.at[chunk, step], st_recv.at[chunk, step],
                                                       device_id=(to,), device_id_type=MESH_ID))
        return copies

    def lab_copies():
        return [pltpu.make_async_remote_copy(labs.at[me], labs.at[me], lab_send.at[step], lab_recv.at[step],
                                             device_id=(lax.rem(me + step, total),), device_id_type=MESH_ID) for step in range(1, total)]

    def label_row(chunk, part):
        lab = lab_ref[pl.ds(chunk * 2 + part, 1), :] - base
        return jnp.where(lab < vocab_rows, lab, -1)

    row_ids = lax.broadcasted_iota(jnp.int32, (VOCAB_TILE, half), 0)

    def forward_half(chunk, part):
        slot = lax.rem(chunk, 2)
        zb = zbuf[chunk, part].reshape(half, dim)
        lab = label_row(chunk, part)
        tops, sums, hits = [], [], []
        for tile in range(tiles):
            rows = slice(tile * VOCAB_TILE, (tile + 1) * VOCAB_TILE)
            logits = lax.dot_general(table_ref[rows, :], zb, COLS_DIMS, preferred_element_type=jnp.float32)
            if (tile + 1) * VOCAB_TILE > vocab_rows:
                logits = jnp.where(row_ids < vocab_rows - tile * VOCAB_TILE, logits, PAD_LOGIT)
            lbuf[slot, rows, part * half:(part + 1) * half] = logits
            top = jnp.max(logits, axis=0, keepdims=True)
            tops.append(top)
            sums.append(jnp.sum(jnp.exp(logits - top), axis=0, keepdims=True))
            hits.append(jnp.sum(jnp.where(row_ids == lab - tile * VOCAB_TILE, logits, 0.0), axis=0, keepdims=True))
        top = functools.reduce(jnp.maximum, tops)
        exp_sum = sum(s * jnp.exp(t - top) for s, t in zip(sums, tops))
        stats[chunk, me, part:part + 1, :] = top + jnp.log(exp_sum)
        labs[me] += sum(hits)

    def combine(chunk):
        for part in range(2):
            tops = stats[chunk, :, part, :]
            top = jnp.max(tops, axis=0, keepdims=True)
            exp_sum = jnp.sum(jnp.exp(tops - top), axis=0, keepdims=True)
            norm[part:part + 1, :] = top
            norm[2 + part:3 + part, :] = 1.0 / exp_sum
            loss_acc[...] += top + jnp.log(exp_sum)

    def table_half(chunk, which):
        slot = lax.rem(chunk, 2)
        zc = zbuf[chunk].reshape(2 * half, dim)
        for tile in range(which * tiles // 2, (which + 1) * tiles // 2):
            rows = slice(tile * VOCAB_TILE, (tile + 1) * VOCAB_TILE)
            for part in range(2):
                lanes = slice(part * half, (part + 1) * half)
                probs = jnp.exp(lbuf[slot, rows, lanes] - norm[part:part + 1, :]) * norm[2 + part:3 + part, :]
                hot = row_ids == label_row(chunk, part) - tile * VOCAB_TILE
                gbuf[rows, lanes] = jnp.where(hot, probs - 1.0, probs).astype(jnp.bfloat16)
            dtable_ref[rows, :] += jnp.dot(gbuf[rows, :], zc, preferred_element_type=jnp.float32)

    def token_half(chunk, part):
        dz = lax.dot_general(gbuf[:, part * half:(part + 1) * half], table_ref[...], ROWS_DIMS, preferred_element_type=jnp.float32)
        dzbuf[lax.rem(chunk, 3), part] = dz.reshape(2, 2, 2, UNIT, dim)

    start(gather_copies(0, 1))
    start(gather_copies(1, 1))
    start(gather_copies(2, 1))
    for chunk in range(3):
        finish(gather_copies(chunk, 1))
        start(gather_copies(chunk, 2))
    for chunk in range(2):
        finish(gather_copies(chunk, 2))
        start(gather_copies(chunk, 3))
    finish(gather_copies(0, 3))
    start(gather_copies(0, 4))
    finish(gather_copies(0, 4))

    def body(i, carry):
        def inside(offset, action):
            chunk = i + offset
            pl.when((chunk >= 0) & (chunk < chunks))(lambda: action(jnp.clip(chunk, 0, chunks - 1)))

        def step_reduce(phase, follow):
            def action(chunk):
                finish(reduce_copies(chunk, phase))
                reduce_add(chunk, phase)
                if follow:
                    start(reduce_copies(chunk, phase + 1))
            return action

        def step_gather(phase):
            def action(chunk):
                finish(gather_copies(chunk, phase))
                start(gather_copies(chunk, phase + 1))
            return action

        inside(-4, step_reduce(2, True))
        inside(-2, lambda chunk: start(reduce_copies(chunk, 0)))
        inside(1, step_gather(3))
        inside(3, lambda chunk: start(gather_copies(chunk, 1)))
        inside(2, step_gather(2))

        @pl.when(i < chunks)
        def _():
            forward_half(i, 0)
            forward_half(i, 1)

        inside(-2, step_reduce(0, False))
        inside(-3, step_reduce(1, True))
        inside(-4, step_reduce(3, False))
        inside(3, step_gather(1))
        inside(1, lambda chunk: finish(gather_copies(chunk, 4)))
        inside(-2, lambda chunk: start(reduce_copies(chunk, 1)))
        inside(0, lambda chunk: start(stat_copies(chunk)))

        @pl.when(i == chunks - 1)
        def _():
            start(lab_copies())

        def backward(chunk):
            finish(stat_copies(chunk))
            combine(chunk)
            table_half(chunk, 0)
            table_half(chunk, 1)
            token_half(chunk, 0)
            token_half(chunk, 1)

        inside(-1, backward)
        return carry

    lax.fori_loop(0, chunks + 4, body, 0)
    finish(lab_copies())
    loss_ref[...] = jnp.broadcast_to(jnp.sum(loss_acc[...] - jnp.sum(labs[...], axis=0), axis=1, keepdims=True), loss_ref.shape)


def head(z_local, table_padded, lab_rows, vocab_rows):
    tokens, dim = z_local.shape
    chunks = tokens // UNIT
    padded = table_padded.shape[0]
    chunk_tokens = 16 * UNIT
    part_cols = dim // PARTS
    f32, bf16 = jnp.float32, jnp.bfloat16
    sems = pltpu.SemaphoreType.DMA
    vmem = pl.BlockSpec(memory_space=pltpu.VMEM)
    cost = 6 * tokens * 16 * padded * dim
    return pl.pallas_call(
        functools.partial(head_kernel, vocab_rows, chunks),
        in_specs=[pl.BlockSpec(memory_space=pl.ANY), vmem, vmem],
        out_specs=[vmem, vmem, vmem],
        out_shape=[jax.ShapeDtypeStruct((tokens, dim), f32),
                   jax.ShapeDtypeStruct((padded, dim), f32),
                   jax.ShapeDtypeStruct((1, 128), f32)],
        scratch_shapes=[pltpu.VMEM((chunks, 2, 2, 2, 2, UNIT, dim), bf16),
                        pltpu.VMEM((2, padded, chunk_tokens), f32),
                        pltpu.VMEM((padded, chunk_tokens), bf16),
                        pltpu.VMEM((3, 2, 2, 2, 2, UNIT, dim), f32),
                        pltpu.VMEM((2, 2, 2, 2, UNIT, dim), f32),
                        pltpu.VMEM((2, PARTS, 2, 2, UNIT, part_cols), f32),
                        pltpu.VMEM((2, PARTS, 2, UNIT, part_cols), f32),
                        pltpu.VMEM((2, PARTS, UNIT, part_cols), f32),
                        pltpu.VMEM((chunks, 16, STAT_ROWS, 8 * UNIT), f32),
                        pltpu.VMEM((16, 1, 8 * UNIT), f32),
                        pltpu.VMEM((8, 8 * UNIT), f32),
                        pltpu.VMEM((1, 8 * UNIT), f32),
                        sems(()),
                        sems((chunks, 10)), sems((chunks, 10)),
                        sems((chunks, 10)), sems((chunks, 10)),
                        sems((chunks, 16)), sems((chunks, 16)),
                        sems((16,)), sems((16,))],
        compiler_params=pltpu.CompilerParams(vmem_limit_bytes=67043328, collective_id=1, has_side_effects=True),
        cost_estimate=pl.CostEstimate(flops=cost, bytes_accessed=4 * padded * dim, transcendentals=2 * tokens * 16 * padded),
        name="head_all",
    )(z_local.reshape(chunks, UNIT, dim), table_padded, lab_rows)


PIECES = 4


def axes(part):
    return part % 3, (part + 1) % 3, (part + 2) % 3


def cube_index(choice):
    return choice.get(2, slice(None)), choice.get(1, slice(None)), choice.get(0, slice(None))


def tail_kernel(table_rows, u_ref, acts_ref, mid_ref, gate_ref, up_ref, send_hbm, row_ref, dtable_hbm, gate_out, up_out, down_out, dtable_hbm_out,
                all_g, all_u, all_d, core_g, core_u, core_d, one_g, one_u, one_d, two_g, two_u, two_d, three_g, three_u, three_d,
                rows_got, split, dtable_out, local_sem, send_sem, recv_sem, row_send, row_recv):
    me = lax.axis_index('fsdp')
    total = 16
    core = lax.rem(me, 2)
    pos = [lax.rem(me // 2, 2), lax.rem(me // 4, 2), me // 8]
    core_peer = me + 1 - 2 * core
    whole = (all_g, all_u, all_d)
    gots = ((core_g, core_u, core_d), (one_g, one_u, one_d), (two_g, two_u, two_d), (three_g, three_u, three_d))
    outs = (gate_out, up_out, down_out)

    barrier = pltpu.get_barrier_semaphore()
    for step in range(1, total):
        pl.semaphore_signal(barrier, inc=1, device_id=(lax.rem(me + step, total),), device_id_type=MESH_ID)
    loads = []
    loads.append(pltpu.make_async_copy(dtable_hbm.at[pl.ds(0, table_rows)], dtable_out, local_sem.at[3]))
    loads.append(pltpu.make_async_copy(send_hbm.at[me], rows_got.at[me], local_sem.at[4]))
    for load in loads:
        load.start()
    pl.semaphore_wait(barrier, total - 1)

    def piece(part, q):
        if part == 2:
            size = all_d.shape[4] // PIECES
            return pl.ds(q * size, size), slice(None)
        size = all_g.shape[5] // PIECES
        return slice(None), pl.ds(q * size, size)

    def copies(phase, q, parts=(0, 1, 2)):
        made = []
        for part in parts:
            rows, lanes = piece(part, q)
            order = axes(part)
            if phase == 0:
                src = whole[part].at[1 - core, :, :, :, rows, lanes]
                dst = gots[0][part].at[:, :, :, rows, lanes]
                to = core_peer
            else:
                fixed = {axis: pos[axis] for axis in order[:phase - 1]}
                fixed[order[phase - 1]] = 1 - pos[order[phase - 1]]
                iz, iy, ix = cube_index(fixed)
                src = whole[part].at[core, iz, iy, ix, rows, lanes]
                lead = (slice(None),) * (3 - phase)
                dst = gots[phase][part].at[lead + (rows, lanes)]
                axis = order[phase - 1]
                to = me + (1 - 2 * pos[axis]) * (2 << axis)
            made.append(pltpu.make_async_remote_copy(src, dst, send_sem.at[phase, part, q], recv_sem.at[phase, part, q],
                                                     device_id=(to,), device_id_type=MESH_ID))
        return made

    def start(made):
        for copy in made:
            copy.start()

    def finish_add(phase, q):
        for copy in copies(phase, q):
            copy.wait()
        for part in range(3):
            rows, lanes = piece(part, q)
            iz, iy, ix = cube_index({axis: pos[axis] for axis in axes(part)[:phase]})
            got = gots[phase][part][(slice(None),) * (3 - phase) + (rows, lanes)]
            if phase == 3:
                outs[part][rows, lanes] = whole[part][core, iz, iy, ix, rows, lanes] + got
            else:
                whole[part][core, iz, iy, ix, rows, lanes] += got

    row_copies = []
    for step in range(1, total):
        to = lax.rem(me + step, total)
        row_copies.append(pltpu.make_async_remote_copy(send_hbm.at[to], rows_got.at[me], row_send.at[step], row_recv.at[step],
                                                       device_id=(to,), device_id_type=MESH_ID))
    start(row_copies)
    down_rows = all_d.shape[4]
    for chip in range(8):
        block = lax.dot_general(acts_ref[:, 2 * chip * down_rows:2 * (chip + 1) * down_rows], mid_ref[...], ROWS_DIMS,
                                preferred_element_type=jnp.float32)
        for c in range(2):
            all_d[c, chip // 4, chip // 2 % 2, chip % 2] = block[c * down_rows:(c + 1) * down_rows]
    for q in range(PIECES):
        start(copies(0, q, (2,)))
    unit, lanes = all_g.shape[4], all_g.shape[5] // PIECES
    for q in range(PIECES):
        here = slice(q * lanes, (q + 1) * lanes)
        for grads, array in ((gate_ref, all_g), (up_ref, all_u)):
            for h in range(2):
                block = lax.dot_general(u_ref[:, 8 * unit * h:8 * unit * (h + 1)], grads[:, here], ROWS_DIMS, preferred_element_type=jnp.float32)
                for k in range(8):
                    array[k % 2, h, k // 4, k // 2 % 2, :, here] = block[k * unit:(k + 1) * unit]
        start(copies(0, q, (0, 1)))
    for load in loads:
        load.wait()
    for q in range(PIECES):
        finish_add(0, q)
        start(copies(1, q))
    for copy in row_copies:
        copy.wait()
    slots, dim = rows_got.shape[0] * rows_got.shape[1], rows_got.shape[2]

    pair = 2 * rows_got.shape[1]

    def split_rows(s, carry):
        vals = rows_got[pl.ds(2 * s, 2)].reshape(pair, dim)
        at = pl.multiple_of(s * pair, pair)
        high = vals.astype(jnp.bfloat16)
        rest = vals - high.astype(jnp.float32)
        mid = rest.astype(jnp.bfloat16)
        split[pl.ds(at, pair), :] = high
        split[pl.ds(slots + at, pair), :] = mid
        split[pl.ds(2 * slots + at, pair), :] = (rest - mid.astype(jnp.float32)).astype(jnp.bfloat16)
        return carry

    lax.fori_loop(0, total // 2, split_rows, 0)

    def add_rows(first, count):
        ids = lax.broadcasted_iota(jnp.int32, (count, slots), 0) + first
        hot = jnp.where(ids == row_ref[...], 1.0, 0.0).astype(jnp.bfloat16)
        dtable_out[pl.ds(first, count), :] += jnp.dot(jnp.concatenate([hot, hot, hot], axis=1), split[...], preferred_element_type=jnp.float32)

    full = table_rows // VOCAB_TILE

    def add_tile(tile, carry):
        add_rows(pl.multiple_of(tile * VOCAB_TILE, VOCAB_TILE), VOCAB_TILE)
        return carry

    lax.fori_loop(0, full, add_tile, 0)
    if table_rows % VOCAB_TILE:
        add_rows(full * VOCAB_TILE, table_rows % VOCAB_TILE)

    save = pltpu.make_async_copy(dtable_out, dtable_hbm_out, local_sem.at[0])
    for q in range(PIECES + 2):
        if q == 1:
            save.start()
        if q < PIECES:
            finish_add(1, q)
            start(copies(2, q))
        if 1 <= q <= PIECES:
            finish_add(2, q - 1)
            start(copies(3, q - 1))
        if q >= 2:
            finish_add(3, q - 2)
    save.wait()


def tail(normed_in, acts, grad_mid, grad_gate_pre, grad_up_proj, send, row_idx, dtable, table_rows):
    f32 = jnp.float32
    vmem = pl.BlockSpec(memory_space=pltpu.VMEM)
    anywhere = pl.BlockSpec(memory_space=pl.ANY)
    sems = pltpu.SemaphoreType.DMA
    ffn = acts.shape[1]
    blocks = [(normed_in.shape[1] // 16, ffn), (normed_in.shape[1] // 16, ffn), (ffn // 16, normed_in.shape[1])]
    scratch = [pltpu.VMEM(lead + block, f32) for lead in ((2, 2, 2, 2), (2, 2, 2), (2, 2), (2,), ()) for block in blocks]
    slots = send.shape[0] * send.shape[1]
    dim = send.shape[2]
    return pl.pallas_call(
        functools.partial(tail_kernel, table_rows),
        in_specs=[vmem, vmem, vmem, vmem, vmem, anywhere, vmem, anywhere],
        out_specs=[vmem, vmem, vmem, anywhere],
        out_shape=[jax.ShapeDtypeStruct(block, f32) for block in blocks] + [jax.ShapeDtypeStruct((table_rows, dim), f32)],
        scratch_shapes=scratch + [pltpu.VMEM(send.shape, f32), pltpu.VMEM((3 * slots, dim), jnp.bfloat16), pltpu.VMEM((table_rows, dim), f32),
                                  sems((5,)), sems((4, 3, PIECES)), sems((4, 3, PIECES)), sems((16,)), sems((16,))],
        compiler_params=pltpu.CompilerParams(vmem_limit_bytes=67043328, collective_id=2, has_side_effects=True),
        cost_estimate=pl.CostEstimate(flops=6 * slots * table_rows * dim, bytes_accessed=40 * 1024 * 1024, transcendentals=0),
        name="tail_all",
    )(normed_in, acts, grad_mid, grad_gate_pre, grad_up_proj, send, row_idx, dtable)


def front_kernel(table_rows, pack_hbm, table_ref, gate_hbm, up_hbm, down_hbm,
                 pack_out, table_hbm_out, gate_hbm_out, up_hbm_out, down_hbm_out, x_out, slots_out, rows_out, rank_out,
                 table_out, gate_out, up_out, down_out, send, got, before_ref, rank_top, local_sem, save_sem, id_send, id_recv, w_send, w_recv, c_send, c_recv, row_send, row_recv):
    me = lax.axis_index('fsdp')
    total = 16
    core = lax.rem(me, 2)
    pos = [lax.rem(me // 2, 2), lax.rem(me // 4, 2), me // 8]
    core_peer = me + 1 - 2 * core
    shards = (gate_hbm, up_hbm, down_hbm)
    outs = (gate_out, up_out, down_out)
    tokens = pack_out.shape[2]
    padded, dim = table_out.shape

    barrier = pltpu.get_barrier_semaphore()
    for step in range(1, total):
        pl.semaphore_signal(barrier, inc=1, device_id=(lax.rem(me + step, total),), device_id_type=MESH_ID)
    loads = [pltpu.make_async_copy(shards[part], outs[part].at[pos[2], pos[1], pos[0], core], local_sem.at[part]) for part in range(3)]
    loads.append(pltpu.make_async_copy(pack_hbm, pack_out.at[me], local_sem.at[3]))
    for load in loads:
        load.start()

    def remote(src, dst, send_sem, recv_sem, to):
        return pltpu.make_async_remote_copy(src, dst, send_sem, recv_sem, device_id=(to,), device_id_type=MESH_ID)

    def wide(phase):
        made = []
        for part in range(3):
            order = axes(part)
            iz, iy, ix = cube_index({axis: pos[axis] for axis in order[phase - 1:]})
            here = outs[part].at[iz, iy, ix, core]
            axis = order[phase - 1]
            made.append(remote(shards[part] if phase == 1 else here, here, w_send.at[phase, part], w_recv.at[phase, part],
                               me + (1 - 2 * pos[axis]) * (2 << axis)))
        return made

    def across(stage):
        made = []
        for part in range(3):
            order = axes(part)
            fixed = {axis: pos[axis] for axis in order[stage:]}
            if stage:
                fixed[order[stage - 1]] = 1 - pos[order[stage - 1]]
            iz, iy, ix = cube_index(fixed)
            here = outs[part].at[iz, iy, ix, core]
            made.append(remote(here if stage else shards[part], here, c_send.at[stage, part], c_recv.at[stage, part], core_peer))
        return made

    def id_copies():
        return [remote(pack_hbm, pack_out.at[me], id_send.at[step], id_recv.at[step], lax.rem(me + step, total)) for step in range(1, total)]

    def row_copy(step):
        to = lax.rem(me + step, total)
        return remote(send.at[to], got.at[me], row_send.at[step], row_recv.at[step], to)

    def start(made):
        for copy in made:
            copy.start()

    def finish(made):
        for copy in made:
            copy.wait()

    pl.semaphore_wait(barrier, total - 1)
    start(id_copies())
    start(wide(1))
    start(across(0))
    table_out[0:table_rows, :] = table_ref[...]
    table_out[table_rows:padded, :] = jnp.zeros((padded - table_rows, dim), table_out.dtype)
    earlier = lax.broadcasted_iota(jnp.int32, (tokens, tokens), 0) < lax.broadcasted_iota(jnp.int32, (tokens, tokens), 1)
    before_ref[...] = jnp.where(earlier, 1.0, 0.0).astype(jnp.bfloat16)
    rank_top[...] = jnp.zeros_like(rank_top)
    for load in loads:
        load.wait()
    finish(id_copies())

    lanes_iota = lax.broadcasted_iota(jnp.int32, (4 * SLOTS, padded), 1)
    slot_iota = lax.broadcasted_iota(jnp.int32, (SLOTS, tokens), 0)
    dev_iota = lax.broadcasted_iota(jnp.int32, (total, tokens), 0)

    def rank_of(to):
        ids = pack_out[to, 0:1, :]
        owner = jnp.zeros_like(ids)
        for k in range(1, total):
            owner = owner + jnp.where(ids >= k * table_rows, 1, 0)
        hot = jnp.where(dev_iota == owner, 1.0, 0.0)
        before = jnp.dot(hot.astype(jnp.bfloat16), before_ref[...], preferred_element_type=jnp.float32)
        rank = jnp.sum(hot * before, axis=0, keepdims=True)
        rank_top[...] = jnp.maximum(rank_top[...], rank)
        return ids, owner, rank.astype(jnp.int32)

    def build(group):
        columns = []
        for step in range(4 * group, 4 * group + 4):
            to = lax.rem(me + step, total)
            ids, owner, rank = rank_of(to)
            if step == 0:
                slots_out[...] = jnp.where(rank < SLOTS, owner * SLOTS + rank, -1)
            picked = jnp.where(slot_iota == jnp.where(owner == me, rank, -1), 1.0, 0.0)
            code = ids - me * table_rows + 1
            columns.append(jnp.sum(picked * code.astype(jnp.float32), axis=1, keepdims=True).astype(jnp.int32) - 1)
            high = lax.shift_right_arithmetic(code, 6)
            digits = jnp.where(owner == me, jnp.concatenate([high, code - high * 64], axis=0), 0)
            digits = jnp.concatenate([digits, jnp.zeros((6, tokens), jnp.int32)], axis=0).astype(jnp.float32).astype(jnp.bfloat16)
            spread = lax.dot_general(digits, picked.astype(jnp.bfloat16), COLS_DIMS, preferred_element_type=jnp.float32)
            rows_out[pl.ds(to, 1), :] = (spread[0:1] * 64.0 + spread[1:2]).astype(jnp.int32) - 1
        choose = jnp.where(lanes_iota == jnp.concatenate(columns, axis=0), 1.0, 0.0).astype(jnp.bfloat16)
        rows = jnp.dot(choose, table_out[...], preferred_element_type=jnp.float32).astype(jnp.bfloat16)
        for j in range(4):
            send[lax.rem(me + 4 * group + j, total)] = rows[j * SLOTS:(j + 1) * SLOTS]

    own_rows = pltpu.make_async_copy(send.at[me], got.at[me], local_sem.at[4])
    build(0)
    finish(wide(1))
    start(wide(2))
    start(across(1))
    start([row_copy(step) for step in range(1, 4)])
    build(1)
    own_rows.start()
    start([row_copy(step) for step in range(4, 8)])
    build(2)
    start([row_copy(step) for step in range(8, 12)])
    build(3)
    rank_out[...] = jnp.broadcast_to(jnp.max(rank_top[...], axis=1, keepdims=True), rank_out.shape).astype(jnp.int32)
    start([row_copy(step) for step in range(12, 16)])
    finish(wide(2))
    start(wide(3))
    start(across(2))
    saves = [pltpu.make_async_copy(table_out, table_hbm_out, save_sem.at[9])]
    saves[0].start()
    results = (gate_hbm_out, up_hbm_out, down_hbm_out)

    def save(mine, which, sem):
        for part in range(3):
            axis = axes(part)[2]
            index = cube_index({axis: pos[axis] if mine else 1 - pos[axis]}) + (which,)
            saves.append(pltpu.make_async_copy(outs[part].at[index], results[part].at[index], save_sem.at[sem * 3 + part]))
            saves[-1].start()

    for stage in range(3):
        finish(across(stage))
    save(True, slice(None), 0)
    own_rows.wait()
    finish([row_copy(step) for step in range(1, total)])
    place = lax.broadcasted_iota(jnp.int32, (total * SLOTS, tokens), 0) == slots_out[...]
    x_out[...] = lax.dot_general(jnp.where(place, 1.0, 0.0).astype(jnp.bfloat16), got[...].reshape(total * SLOTS, dim), ROWS_DIMS,
                                 preferred_element_type=jnp.float32).astype(jnp.bfloat16)
    finish(wide(3))
    start(across(3))
    save(False, core, 1)
    finish(across(3))
    save(False, 1 - core, 2)
    for copy in saves:
        copy.wait()


def front(packed, table_shard, gate_shard, up_shard, down_shard):
    bf16 = jnp.bfloat16
    rows, dim = table_shard.shape
    padded = -(-rows // VOCAB_TILE) * VOCAB_TILE
    tokens = packed.shape[1]
    vmem = pl.BlockSpec(memory_space=pltpu.VMEM)
    anywhere = pl.BlockSpec(memory_space=pl.ANY)
    sems = pltpu.SemaphoreType.DMA
    shards = (gate_shard, up_shard, down_shard)
    return pl.pallas_call(
        functools.partial(front_kernel, rows),
        in_specs=[anywhere, vmem, anywhere, anywhere, anywhere],
        out_specs=[vmem] + [anywhere] * 4 + [vmem] * 4,
        out_shape=[jax.ShapeDtypeStruct((16,) + packed.shape, jnp.int32), jax.ShapeDtypeStruct((padded, dim), bf16)]
        + [jax.ShapeDtypeStruct((2, 2, 2, 2) + shard.shape, bf16) for shard in shards]
        + [jax.ShapeDtypeStruct((tokens, dim), bf16), jax.ShapeDtypeStruct((1, tokens), jnp.int32),
           jax.ShapeDtypeStruct((16, SLOTS), jnp.int32), jax.ShapeDtypeStruct((1, 128), jnp.int32)],
        scratch_shapes=[pltpu.VMEM((padded, dim), bf16)] + [pltpu.VMEM((2, 2, 2, 2) + shard.shape, bf16) for shard in shards]
        + [pltpu.VMEM((16, SLOTS, dim), bf16), pltpu.VMEM((16, SLOTS, dim), bf16), pltpu.VMEM((tokens, tokens), bf16), pltpu.VMEM((1, tokens), jnp.float32),
           sems((5,)), sems((10,)), sems((16,)), sems((16,)), sems((4, 3)), sems((4, 3)), sems((4, 3)), sems((4, 3)), sems((16,)), sems((16,))],
        compiler_params=pltpu.CompilerParams(vmem_limit_bytes=60 * 1024 * 1024, collective_id=3, has_side_effects=True),
        cost_estimate=pl.CostEstimate(flops=4 * 16 * SLOTS * padded * dim, bytes_accessed=20 * 1024 * 1024, transcendentals=0),
        name="front_all",
    )(packed, table_shard, gate_shard, up_shard, down_shard)


def split3(values):
    high = lax.reduce_precision(values, 8, 7)
    rest = values - high
    mid = lax.reduce_precision(rest, 8, 7)
    low = rest - mid
    return [part.astype(jnp.bfloat16) for part in (high, mid, low)]


def pick_rows(select, values):
    return jnp.dot(select, jnp.concatenate(split3(values), axis=0), preferred_element_type=jnp.float32)


def solution(mesh):
    groups = mesh.shape['fsdp']

    def device_step(token_ids, labels, table_shard, gate_shard, up_shard, down_shard, gain_in, gain_out):
        micro_count = token_ids.shape[0]
        tok_micro = token_ids.shape[1] * token_ids.shape[2]
        tok_dev = micro_count * tok_micro
        total_tokens = tok_dev * groups
        rows, dim = table_shard.shape
        me = lax.axis_index('fsdp')

        packed = jnp.stack([token_ids.reshape(tok_dev), labels.reshape(tok_dev)])
        gate_rows, ffn = gate_shard.shape
        down_rows = down_shard.shape[0]
        (packed_all, table_padded, w_gate, w_up, w_down, emb_rows, slots, row_idx, top_rank) = front(
            packed, table_shard, gate_shard, up_shard, down_shard)
        w_gate = w_gate.reshape(groups * gate_rows, ffn)
        w_up = w_up.reshape(groups * gate_rows, ffn)
        w_down = w_down.reshape(groups * down_rows, dim)
        rounds = top_rank[0, 0] // SLOTS + 1
        back_rounds = top_rank[0, 0] // BACK_SLOTS + 1

        def ranks(round_idx, count):
            ids_all, round_idx = lax.optimization_barrier((packed_all[:, 0], round_idx))
            owner = ids_all // rows
            owner_hot = owner[:, :, None] == jnp.arange(groups, dtype=jnp.int32)
            tri = jnp.tril(jnp.ones((tok_dev, tok_dev), jnp.bfloat16), -1)
            before = jnp.einsum('tu,suo->sto', tri, owner_hot.astype(jnp.bfloat16), preferred_element_type=jnp.float32)
            rank = jnp.sum(jnp.where(owner_hot, before, 0.0), axis=-1).astype(jnp.int32)
            return owner, ids_all - owner * rows, rank - round_idx * count

        def owned_rows(owner, local, rank, count):
            hit = (owner == me)[:, None, :] & (rank[:, None, :] == jnp.arange(count, dtype=jnp.int32)[None, :, None])
            return (jnp.sum(jnp.where(hit, local[:, None, :] + 1, 0), axis=-1) - 1).reshape(groups * count)

        def my_slots(owner, rank, count):
            mine = lax.dynamic_index_in_dim(owner, me, 0, keepdims=False)
            off = lax.dynamic_index_in_dim(rank, me, 0, keepdims=False)
            return jnp.where((off >= 0) & (off < count), mine * count + off, -1)

        def slot_place(slot_row, count):
            return (jnp.arange(groups * count, dtype=jnp.int32)[:, None] == slot_row[None, :]).astype(jnp.bfloat16)

        def fetch_round(round_idx):
            owner, local, rank = ranks(round_idx, SLOTS)
            select = (owned_rows(owner, local, rank, SLOTS)[:, None] == jnp.arange(rows, dtype=jnp.int32)[None, :]).astype(jnp.bfloat16)
            send = jnp.dot(select, table_shard, preferred_element_type=jnp.float32).astype(jnp.bfloat16)
            got = lax.all_to_all(send.reshape(groups, SLOTS, dim), 'fsdp', 0, 0).reshape(groups * SLOTS, dim)
            place = slot_place(my_slots(owner, rank, SLOTS), SLOTS)
            return lax.dot_general(place, got, ROWS_DIMS, preferred_element_type=jnp.float32).astype(jnp.bfloat16)

        def return_round(round_idx, grad_rows):
            owner, local, rank = ranks(round_idx, BACK_SLOTS)
            send = pick_rows(slot_place(jnp.tile(my_slots(owner, rank, BACK_SLOTS), 3), BACK_SLOTS), grad_rows)
            got = lax.all_to_all(send.reshape(groups, BACK_SLOTS, dim), 'fsdp', 0, 0).reshape(groups * BACK_SLOTS, dim)
            row_of = jnp.tile(owned_rows(owner, local, rank, BACK_SLOTS), 3)
            return pick_rows((jnp.arange(rows, dtype=jnp.int32)[:, None] == row_of[None, :]).astype(jnp.bfloat16), got)

        emb_rows = lax.fori_loop(1, rounds, lambda r, acc: acc + fetch_round(r), emb_rows)

        normed_out, saved = mlp_forward(emb_rows, gain_in, gain_out, w_gate, w_up, w_down)
        chunks = tok_dev // UNIT
        lab_rows = jnp.transpose(packed_all[:, 1].reshape(groups, chunks, UNIT), (1, 0, 2)).reshape(2 * chunks, groups * UNIT // 2)
        dz, dtable, loss_rows = head(normed_out, table_padded, lab_rows, rows)
        loss_total = loss_rows[0, 0]
        grad_rows, grad_mid, grad_gate_pre, grad_up_proj = mlp_backward(saved, dz, gain_in, gain_out, w_gate, w_up, w_down)
        normed_in, acts = saved[1], saved[5]
        first_rank = slots[0] % SLOTS
        back_slots = jnp.where((slots[0] >= 0) & (first_rank < BACK_SLOTS), slots[0] // SLOTS * BACK_SLOTS + first_rank, -1)
        send = pick_rows(slot_place(jnp.tile(back_slots, 3), BACK_SLOTS), grad_rows).reshape(groups, BACK_SLOTS, dim)
        out_gate, out_up, out_down, dtable = tail(normed_in, acts, grad_mid, grad_gate_pre, grad_up_proj, send,
                                                  row_idx[:, :BACK_SLOTS].reshape(1, groups * BACK_SLOTS), dtable, rows)
        dtable = lax.fori_loop(1, back_rounds, lambda r, acc: acc + return_round(r, grad_rows), dtable)
        return (loss_total / total_tokens, dtable, out_gate, out_up, out_down)

    row_spec = P('fsdp', None)
    tok_spec = P(None, 'fsdp', None)
    return jax.shard_map(device_step, mesh=mesh,
                         in_specs=(tok_spec, tok_spec, row_spec, row_spec, row_spec, row_spec, P(), P()),
                         out_specs=(P(), row_spec, row_spec, row_spec, row_spec), check_vma=False)
```
